32 devices in a mesh: dp: 1 (over z), tx: 4 (over y), ty: 8 (over x, core).
Axes of the slice: x: 4, y: 4, z: 1, core: 2. Of those that a mesh axis runs over, the one named last changes fastest.
The devices are a block of a 4x4x8 slice.
Arguments:
- x: bfloat16 [4096, 2048], P('dp', ('tx', 'ty'))
- seg_ids: int32 [4096], P('dp')
- positions: int32 [4096], P('dp')
- ln1_gain: bfloat16 [2, 2048], P(None, ('tx', 'ty'))
- ln1_bias: bfloat16 [2, 2048], P(None, ('tx', 'ty'))
- w_q: bfloat16 [2, 2048, 16, 128], P(None, 'tx', 'ty')
- b_q: bfloat16 [2, 16, 128], P(None, 'ty')
- w_k: bfloat16 [2, 2048, 16, 128], P(None, 'tx', 'ty')
- b_k: bfloat16 [2, 16, 128], P(None, 'ty')
- w_v: bfloat16 [2, 2048, 16, 128], P(None, 'tx', 'ty')
- b_v: bfloat16 [2, 16, 128], P(None, 'ty')
- w_o: bfloat16 [2, 16, 128, 2048], P(None, 'ty', None, 'tx')
- b_o: bfloat16 [2, 2048], P(None, ('tx', 'ty'))
- ln2_gain: bfloat16 [2, 2048], P(None, ('tx', 'ty'))
- ln2_bias: bfloat16 [2, 2048], P(None, ('tx', 'ty'))
- w_up: bfloat16 [2, 2048, 8192], P(None, 'tx', 'ty')
- b_up: bfloat16 [2, 8192], P(None, ('ty', 'tx'))
- w_down: bfloat16 [2, 8192, 2048], P(None, 'ty', 'tx')
- b_down: bfloat16 [2, 2048], P(None, ('tx', 'ty'))
Outputs:
- output 1: bfloat16 [4096, 2048], P('dp', ('tx', 'ty'))
- output 2: bfloat16 [2, 4096, 16, 128], P(None, ('dp', 'tx'), 'ty')
- output 3: bfloat16 [2, 4096, 16, 128], P(None, ('dp', 'tx'), 'ty')
All inputs are finite; a program needn't handle non-finite values.
Results may differ from the reference program's by a relative error of at most 0.0119909.
Values are sent between devices in bfloat16 or wider.
A program may use at most 768 MiB of HBM per device.

```python
import math
import jax
import jax.numpy as jnp
from jax import lax

TOKENS = 4096
D_MODEL = 2048
NUM_HEADS = 16
KV_HEADS = 16
HEAD_DIM = 128
FF_DIM = 8192
LAYERS = 2
WINDOW = 4096
ROPE_THETA = 100000
Q_BLOCK = 128


def draw_segments(seg_key):
    eighth = TOKENS // 8
    cut_low = jnp.array([1, eighth, 6 * eighth, 7 * eighth], dtype=jnp.int32)
    cut_high = jnp.array([eighth, 2 * eighth, 7 * eighth, TOKENS], dtype=jnp.int32)
    cut_points = jax.random.randint(seg_key, (4,), cut_low, cut_high, dtype=jnp.int32)
    tok_idx = jnp.arange(TOKENS, dtype=jnp.int32)
    after_cut = tok_idx[:, None] >= cut_points[None, :]
    seg_ids = jnp.sum(after_cut.astype(jnp.int32), axis=1)
    seg_start = jnp.max(jnp.where(after_cut, cut_points[None, :], 0), axis=1)
    return seg_ids, tok_idx - seg_start


def setup_inputs(seed: int = 0, part: int = 0) -> dict:
    part_key = jax.random.fold_in(jax.random.key(seed), part)
    key_x, key_mean, key_scale, key_slope, key_seg = jax.random.split(part_key, 5)
    width_ramp = jnp.linspace(-1.0, 1.0, D_MODEL, dtype=jnp.float32)
    ramp_slope = jax.random.uniform(key_slope, (2,), jnp.float32, 0.5, 1.0)
    col_mean = 0.4 * jax.random.normal(key_mean, (D_MODEL,), jnp.float32) + ramp_slope[0] * width_ramp
    col_scale = jnp.exp(0.3 * jax.random.normal(key_scale, (D_MODEL,), jnp.float32) - 0.5 * ramp_slope[1] * width_ramp)
    x_val = col_mean + col_scale * jax.random.normal(key_x, (TOKENS, D_MODEL), jnp.float32)
    seg_ids, positions = draw_segments(key_seg)
    w_keys = jax.random.split(jax.random.key(seed + 1), 16)

    def draw_param(key_idx, arr_shape, spread, offset):
        return (offset + spread * jax.random.normal(w_keys[key_idx], arr_shape, jnp.float32)).astype(jnp.bfloat16)

    vec_shape = (LAYERS, D_MODEL)
    qw_shape = (LAYERS, D_MODEL, NUM_HEADS, HEAD_DIM)
    kv_shape = (LAYERS, D_MODEL, KV_HEADS, HEAD_DIM)
    d_scale = D_MODEL ** -0.5
    return {
        'x': x_val.astype(jnp.bfloat16),
        'seg_ids': seg_ids,
        'positions': positions,
        'ln1_gain': draw_param(0, vec_shape, 0.25, 1.0),
        'ln1_bias': draw_param(1, vec_shape, 0.3, 0.0),
        'w_q': draw_param(2, qw_shape, 1.2 * d_scale, 0.0),
        'b_q': draw_param(3, (LAYERS, NUM_HEADS, HEAD_DIM), 0.3, 0.0),
        'w_k': draw_param(4, kv_shape, 1.2 * d_scale, 0.0),
        'b_k': draw_param(5, (LAYERS, KV_HEADS, HEAD_DIM), 0.3, 0.0),
        'w_v': draw_param(6, kv_shape, d_scale, 0.0),
        'b_v': draw_param(7, (LAYERS, KV_HEADS, HEAD_DIM), 0.3, 0.0),
        'w_o': draw_param(8, (LAYERS, NUM_HEADS, HEAD_DIM, D_MODEL), 2.0 * (NUM_HEADS * HEAD_DIM) ** -0.5, 0.0),
        'b_o': draw_param(9, vec_shape, 0.3, 0.0),
        'ln2_gain': draw_param(10, vec_shape, 0.25, 1.0),
        'ln2_bias': draw_param(11, vec_shape, 0.3, 0.0),
        'w_up': draw_param(12, (LAYERS, D_MODEL, FF_DIM), d_scale, 0.0),
        'b_up': draw_param(13, (LAYERS, FF_DIM), 0.3, 0.0),
        'w_down': draw_param(14, (LAYERS, FF_DIM, D_MODEL), 1.5 * FF_DIM ** -0.5, 0.0),
        'b_down': draw_param(15, vec_shape, 0.3, 0.0),
    }


def layer_norm(x_in, gain, bias):
    x_f32 = x_in.astype(jnp.float32)
    row_mean = jnp.sum(x_f32, axis=-1, keepdims=True) / D_MODEL
    row_var = jnp.sum(x_f32 * x_f32, axis=-1, keepdims=True) / D_MODEL - row_mean * row_mean
    normed = (x_f32 - row_mean) * lax.rsqrt(row_var + 1e-5)
    return (normed * gain.astype(jnp.float32) + bias.astype(jnp.float32)).astype(jnp.bfloat16)


def rotary_tables(positions):
    half_dim = HEAD_DIM // 2
    inv_freq = jnp.exp(jnp.arange(half_dim, dtype=jnp.float32) * (-2.0 * math.log(ROPE_THETA) / HEAD_DIM))
    angles = positions.astype(jnp.float32)[:, None] * inv_freq[None, :]
    return jnp.cos(angles)[:, None, :], jnp.sin(angles)[:, None, :]


def rotary(head_vals, cos_t, sin_t):
    half_dim = head_vals.shape[-1] // 2
    first_half = head_vals[..., :half_dim]
    second_half = head_vals[..., half_dim:]
    return jnp.concatenate([first_half * cos_t - second_half * sin_t, second_half * cos_t + first_half * sin_t], axis=-1)


def project(normed, weight, n_heads):
    flat = jnp.dot(normed, weight.reshape(D_MODEL, n_heads * HEAD_DIM), preferred_element_type=jnp.float32)
    return flat.reshape(TOKENS, n_heads, HEAD_DIM)


def attention(q_rot, key_rows, val_rows, seg_ids):
    q_block = min(TOKENS, Q_BLOCK)
    key_len = min(TOKENS, WINDOW + q_block)
    n_blocks = TOKENS // q_block
    group_size = NUM_HEADS // KV_HEADS
    score_scale = HEAD_DIM ** -0.5
    q_blocks = q_rot.astype(jnp.float32).reshape(n_blocks, q_block, KV_HEADS, group_size, HEAD_DIM)
    keys_f32 = key_rows.astype(jnp.float32)
    vals_f32 = val_rows.astype(jnp.float32)

    def one_block(block_args):
        blk_idx, q_blk = block_args
        q_first = blk_idx * q_block
        k_first = jnp.clip(q_first + q_block - key_len, 0, TOKENS - key_len)
        k_blk = lax.dynamic_slice_in_dim(keys_f32, k_first, key_len, 0)
        v_blk = lax.dynamic_slice_in_dim(vals_f32, k_first, key_len, 0)
        seg_kb = lax.dynamic_slice_in_dim(seg_ids, k_first, key_len, 0)
        seg_qb = lax.dynamic_slice_in_dim(seg_ids, q_first, q_block, 0)
        scores = jnp.einsum('qkgd,skd->kgqs', q_blk, k_blk) * score_scale
        key_gap = (q_first + jnp.arange(q_block))[:, None] - (k_first + jnp.arange(key_len))[None, :]
        allowed = (key_gap >= 0) & (key_gap < WINDOW) & (seg_qb[:, None] == seg_kb[None, :])
        scores = jnp.where(allowed, scores, -1e30)
        attn_prob = jax.nn.softmax(scores, axis=-1).astype(jnp.bfloat16).astype(jnp.float32)
        blk_out = jnp.einsum('kgqs,skd->qkgd', attn_prob, v_blk)
        return blk_out.astype(jnp.bfloat16)

    block_outs = lax.map(one_block, (jnp.arange(n_blocks), q_blocks))
    return block_outs.reshape(TOKENS, NUM_HEADS, HEAD_DIM)


def reference(x, seg_ids, positions, ln1_gain, ln1_bias, w_q, b_q, w_k, b_k, w_v, b_v, w_o, b_o, ln2_gain, ln2_bias, w_up, b_up, w_down, b_down):
    cos_t, sin_t = rotary_tables(positions)
    hidden = x
    k_list = []
    v_list = []
    for layer_idx in range(LAYERS):
        normed = layer_norm(hidden, ln1_gain[layer_idx], ln1_bias[layer_idx])
        q_lin = project(normed, w_q[layer_idx], NUM_HEADS) + b_q[layer_idx].astype(jnp.float32)
        k_lin = project(normed, w_k[layer_idx], KV_HEADS) + b_k[layer_idx].astype(jnp.float32)
        v_lin = project(normed, w_v[layer_idx], KV_HEADS) + b_v[layer_idx].astype(jnp.float32)
        q_rot = rotary(q_lin, cos_t, sin_t).astype(jnp.bfloat16)
        k_new = rotary(k_lin, cos_t, sin_t).astype(jnp.bfloat16)
        v_new = v_lin.astype(jnp.bfloat16)
        attn_out = attention(q_rot, k_new, v_new, seg_ids)
        o_lin = jnp.dot(attn_out.reshape(TOKENS, NUM_HEADS * HEAD_DIM), w_o[layer_idx].reshape(NUM_HEADS * HEAD_DIM, D_MODEL), preferred_element_type=jnp.float32)
        hidden = (hidden.astype(jnp.float32) + o_lin + b_o[layer_idx].astype(jnp.float32)).astype(jnp.bfloat16)
        normed2 = layer_norm(hidden, ln2_gain[layer_idx], ln2_bias[layer_idx])
        up_lin = jnp.dot(normed2, w_up[layer_idx], preferred_element_type=jnp.float32) + b_up[layer_idx].astype(jnp.float32)
        gelu_out = jax.nn.gelu(up_lin, approximate=True).astype(jnp.bfloat16)
        down_lin = jnp.dot(gelu_out, w_down[layer_idx], preferred_element_type=jnp.float32)
        hidden = (hidden.astype(jnp.float32) + down_lin + b_down[layer_idx].astype(jnp.float32)).astype(jnp.bfloat16)
        k_list.append(k_new)
        v_list.append(v_new)
    return (hidden, jnp.stack(k_list), jnp.stack(v_list))
```

```python
import math
import functools
import jax
import jax.numpy as jnp
from jax import lax
from jax.experimental import pallas as pl
from jax.experimental.pallas import tpu as pltpu
from jax.sharding import PartitionSpec as P

MESH = pl.DeviceIdType.MESH
F32 = jnp.float32
BF16 = jnp.bfloat16
ROPE_THETA = 100000.0
BK = 256
LOG2E = 1.4426950408889634


def rows_norm(x_f32, gain, bias):
    width = x_f32.shape[-1]
    mean = jnp.sum(x_f32, axis=-1, keepdims=True) / width
    var = jnp.sum(x_f32 * x_f32, axis=-1, keepdims=True) / width - mean * mean
    normed = (x_f32 - mean) * lax.rsqrt(var + 1e-5)
    return (normed * gain.astype(F32) + bias.astype(F32)).astype(BF16)


class Ring:
    def __init__(self, num_tx, num_ty):
        self.ty = lax.axis_index('ty')
        self.y = lax.axis_index('tx')
        self.num_tx, self.num_ty = num_tx, num_ty
        self.n_chip = num_ty // 2
        self.x = self.ty // 2
        self.c = self.ty % 2

    def side(self, k):
        return lax.rem(self.y + k, self.num_tx)

    def chip(self, k):
        return lax.rem(self.x + k, self.n_chip)

    def peer(self, k):
        return {'ty': self.chip(k) * 2 + self.c}

    def sibling(self):
        return {'ty': self.x * 2 + (1 - self.c)}


def remote(src, dst, send_sem, recv_sem, to):
    return pltpu.make_async_remote_copy(src_ref=src, dst_ref=dst, send_sem=send_sem, recv_sem=recv_sem, device_id=to,
                                        device_id_type=MESH)


def at(y, ty):
    return {'tx': y, 'ty': ty}


def signal(to):
    pl.semaphore_signal(pltpu.get_barrier_semaphore(), inc=1, device_id=to, device_id_type=MESH)


def copy_or_send(here, src, dst, send_sem, recv_sem, to):
    @pl.when(here)
    def _():
        pltpu.make_async_copy(src, dst, recv_sem).start()

    @pl.when(jnp.logical_not(here))
    def _():
        remote(src, dst, send_sem, recv_sem, to).start()


def sent(here, src, dst, send_sem, recv_sem, to):
    @pl.when(jnp.logical_not(here))
    def _():
        remote(src, dst, send_sem, recv_sem, to).wait_send()


AG_SIB, AG_R0, AG_R1, AG_L1, AG_L0, AG_FR, AG_FL = 0, 1, 2, 3, 4, 5, 6
AG_SL, AG_SR, AG_SO0, AG_SO1 = 7, 8, 9, 10
AG_SEMS = 11


class RowGather:
    def __init__(self, ring, buf, sems, rows):
        r = ring
        half = rows // 2
        mine, other = r.c * rows, (1 - r.c) * rows
        right, left, far = r.chip(1), r.chip(r.n_chip - 1), r.chip(2)

        def cp(slot, i, off, n, to):
            ref = buf.at[slot, pl.ds(pl.multiple_of(off, 16), n)]
            return remote(ref, ref, sems.at[0, i], sems.at[1, i], to)

        sib, to_r, to_l = r.sibling(), r.peer(1), r.peer(r.n_chip - 1)
        self.s_sib = cp(r.x, AG_SIB, mine, rows, sib)
        self.s_r0 = cp(r.x, AG_R0, mine, half, to_r)
        self.s_r1 = cp(r.x, AG_R1, mine + half, half, to_r)
        self.s_l1 = cp(r.x, AG_L1, mine + half, half, to_l)
        self.s_l0 = cp(r.x, AG_L0, mine, half, to_l)
        self.s_fr = cp(left, AG_FR, mine, half, to_r)
        self.s_fl = cp(right, AG_FL, mine + half, half, to_l)
        self.s_sl = cp(left, AG_SL, mine, rows, sib)
        self.s_sr = cp(right, AG_SR, mine, rows, sib)
        self.s_so0 = cp(far, AG_SO0, mine, half, sib)
        self.s_so1 = cp(far, AG_SO1, mine + half, half, sib)
        self.r_sib = cp(r.x, AG_SIB, other, rows, sib)
        self.r_r0 = cp(left, AG_R0, mine, half, to_r)
        self.r_r1 = cp(left, AG_R1, mine + half, half, to_r)
        self.r_l1 = cp(right, AG_L1, mine + half, half, to_l)
        self.r_l0 = cp(right, AG_L0, mine, half, to_l)
        self.r_fr = cp(far, AG_FR, mine, half, to_r)
        self.r_fl = cp(far, AG_FL, mine + half, half, to_l)
        self.r_sl = cp(left, AG_SL, other, rows, sib)
        self.r_sr = cp(right, AG_SR, other, rows, sib)
        self.r_so0 = cp(far, AG_SO0, other, half, sib)
        self.r_so1 = cp(far, AG_SO1, other + half, half, sib)

    def start(self):
        for s in (self.s_sib, self.s_r0, self.s_l1, self.s_r1, self.s_l0):
            s.start()

    def own(self):
        self.r_sib.wait_recv()

    def relay(self):
        self.r_r0.wait_recv()
        self.s_fr.start()
        self.r_l1.wait_recv()
        self.s_fl.start()

    def near(self):
        self.r_r1.wait_recv()
        self.s_sl.start()
        self.r_l0.wait_recv()
        self.s_sr.start()

    def near_left(self):
        self.r_sl.wait_recv()

    def near_right(self):
        self.r_sr.wait_recv()

    def far(self):
        self.r_fr.wait_recv()
        self.s_so0.start()
        self.r_fl.wait_recv()
        self.s_so1.start()
        self.r_so0.wait_recv()
        self.r_so1.wait_recv()

    def finish(self):
        for s in (self.s_sib, self.s_r0, self.s_r1, self.s_l1, self.s_l0, self.s_fr, self.s_fl, self.s_sl, self.s_sr,
                  self.s_so0, self.s_so1):
            s.wait_send()


def gelu_tanh(x):
    return 0.5 * x * (1.0 + jnp.tanh(0.7978845608028654 * (x + 0.044715 * (x * x * x))))


RS_SIB, RS_B, RS_A, RS_OA, RS_OB, RS_SA, RS_SB = 0, 4, 5, 6, 7, 8, 9
RS_SEMS = 10


def mlp_kernel(num_tx, num_ty, o_hbm, hid_ref, wo_hbm, wu_hbm, wd_hbm, bo_ref, g2_ref, b2_ref, bu_ref, bd_ref, y_ref,
               wo, wu, wd, obuf, u_all, x1, g_ref, full, sibin, far_in, fin, w_sems, a_sems, g_sems, r_sems):
    ring = Ring(num_tx, num_ty)
    rows, width = hid_ref.shape
    head_w = o_hbm.shape[1]
    n_col = wo_hbm.shape[0]
    col_w = wo_hbm.shape[2]
    half_w = width // 2
    n_chip = ring.n_chip
    last = n_chip - 1
    x, y, c = ring.x, ring.y, ring.c
    loads = [pltpu.make_async_copy(wo_hbm, wo, w_sems.at[0]), pltpu.make_async_copy(wu_hbm, wu, w_sems.at[1]),
             pltpu.make_async_copy(wd_hbm, wd, w_sems.at[2])]
    for ld in loads:
        ld.start()

    par = lax.rem(x, 2)
    targets, sources = [], []
    for dy in range(num_tx):
        for dx in range(n_chip // 2):
            for dc in range(2):
                targets.append((ring.side(dy), lax.rem(x // 2 + dx, n_chip // 2) * 2 + c, lax.rem(c + dc, 2)))
        for dx in range(n_chip):
            sources.append((ring.side(num_tx - dy), lax.rem(x + n_chip - dx, n_chip)))
    for ys, xs in sources[1:]:
        signal(at(ys, xs * 2 + par))

    @pl.when(par != c)
    def _():
        signal(ring.sibling())
    for to in (ring.sibling(), ring.peer(1), ring.peer(last)):
        signal(to)
    n_far = len(targets) - 1
    barrier = pltpu.get_barrier_semaphore()

    @pl.when(par == c)
    def _():
        pl.semaphore_wait(barrier, n_far + 3)

    @pl.when(par != c)
    def _():
        pl.semaphore_wait(barrier, n_far + 4)

    head_cols = pl.ds(pl.multiple_of((x * num_tx + y) * head_w, head_w), head_w)
    here = par == c

    def o_piece(n):
        yt, xt, ct = targets[n]
        at_row = (yt * (n_chip // 2) + xt // 2) * (2 * rows) + ct * rows
        return (o_hbm.at[pl.ds(pl.multiple_of(at_row, rows), rows)], obuf.at[:, head_cols], a_sems.at[0, n],
                a_sems.at[1, y * n_chip + x], at(yt, xt * 2 + ct))
    for n in list(range(1, len(targets))) + [0]:
        if n == 0:
            copy_or_send(here, *o_piece(n))
        else:
            remote(*o_piece(n)).start()
    loads[0].wait()
    for ys in range(num_tx):
        for xs in range(n_chip):
            remote(o_hbm.at[pl.ds(0, rows)], obuf.at[:, pl.ds((xs * num_tx + ys) * head_w, head_w)], a_sems.at[0, 0],
                   a_sems.at[1, ys * n_chip + xs], ring.sibling()).wait_recv()

    def project(t, carry):
        cols = pl.ds(pl.multiple_of(t * col_w, col_w), col_w)
        x1[:, cols] = (hid_ref[:, cols].astype(F32) + jnp.dot(obuf[...], wo[t], preferred_element_type=F32)
                       + bo_ref[:, cols].astype(F32)).astype(BF16)
        return carry
    lax.fori_loop(0, n_col, project, 0)
    u_all[ring.x, pl.ds(pl.multiple_of(c * rows, rows), rows), :] = rows_norm(x1[...].astype(F32), g2_ref[...], b2_ref[...])

    gather = RowGather(ring, u_all, g_sems, rows)
    gather.start()
    loads[1].wait()
    loads[2].wait()

    mine = pl.ds(pl.multiple_of(c * rows, rows), rows)
    other = pl.ds(pl.multiple_of((1 - c) * rows, rows), rows)
    sib = [remote(full.at[k, other], sibin.at[k], r_sems.at[0, RS_SIB + k], r_sems.at[1, RS_SIB + k], ring.sibling()) for k in range(4)]

    def mlp(k):
        slot = ring.chip(k)
        n_up = wu.shape[1] // 512

        def up(n, carry):
            cols = pl.ds(pl.multiple_of(n * 512, 512), 512)
            h = jnp.dot(u_all[slot], wu[:, cols], preferred_element_type=F32) + bu_ref[:, cols].astype(F32)
            g_ref[:, cols] = gelu_tanh(h).astype(BF16)
            return carry
        lax.fori_loop(0, n_up, up, 0)

        def down(t, carry):
            full[k, :, pl.ds(pl.multiple_of(t * col_w, col_w), col_w)] = jnp.dot(g_ref[...], wd[t], preferred_element_type=F32)
            return carry
        lax.fori_loop(0, n_col, down, 0)
        sib[k].start()

    def add_half(k, lo, src):
        cols = pl.ds(lo, half_w)
        full[k, mine, cols] = full[k, mine, cols] + src

    left_h, right_h = pl.ds(0, half_w), pl.ds(half_w, half_w)
    to_r, to_l = ring.peer(1), ring.peer(last)
    s_b = remote(full.at[1, mine, right_h], fin.at[0], r_sems.at[0, RS_B], r_sems.at[1, RS_B], to_r)
    s_a = remote(full.at[3, mine, left_h], fin.at[1], r_sems.at[0, RS_A], r_sems.at[1, RS_A], to_l)
    s_oa = remote(full.at[2, mine, left_h], far_in.at[0], r_sems.at[0, RS_OA], r_sems.at[1, RS_OA], to_r)
    s_ob = remote(full.at[2, mine, right_h], far_in.at[1], r_sems.at[0, RS_OB], r_sems.at[1, RS_OB], to_l)
    s_sa = remote(full.at[1, mine, left_h], fin.at[2], r_sems.at[0, RS_SA], r_sems.at[1, RS_SA], to_r)
    s_sb = remote(full.at[3, mine, right_h], fin.at[3], r_sems.at[0, RS_SB], r_sems.at[1, RS_SB], to_l)

    def pair_sum(k):
        sib[k].wait_recv()
        full[k, mine] = full[k, mine] + sibin[k]

    gather.own()
    mlp(0)
    gather.relay()
    gather.near()
    gather.near_right()
    mlp(1)
    gather.near_left()
    pair_sum(1)
    s_b.start()
    mlp(3)
    gather.far()
    pair_sum(3)
    s_a.start()
    mlp(2)
    pair_sum(0)
    pair_sum(2)
    s_oa.start()
    s_ob.start()
    x1_f = x1[...].astype(F32) + bd_ref[...].astype(F32)
    full[0, mine] = full[0, mine] + x1_f
    s_oa.wait_recv()
    add_half(1, 0, far_in[0])
    s_sa.start()
    s_ob.wait_recv()
    add_half(3, half_w, far_in[1])
    s_sb.start()
    s_b.wait_recv()
    add_half(0, half_w, fin[0])
    s_a.wait_recv()
    add_half(0, 0, fin[1])
    s_sa.wait_recv()
    y_ref[:, left_h] = (full[0, mine, left_h] + fin[2]).astype(BF16)
    s_sb.wait_recv()
    y_ref[:, right_h] = (full[0, mine, right_h] + fin[3]).astype(BF16)
    for n in range(1, len(targets)):
        remote(*o_piece(n)).wait_send()
    sent(here, *o_piece(0))
    for s in sib + [s_b, s_a, s_oa, s_ob, s_sa, s_sb]:
        s.wait_send()
    gather.finish()


def mlp_call(num_tx, num_ty, o, hid, wo, wu, wd, bo, g2, b2, bu, bd, cid):
    rows, width = hid.shape
    n_chip = num_ty // 2
    vm = pl.BlockSpec(memory_space=pltpu.VMEM)
    hb = pl.BlockSpec(memory_space=pl.ANY)
    half_w = width // 2
    ff = wu.shape[1]
    dma = pltpu.SemaphoreType.DMA
    return pl.pallas_call(
        functools.partial(mlp_kernel, num_tx, num_ty),
        out_shape=jax.ShapeDtypeStruct((rows, width), BF16),
        in_specs=[hb, vm, hb, hb, hb] + [vm] * 5,
        out_specs=vm,
        scratch_shapes=[pltpu.VMEM(wo.shape, BF16), pltpu.VMEM(wu.shape, BF16), pltpu.VMEM(wd.shape, BF16),
                        pltpu.VMEM((rows, width), BF16), pltpu.VMEM((n_chip, 2 * rows, width), BF16),
                        pltpu.VMEM((rows, width), BF16), pltpu.VMEM((2 * rows, ff), BF16),
                        pltpu.VMEM((n_chip, 2 * rows, width), F32), pltpu.VMEM((n_chip, rows, width), F32),
                        pltpu.VMEM((2, rows, half_w), F32), pltpu.VMEM((4, rows, half_w), F32),
                        dma((4,)), dma((2, num_tx * n_chip)), dma((2, AG_SEMS)), dma((2, RS_SEMS))],
        compiler_params=pltpu.CompilerParams(collective_id=cid, has_side_effects=True, vmem_limit_bytes=56 << 20),
        cost_estimate=pl.CostEstimate(flops=80_000_000_000, bytes_accessed=20 << 20, transcendentals=0),
        name="mlp",
    )(o, hid, wo, wu, wd, bo, g2, b2, bu, bd)


def qkv_kernel(num_tx, num_ty, hid_ref, g1_ref, b1_ref, wq_hbm, wk_hbm, wv_hbm, bq_ref, bk_ref, bv_ref, cos_ref, sin_ref,
               kc_ref, vc_ref, kv_hbm, qh_hbm, w, a_all, st, w_sems, g_sems, snd_sems, kv_sems, q_sems, f_sems):
    ring = Ring(num_tx, num_ty)
    rows, width = hid_ref.shape
    loc_w = wq_hbm.shape[1]
    head_w = kv_hbm.shape[2]
    loc_heads = loc_w // head_w
    n_chip = ring.n_chip
    last = n_chip - 1
    blk = 2 * rows
    x, y, c = ring.x, ring.y, ring.c
    loads = [pltpu.make_async_copy(src, w.at[:, pl.ds(i * loc_w, loc_w)], w_sems.at[i])
             for i, src in enumerate((wq_hbm, wk_hbm, wv_hbm))]
    for ld in loads:
        ld.start()

    src_core = y // loc_heads
    for dy in range(1, num_tx):
        signal(at(ring.side(dy), x * 2 + src_core))

    @pl.when(src_core != c)
    def _():
        signal(ring.sibling())
    for to in (ring.sibling(), ring.peer(1), ring.peer(last)):
        signal(to)
    barrier = pltpu.get_barrier_semaphore()

    @pl.when(src_core == c)
    def _():
        pl.semaphore_wait(barrier, 2 * loc_heads - 1 + 3)

    @pl.when(src_core != c)
    def _():
        pl.semaphore_wait(barrier, 2 * loc_heads + 3)

    a_all[x, pl.ds(pl.multiple_of(c * rows, rows), rows), :] = rows_norm(hid_ref[...].astype(F32), g1_ref[...], b1_ref[...])
    gather = RowGather(ring, a_all, g_sems, rows)
    gather.start()
    for ld in loads:
        ld.wait()

    def block_rows(ys, slot):
        return pl.ds(pl.multiple_of((ys * n_chip + slot) * blk, blk), blk)

    def pieces(k):
        slot = ring.chip(k)
        out = []
        for h in range(loc_heads):
            yd = c * loc_heads + h
            for r in range(2):
                here = jnp.logical_and(yd == y, c == r)
                out.append((here, st.at[k, h, r], kv_hbm.at[r, block_rows(y, slot)], snd_sems.at[(k * loc_heads + h) * 3 + r],
                            kv_sems.at[y * n_chip + slot], at(yd, x * 2 + r)))
            par = lax.rem(slot, 2)
            q_at = y * (n_chip // 2) + slot // 2
            here = jnp.logical_and(yd == y, c == par)
            out.append((here, st.at[k, h, 2], qh_hbm.at[pl.ds(pl.multiple_of(q_at * blk, blk), blk)],
                        snd_sems.at[(k * loc_heads + h) * 3 + 2], q_sems.at[q_at], at(yd, x * 2 + par)))
        return out

    def project(k):
        slot = ring.chip(k)
        at_row = pl.ds(pl.multiple_of(slot * blk, blk), blk)
        acc = jnp.dot(a_all[slot], w[...], preferred_element_type=F32)
        cos_t, sin_t = cos_ref[at_row, :], sin_ref[at_row, :]

        def turned(i, h, bias_ref):
            lanes = slice(h * head_w, (h + 1) * head_w)
            v = acc[:, i * loc_w + h * head_w:i * loc_w + (h + 1) * head_w] + bias_ref[:, lanes].astype(F32)
            if i < 2:
                v = v * cos_t + pltpu.roll(v, head_w // 2, 1) * sin_t
            return v.astype(BF16)
        for h in range(loc_heads):
            lanes = slice(h * head_w, (h + 1) * head_w)
            st[k, h, 2] = turned(0, h, bq_ref)
            k_new = turned(1, h, bk_ref)
            st[k, h, 0] = k_new
            kc_ref[at_row, lanes] = k_new
            v_new = turned(2, h, bv_ref)
            st[k, h, 1] = v_new
            vc_ref[at_row, lanes] = v_new
        for p in pieces(k):
            copy_or_send(*p)

    gather.own()
    project(0)
    gather.relay()
    gather.near()
    gather.near_right()
    project(1)
    gather.near_left()
    project(last)
    gather.far()
    project(2)

    def forward(i, r):
        ref = kv_hbm.at[r, pl.ds(pl.multiple_of(i * blk, blk), blk)]
        return remote(ref, ref, f_sems.at[0, i], f_sems.at[1, i], ring.sibling())

    for k in (0, 1, last, 2):
        for dy in (0, 1, num_tx - 1, 2):
            i = ring.side(dy) * n_chip + ring.chip(k)
            remote(st.at[0, 0, 0], kv_hbm.at[c, pl.ds(pl.multiple_of(i * blk, blk), blk)], snd_sems.at[0], kv_sems.at[i],
                   ring.sibling()).wait_recv()
            forward(i, c).start()
    for i in range(num_tx * n_chip // 2):
        remote(st.at[0, 0, 0], qh_hbm.at[pl.ds(i * blk, blk)], snd_sems.at[0], q_sems.at[i], ring.sibling()).wait_recv()
    for i in range(num_tx * n_chip):
        forward(i, 1 - c).wait_recv()
        forward(i, c).wait_send()
    for k in range(n_chip):
        for p in pieces(k):
            sent(*p)
    gather.finish()


def qkv_call(num_tx, num_ty, hid, g1, b1, wq, wk, wv, bq, bk, bv, cos2, sin2, head_w, cid):
    rows, width = hid.shape
    n_chip = num_ty // 2
    loc_w = wq.shape[1]
    loc_heads = loc_w // head_w
    blk = 2 * rows
    n_blk = num_tx * n_chip
    vm = pl.BlockSpec(memory_space=pltpu.VMEM)
    hb = pl.BlockSpec(memory_space=pl.ANY)
    dma = pltpu.SemaphoreType.DMA
    cache = jax.ShapeDtypeStruct((n_chip * blk, loc_w), BF16)
    return pl.pallas_call(
        functools.partial(qkv_kernel, num_tx, num_ty),
        out_shape=(cache, cache, jax.ShapeDtypeStruct((2, n_blk * blk, head_w), BF16),
                   jax.ShapeDtypeStruct((n_blk // 2 * blk, head_w), BF16)),
        in_specs=[vm] * 3 + [hb] * 3 + [vm] * 5,
        out_specs=(vm, vm, hb, hb),
        scratch_shapes=[pltpu.VMEM((width, 3 * loc_w), BF16), pltpu.VMEM((n_chip, blk, width), BF16),
                        pltpu.VMEM((n_chip, loc_heads, 3, blk, head_w), BF16),
                        dma((3,)), dma((2, AG_SEMS)), dma((n_chip * loc_heads * 3,)), dma((n_blk,)), dma((n_blk // 2,)),
                        dma((2, n_blk))],
        compiler_params=pltpu.CompilerParams(collective_id=cid, has_side_effects=True, vmem_limit_bytes=40 << 20),
        cost_estimate=pl.CostEstimate(flops=30_000_000_000, bytes_accessed=8 << 20, transcendentals=0),
        name="qkv",
    )(hid, g1, b1, wq, wk, wv, bq, bk, bv, cos2, sin2)


def attn_kernel(bounds, q_ref, k_ref, v_ref, start_ref, o_ref, s_ref):
    bq, head_dim = q_ref.shape
    n_blocks = pl.num_programs(0)
    blk = pl.program_id(0)
    q0 = (2 * blk + bounds[0]) * bq
    s_min = bounds[1 + blk]
    s_max = bounds[1 + n_blocks + blk]
    lo = s_min // BK
    hi = (q0 + bq - 1) // BK + 1
    diag = q0 // BK
    mid = jnp.minimum((s_max + BK - 1) // BK, diag)
    scale = head_dim ** -0.5 * LOG2E
    q = q_ref[...]
    start = start_ref[...]
    q_pos = q0 + lax.broadcasted_iota(jnp.int32, (bq, BK), 0)

    def fold(op, m, s):
        for i in range(BK // 128):
            m = op(m, s[:, i * 128:(i + 1) * 128])
        return m

    def score(j):
        k = k_ref[0, pl.ds(pl.multiple_of(j * BK, BK), BK), :]
        return lax.dot_general(q, k, (((1,), (1,)), ((), ())), preferred_element_type=F32) * scale

    def masked(j, m):
        s = score(j)
        k_pos = j * BK + lax.broadcasted_iota(jnp.int32, (bq, BK), 1)
        s = jnp.where((k_pos <= q_pos) & (k_pos >= start), s, -1e30)
        s_ref[j] = s
        return fold(jnp.maximum, m, s)

    def plain(j, m):
        s = score(j)
        s_ref[j] = s
        return fold(jnp.maximum, m, s)

    m = jnp.full((bq, 128), -1e30, F32)
    m = lax.fori_loop(lo, mid, masked, m)
    m = lax.fori_loop(mid, diag, plain, m)
    m = lax.fori_loop(diag, hi, masked, m)
    m = jnp.max(m, axis=1, keepdims=True)

    def expo(j, l):
        p = jnp.exp2(s_ref[j] - m)
        s_ref[j] = p
        return fold(jnp.add, l, p)

    l = lax.fori_loop(lo, hi, expo, jnp.zeros((bq, 128), F32))
    inv = 1.0 / jnp.sum(l, axis=1, keepdims=True)

    def apply(j, acc):
        p = (s_ref[j] * inv).astype(BF16)
        v = v_ref[0, pl.ds(pl.multiple_of(j * BK, BK), BK), :]
        return acc + jnp.dot(p, v, preferred_element_type=F32)

    o_ref[...] = lax.fori_loop(lo, hi, apply, jnp.zeros((bq, head_dim), F32)).astype(BF16)


def attention(q, kv, bounds, start, bq):
    n_query, head_dim = q.shape
    n_key = kv.shape[1]
    return pl.pallas_call(
        attn_kernel,
        grid_spec=pltpu.PrefetchScalarGridSpec(
            num_scalar_prefetch=1,
            grid=(n_query // bq,),
            in_specs=[pl.BlockSpec((bq, head_dim), lambda i, b: (i, 0)),
                      pl.BlockSpec((1, n_key, head_dim), lambda i, b: (0, 0, 0)),
                      pl.BlockSpec((1, n_key, head_dim), lambda i, b: (1, 0, 0)),
                      pl.BlockSpec((bq, 1), lambda i, b: (i, 0))],
            out_specs=pl.BlockSpec((bq, head_dim), lambda i, b: (i, 0)),
            scratch_shapes=[pltpu.VMEM((n_key // BK, bq, BK), F32)]),
        out_shape=jax.ShapeDtypeStruct((n_query, head_dim), BF16),
        cost_estimate=pl.CostEstimate(flops=10_000_000_000, bytes_accessed=4 * n_key * head_dim, transcendentals=0),
        name="attn",
    )(bounds, q, kv, kv, start)


def solution(mesh):
    num_tx = mesh.shape['tx']
    num_ty = mesh.shape['ty']
    width_spec = P('dp', ('tx', 'ty'))
    vec_spec = P(None, ('tx', 'ty'))
    proj_spec = P(None, 'tx', 'ty', None)
    head_spec = P(None, 'ty', None)
    cache_spec = P(None, ('dp', 'tx'), 'ty', None)
    in_specs = (width_spec, P('dp'), P('dp'), vec_spec, vec_spec, proj_spec, head_spec, proj_spec, head_spec,
                proj_spec, head_spec, P(None, 'ty', None, 'tx'), vec_spec, vec_spec, vec_spec,
                P(None, 'tx', 'ty'), P(None, ('ty', 'tx')), P(None, 'ty', 'tx'), vec_spec)
    out_specs = (width_spec, cache_spec, cache_spec)

    def device_fn(x_loc, seg_all, pos_all, ln1_gain, ln1_bias, w_q, b_q, w_k, b_k, w_v, b_v, w_o, b_o,
                  ln2_gain, ln2_bias, w_up, b_up, w_down, b_down):
        n_tok = x_loc.shape[0]
        tok_loc = n_tok // num_tx
        L, d_rows, loc_heads, head_dim = w_q.shape
        both = ('tx', 'ty')
        blk = 2 * tok_loc // num_ty
        core = lax.axis_index('ty') % 2

        q_start = lax.axis_index('tx') * tok_loc
        pos_q = lax.dynamic_slice_in_dim(pos_all, q_start, tok_loc, 0)
        inv_freq = jnp.exp(jnp.arange(head_dim // 2, dtype=F32) * (-2.0 * math.log(ROPE_THETA) / head_dim))
        angles = pos_q.astype(F32)[:, None] * inv_freq[None, :]
        cos_t, sin_t = jnp.cos(angles), jnp.sin(angles)
        cos2 = jnp.concatenate([cos_t, cos_t], axis=1)
        sin2 = jnp.concatenate([-sin_t, sin_t], axis=1)
        start = (jnp.arange(n_tok, dtype=jnp.int32) - pos_all).reshape(-1, 2, blk)
        start = lax.dynamic_index_in_dim(start, core, 1, keepdims=False)
        bounds = jnp.concatenate([core[None].astype(jnp.int32), start[:, 0], start[:, -1]])
        start = start.reshape(-1, 1)

        def gathered(l):
            wq, wk, wv = [lax.all_gather(w[l].reshape(d_rows, -1), 'tx', axis=0, tiled=True) for w in (w_q, w_k, w_v)]
            wo = lax.all_gather(w_o[l].reshape(-1, w_o.shape[-1]), 'tx', axis=0, tiled=False)
            wo = lax.all_gather(wo, 'ty', axis=1, tiled=True)
            wu = lax.all_gather(w_up[l], 'tx', axis=0, tiled=True)
            wd = lax.all_gather(w_down[l], 'tx', axis=0, tiled=False)
            return wq, wk, wv, wo, wu, wd

        weights = [gathered(l) for l in range(L)]
        hidden = lax.all_to_all(x_loc, both, split_axis=0, concat_axis=1, tiled=True)
        vecs = jnp.concatenate([ln1_gain, ln1_bias, ln2_gain, ln2_bias, b_o, b_down], axis=0)
        vecs = lax.all_gather(vecs, both, axis=1, tiled=True)
        b_up_all = lax.all_gather(b_up, 'tx', axis=1, tiled=True)
        k_list = []
        v_list = []
        for l in range(L):
            wq, wk, wv, wo, wu, wd = weights[l]
            vec = [vecs[i * L + l][None] for i in range(6)]
            k, v, kv, q = qkv_call(num_tx, num_ty, hidden, vec[0], vec[1], wq, wk, wv, b_q[l].reshape(1, -1),
                                   b_k[l].reshape(1, -1), b_v[l].reshape(1, -1), cos2, sin2, head_dim, 1)
            o = attention(q, kv, bounds, start, blk)
            hidden = mlp_call(num_tx, num_ty, o, hidden, wo, wu, wd, vec[4], vec[2], vec[3], b_up_all[l][None], vec[5], 2)
            k_list.append(k.reshape(tok_loc, loc_heads, head_dim))
            v_list.append(v.reshape(tok_loc, loc_heads, head_dim))
        y = lax.all_to_all(hidden, both, split_axis=1, concat_axis=0, tiled=True)
        return y, jnp.stack(k_list), jnp.stack(v_list)

    return jax.shard_map(device_fn, mesh=mesh, in_specs=in_specs, out_specs=out_specs, check_vma=False)
```

```python
import math
import functools
import jax
import jax.numpy as jnp
from jax import lax
from jax.experimental import pallas as pl
from jax.experimental.pallas import tpu as pltpu
from jax.sharding import PartitionSpec as P

MESH = pl.DeviceIdType.MESH
F32 = jnp.float32
BF16 = jnp.bfloat16
ROPE_THETA = 100000.0
LOG2E = 1.4426950408889634
LANES = 128
BK = 1024


def rows_norm(x_f32, gain, bias):
    width = x_f32.shape[-1]
    mean = jnp.sum(x_f32, axis=-1, keepdims=True) / width
    var = jnp.sum(x_f32 * x_f32, axis=-1, keepdims=True) / width - mean * mean
    normed = (x_f32 - mean) * lax.rsqrt(var + 1e-5)
    return (normed * gain + bias).astype(BF16)


def gelu_tanh(x):
    return 0.5 * x * (1.0 + jnp.tanh(0.7978845608028654 * (x + 0.044715 * (x * x * x))))


def rows(at, n):
    return pl.ds(pl.multiple_of(at, n), n)


class Place:
    def __init__(self, num_tx, num_ty):
        self.num_tx, self.num_ty, self.n_chip = num_tx, num_ty, num_ty // 2
        self.y = lax.axis_index('tx')
        self.ty = lax.axis_index('ty')
        self.x = self.ty // 2
        self.c = lax.rem(self.ty, 2)
        self.me = self.y * num_ty + self.ty
        self.sib = self.at(self.y, self.x * 2 + 1 - self.c)
        self.right, self.left = self.beside(1), self.beside(self.n_chip - 1)
        self.above, self.below = self.over(1), self.over(num_tx - 1)

    def at(self, y, ty):
        return {'tx': y, 'ty': ty}

    def chip(self, k):
        return lax.rem(self.x + k, self.n_chip)

    def side(self, k):
        return lax.rem(self.y + k, self.num_tx)

    def beside(self, k):
        return self.at(self.y, self.chip(k) * 2 + self.c)

    def over(self, k):
        return self.at(self.side(k), self.ty)


def remote(src, dst, send_sem, recv_sem, to):
    return pltpu.make_async_remote_copy(src_ref=src, dst_ref=dst, send_sem=send_sem, recv_sem=recv_sem, device_id=to,
                                        device_id_type=MESH)


def copy_or_send(here, src, dst, send_sem, recv_sem, to):
    @pl.when(here)
    def _():
        pltpu.make_async_copy(src, dst, recv_sem).start()

    @pl.when(jnp.logical_not(here))
    def _():
        remote(src, dst, send_sem, recv_sem, to).start()


def took(ref, sem):
    pltpu.make_async_copy(ref, ref, sem).wait()


class RingGather:
    SEMS = 14

    def __init__(self, p, view, sems):
        self.p = p
        self.view = view
        self.sems = sems
        x, c, d = p.x, p.c, 1 - p.c
        far, left, right = p.chip(2), p.chip(p.n_chip - 1), p.chip(1)
        self.plan = [(x, 0, p.right, left), (x, 1, p.left, right), (x, 1, p.right, left), (x, 0, p.left, right),
                     (left, 0, p.right, far), (right, 1, p.left, far),
                     (x, 0, p.sib, x), (x, 1, p.sib, x), (left, 0, p.sib, left), (left, 1, p.sib, left),
                     (right, 0, p.sib, right), (right, 1, p.sib, right), (far, 0, p.sib, far), (far, 1, p.sib, far)]

    def out(self, i):
        chip, half, to, _ = self.plan[i]
        ref = self.view(chip, self.p.c, half)
        return remote(ref, ref, self.sems.at[0, i], self.sems.at[1, i], to)

    def arrived(self, i):
        _, half, to, chip = self.plan[i]
        core = self.p.c if i < 6 else 1 - self.p.c
        ref = self.view(chip, core, half)
        remote(ref, ref, self.sems.at[0, i], self.sems.at[1, i], to).wait_recv()

    def start(self):
        for i in (6, 7, 0, 1, 2, 3):
            self.out(i).start()

    def own(self):
        self.arrived(6)
        self.arrived(7)

    def relay(self):
        self.arrived(0)
        self.out(4).start()
        self.arrived(1)
        self.out(5).start()
        self.out(8).start()
        self.out(11).start()

    def near(self):
        self.arrived(2)
        self.out(9).start()
        self.arrived(3)
        self.out(10).start()

    def near_right(self):
        self.arrived(10)
        self.arrived(11)

    def near_left(self):
        self.arrived(8)
        self.arrived(9)

    def far(self):
        self.arrived(4)
        self.out(12).start()
        self.arrived(5)
        self.out(13).start()

    def far_done(self):
        self.arrived(12)
        self.arrived(13)

    def drain(self):
        for i in range(self.SEMS):
            self.out(i).wait_send()


class ColumnGather:
    SEMS = 8

    def __init__(self, p, pieces, sems):
        self.p = p
        self.pieces = pieces
        self.sems = sems

    def copy(self, n, i):
        p = self.p
        src, dst = self.pieces[n]
        up, down = p.side(1), p.side(p.num_tx - 1)
        half, to = ((0, p.above), (1, p.below), (1, p.above), (0, p.below), (0, p.above), (1, p.below))[i]
        here = src(half) if i < 4 else dst(down if i == 4 else up, half)
        there = dst((p.y, p.y, p.y, p.y, down, up)[i], half)
        return remote(here, there, self.sems.at[0, n * self.SEMS + i], self.sems.at[1, n * self.SEMS + i], to)

    def arrived(self, n, i):
        p = self.p
        src, dst = self.pieces[n]
        up, down, far = p.side(1), p.side(p.num_tx - 1), p.side(2)
        half, frm = ((0, down), (1, up), (1, down), (0, up), (0, far), (1, far))[i]
        remote(src(half), dst(frm, half), self.sems.at[0, n * self.SEMS + i], self.sems.at[1, n * self.SEMS + i],
               p.above).wait_recv()

    def own(self, n, half):
        src, dst = self.pieces[n]
        return pltpu.make_async_copy(src(half), dst(self.p.y, half), self.sems.at[1, n * self.SEMS + 6 + half])

    def start(self):
        for i in range(4):
            for n in range(len(self.pieces)):
                self.copy(n, i).start()
        for n in range(len(self.pieces)):
            self.own(n, 0).start()
            self.own(n, 1).start()

    def relay(self):
        for n in range(len(self.pieces)):
            self.arrived(n, 0)
            self.copy(n, 4).start()
            self.arrived(n, 1)
            self.copy(n, 5).start()

    def finish(self):
        for n in range(len(self.pieces)):
            for i in (2, 3, 4, 5):
                self.arrived(n, i)
            self.own(n, 0).wait()
            self.own(n, 1).wait()

    def drain(self):
        for n in range(len(self.pieces)):
            for i in range(6):
                self.copy(n, i).wait_send()


RS_SIB, RS_B, RS_A, RS_OA, RS_OB, RS_SA, RS_SB = 0, 4, 5, 6, 7, 8, 9
RS_SEMS = 10


def decoder_kernel(num_tx, num_ty, n_layers,
                   xt_hbm, vec_ref, bup_ref, wq_hbm, wk_hbm, wv_hbm, wo_hbm, wu_hbm, wd_hbm, bqkv_ref, cos_ref, sin_ref,
                   start_ref,
                   yt_hbm, kc_hbm, vc_hbm, go_hbm,
                   xt, vbuf, vec, bup, w, wu, wd, wo, a_all, hid, x1, st, kv, qh, ob, obuf, g, full, sibin, far_in, fin,
                   x_sems, v_sems, b_sems, y_sems, a_sems, u_sems, wq_sems, wo_sems, wx_sems, wu_sems, wd_sems,
                   kv_sems, o_sems, r_sems, l_sems, c_sems):
    p = Place(num_tx, num_ty)
    n_dev = num_tx * num_ty
    n_chip, x, y, c, ty = p.n_chip, p.x, p.y, p.c, p.ty
    n_row, width = hid.shape
    blk = 2 * n_row
    loc_w = wq_hbm.shape[2]
    head_w = kv.shape[2]
    loc_heads = loc_w // head_w
    col_w = wd.shape[3]
    n_col = num_tx
    half_w = width // 2
    piece_w = xt_hbm.shape[0]
    last = n_chip - 1
    mine, other = rows(c * n_row, n_row), rows((1 - c) * n_row, n_row)

    barrier = pltpu.get_barrier_semaphore()
    devs = [lax.rem(p.me + k, n_dev) for k in range(1, n_dev)]
    devs = [p.at(d // num_ty, lax.rem(d, num_ty)) for d in devs]
    for to in devs:
        pl.semaphore_signal(barrier, inc=1, device_id=to, device_id_type=MESH)
    pl.semaphore_wait(barrier, n_dev - 1)

    def halves(ref, l, n):
        return lambda h: ref.at[l, pl.ds(h * n, n)]

    def shard_rows(dst, l, n_shard, n, cols):
        return lambda ys, h: dst.at[l, rows(ys * n_shard + h * n, n), cols]

    qkv_rows = wq_hbm.shape[1]
    up_rows = wu_hbm.shape[1]
    down_rows = wd_hbm.shape[1]
    o_rows = wo_hbm.shape[1]

    def gather_qkv(l):
        n = qkv_rows // 2
        return ColumnGather(p, [(halves(s, l, n), shard_rows(w, l, qkv_rows, n, pl.ds(i * loc_w, loc_w)))
                                for i, s in enumerate((wq_hbm, wk_hbm, wv_hbm))], wq_sems)

    def gather_up(l):
        n = up_rows // 2
        return ColumnGather(p, [(halves(wu_hbm, l, n), shard_rows(wu, l, up_rows, n, slice(None)))], wu_sems)

    def gather_down(l):
        n = down_rows // 2
        return ColumnGather(p, [(halves(wd_hbm, l, n), lambda ys, h: wd.at[l, ys, pl.ds(h * n, n)])], wd_sems)

    def gather_o(l):
        n = o_rows // 2
        return ColumnGather(p, [(halves(wo_hbm, l, n), lambda ys, h: go_hbm.at[l, ys, rows(ty * o_rows + h * n, n)])], wo_sems)

    def spread_o(l):
        n = n_col // 2
        return RingGather(p, lambda chip, core, h: go_hbm.at[l, pl.ds(h * n, n), rows((chip * 2 + core) * o_rows, o_rows)],
                          wx_sems)

    g_qkv = [gather_qkv(l) for l in range(n_layers)]
    g_up = [gather_up(l) for l in range(n_layers)]
    g_down = [gather_down(l) for l in range(n_layers)]
    g_o = [gather_o(l) for l in range(n_layers)]
    s_o = [spread_o(l) for l in range(n_layers)]

    for d, to in zip([lax.rem(p.me + k, n_dev) for k in range(1, n_dev)], devs):
        remote(xt_hbm.at[:, rows(d * n_row, n_row)], xt.at[rows(p.me * piece_w, piece_w)], x_sems.at[0], x_sems.at[1], to).start()
    pltpu.make_async_copy(xt_hbm.at[:, rows(p.me * n_row, n_row)], xt.at[rows(p.me * piece_w, piece_w)], x_sems.at[1]).start()
    for to in devs:
        remote(vec_ref, vbuf.at[p.me], v_sems.at[0], v_sems.at[1], to).start()
    pltpu.make_async_copy(vec_ref, vbuf.at[p.me], v_sems.at[1]).start()
    bup_w = bup_ref.shape[1]
    for k in range(1, num_tx):
        remote(bup_ref, bup.at[:, rows(y * bup_w, bup_w)], b_sems.at[0], b_sems.at[1], p.over(k)).start()
    pltpu.make_async_copy(bup_ref, bup.at[:, rows(y * bup_w, bup_w)], b_sems.at[1]).start()
    g_qkv[0].start()
    g_o[0].start()
    took(xt, x_sems.at[1])

    def turn(j, carry):
        hid[:, rows(j * LANES, LANES)] = xt[rows(j * LANES, LANES), :].T
        return carry
    lax.fori_loop(0, width // LANES, turn, 0)
    took(vbuf, v_sems.at[1])
    per = LANES // piece_w
    for j in range(width // LANES):
        vec[:, j * LANES:(j + 1) * LANES] = jnp.concatenate([vbuf[per * j + i][:, :piece_w] for i in range(per)], axis=1)
    took(bup, b_sems.at[1])

    def vector(i, l):
        return vec[i * n_layers + l:i * n_layers + l + 1, :]

    def row_gather(buf, sems):
        return RingGather(p, lambda chip, core, h: buf.at[chip, rows(core * n_row + h * (n_row // 2), n_row // 2)], sems)

    def project(l, k):
        slot = p.chip(k)
        at_row = rows(slot * blk, blk)
        acc = jnp.dot(a_all[slot], w[l], preferred_element_type=F32) + bqkv_ref[l:l + 1, :]
        cos_t, sin_t = cos_ref[at_row, :], sin_ref[at_row, :]
        for h in range(loc_heads):
            for i in range(3):
                v = acc[:, i * loc_w + h * head_w:i * loc_w + (h + 1) * head_w]
                if i < 2:
                    v = v * cos_t + pltpu.roll(v, head_w // 2, 1) * sin_t
                st[k, h, i] = v.astype(BF16)
        at_tok = rows((y * n_chip + slot) * blk, blk)
        par = lax.rem(slot, 2)
        at_q = rows((y * (n_chip // 2) + slot // 2) * blk, blk)
        for h in range(loc_heads):
            yd = c * loc_heads + h
            for r in range(2):
                copy_or_send(jnp.logical_and(yd == y, c == r), st.at[k, h, 1 + r], kv.at[r, at_tok], kv_sems.at[0],
                             kv_sems.at[1], p.at(yd, x * 2 + r))
            copy_or_send(jnp.logical_and(yd == y, c == par), st.at[k, h, 0], qh.at[at_q], kv_sems.at[2], kv_sems.at[3],
                         p.at(yd, x * 2 + par))
        for h in range(loc_heads):
            pltpu.make_async_copy(st.at[k, h, 1], kc_hbm.at[l, at_row, pl.ds(h * head_w, head_w)], c_sems.at[0]).start()
            pltpu.make_async_copy(st.at[k, h, 2], vc_hbm.at[l, at_row, pl.ds(h * head_w, head_w)], c_sems.at[1]).start()

    def attend(i, carry):
        b = 2 * i + c
        jd = i // 2
        q = qh[rows(i * blk, blk), :]
        first = jnp.broadcast_to(start_ref[rows(i * blk, blk), :], (blk, LANES))
        lane = lax.broadcasted_iota(jnp.int32, (blk, LANES), 1)
        q_pos = b * blk + lax.broadcasted_iota(jnp.int32, (blk, LANES), 0)
        scale = head_w ** -0.5 * LOG2E

        def cols(j, n):
            return j // 2, pl.ds(pl.multiple_of(lax.rem(j, 2) * BK, BK) + n * LANES, LANES)

        def score(j, m, diag):
            s = lax.dot_general(q, kv[0, rows(j * BK, BK), :], (((1,), (1,)), ((), ())), preferred_element_type=F32) * scale
            for n in range(BK // LANES):
                k_pos = lane + (j * BK + n * LANES)
                ok = k_pos >= first
                if diag:
                    ok = jnp.logical_and(ok, k_pos <= q_pos)
                part = jnp.where(ok, s[:, n * LANES:(n + 1) * LANES], -1e30)
                jj, cc = cols(j, n)
                full[jj, :, cc] = part
                m = jnp.maximum(m, part)
            return m
        m = lax.fori_loop(0, jd, lambda j, m: score(j, m, False), jnp.full((blk, LANES), -1e30, F32))
        m = jnp.max(score(jd, m, True), axis=1, keepdims=True)

        def expo(j, t):
            for n in range(BK // LANES):
                jj, cc = cols(j, n)
                e = jnp.exp2(full[jj, :, cc] - m)
                full[jj, :, cc] = e
                t = t + e
            return t
        t = lax.fori_loop(0, jd + 1, expo, jnp.zeros((blk, LANES), F32))
        inv = 1.0 / jnp.sum(t, axis=1, keepdims=True)

        def apply(j, acc):
            prob = (full[j // 2, :, rows(lax.rem(j, 2) * BK, BK)] * inv).astype(BF16)
            return acc + jnp.dot(prob, kv[1, rows(j * BK, BK), :], preferred_element_type=F32)
        ob[i] = lax.fori_loop(0, jd + 1, apply, jnp.zeros((blk, head_w), F32)).astype(BF16)
        yt, xd = b // n_chip, lax.rem(b, n_chip)
        cols_o = rows((x * num_tx + y) * head_w, head_w)
        for r in range(2):
            here = jnp.logical_and(jnp.logical_and(yt == y, xd == x), c == r)
            copy_or_send(here, ob.at[i, pl.ds(r * n_row, n_row)], obuf.at[:, cols_o], o_sems.at[0], o_sems.at[1],
                         p.at(yt, xd * 2 + r))
        return carry

    def up(l, k):
        slot = p.chip(k)

        def part(n, carry):
            cc = rows(n * 512, 512)
            h = jnp.dot(a_all[slot], wu[l, :, cc], preferred_element_type=F32) + bup[l:l + 1, cc]
            g[k, :, cc] = gelu_tanh(h).astype(BF16)
            return carry
        lax.fori_loop(0, wu.shape[2] // 512, part, 0)

    sib = [remote(full.at[k, other], sibin.at[k], r_sems.at[0, RS_SIB + k], r_sems.at[1, RS_SIB + k], p.sib)
           for k in range(n_chip)]

    def down(l, k):
        def part(t, carry):
            full[k, :, rows(t * col_w, col_w)] = jnp.dot(g[k], wd[l, t], preferred_element_type=F32)
            return carry
        lax.fori_loop(0, n_col, part, 0)
        sib[k].start()

    def pair_sum(k):
        sib[k].wait_recv()
        full[k, mine] = full[k, mine] + sibin[k]

    def rs(k, half, dst, i, to):
        return remote(full.at[k, mine, half], dst, r_sems.at[0, i], r_sems.at[1, i], to)

    lo, hi = pl.ds(0, half_w), pl.ds(half_w, half_w)
    s_b = rs(1, hi, fin.at[0], RS_B, p.right)
    s_a = rs(last, lo, fin.at[1], RS_A, p.left)
    s_oa = rs(2, lo, far_in.at[0], RS_OA, p.right)
    s_ob = rs(2, hi, far_in.at[1], RS_OB, p.left)
    s_sa = rs(1, lo, fin.at[2], RS_SA, p.right)
    s_sb = rs(last, hi, fin.at[3], RS_SB, p.left)

    for l in range(n_layers):
        first_layer, last_layer = l == 0, l == n_layers - 1
        a_all[x, mine, :] = rows_norm(hid[...].astype(F32), vector(0, l), vector(1, l))
        ga = row_gather(a_all, a_sems)
        ga.start()
        if first_layer:
            g_qkv[l].relay()
        ga.relay()
        ga.own()
        ga.near()
        if first_layer:
            g_o[l].relay()
        g_qkv[l].finish()
        g_o[l].finish()
        s_o[l].start()
        project(l, 0)
        ga.near_right()
        project(l, 1)
        ga.near_left()
        project(l, last)
        ga.far()
        ga.far_done()
        ga.drain()
        project(l, 2)
        if first_layer:
            g_up[l].start()
        else:
            g_up[l].relay()
            g_down[l].start()
        role = kv.at[c]
        took(role, kv_sems.at[1])
        forward = remote(role, role, kv_sems.at[4], kv_sems.at[5], p.sib)
        forward.start()
        s_o[l].relay()
        took(qh, kv_sems.at[3])
        remote(kv.at[1 - c], kv.at[1 - c], kv_sems.at[4], kv_sems.at[5], p.sib).wait_recv()
        forward.wait_send()
        n_q = ob.shape[0]
        lax.fori_loop(0, n_q // 2, attend, 0)
        s_o[l].near()
        lax.fori_loop(n_q // 2, n_q, attend, 0)
        if first_layer:
            g_up[l].relay()
            g_down[l].start()
        s_o[l].far()
        s_o[l].own()
        s_o[l].near_right()
        s_o[l].near_left()
        s_o[l].far_done()
        loads = [pltpu.make_async_copy(go_hbm.at[l, t], wo.at[t % 2], l_sems.at[t % 2]) for t in range(n_col)]
        loads[0].start()
        loads[1].start()
        took(obuf, o_sems.at[1])
        for t in range(n_col):
            loads[t].wait()
            cc = pl.ds(t * col_w, col_w)
            x1[:, cc] = (hid[:, cc].astype(F32) + jnp.dot(obuf[...], wo[t % 2], preferred_element_type=F32)
                         + vector(4, l)[:, t * col_w:(t + 1) * col_w]).astype(BF16)
            if t + 2 < n_col:
                loads[t + 2].start()
        a_all[x, mine, :] = rows_norm(x1[...].astype(F32), vector(2, l), vector(3, l))
        gu = row_gather(a_all, u_sems)
        gu.start()
        g_up[l].finish()
        if not first_layer:
            g_down[l].relay()
        gu.own()
        up(l, 0)
        gu.relay()
        gu.near()
        if not first_layer:
            g_down[l].finish()
        gu.near_right()
        up(l, 1)
        if not last_layer:
            gu.near_left()
            up(l, last)
            gu.far()
            gu.far_done()
            gu.drain()
            up(l, 2)
            g_down[l].relay()
            g_qkv[l].drain()
            g_o[l].drain()
            g_qkv[l + 1].start()
            g_o[l + 1].start()
            g_down[l].finish()
            down(l, 1)
            down(l, last)
            pair_sum(1)
            s_b.start()
            down(l, 2)
            pair_sum(last)
            s_a.start()
            down(l, 0)
        else:
            down(l, 1)
            gu.near_left()
            up(l, last)
            down(l, last)
            pair_sum(1)
            s_b.start()
            gu.far()
            down(l, 0)
            pair_sum(last)
            s_a.start()
            gu.far_done()
            up(l, 2)
            down(l, 2)
        pair_sum(2)
        s_oa.start()
        s_ob.start()
        if not last_layer:
            g_qkv[l + 1].relay()
            g_o[l + 1].relay()
            g_up[l].drain()
            g_up[l + 1].start()
        pair_sum(0)
        full[0, mine] = full[0, mine] + (x1[...].astype(F32) + vector(5, l))
        s_oa.wait_recv()
        full[1, mine, lo] = full[1, mine, lo] + far_in[0]
        s_sa.start()
        s_ob.wait_recv()
        full[last, mine, hi] = full[last, mine, hi] + far_in[1]
        s_sb.start()
        s_b.wait_recv()
        full[0, mine, hi] = full[0, mine, hi] + fin[0]
        s_a.wait_recv()
        full[0, mine, lo] = full[0, mine, lo] + fin[1]
        s_sa.wait_recv()
        hid[:, lo] = (full[0, mine, lo] + fin[2]).astype(BF16)
        s_sb.wait_recv()
        hid[:, hi] = (full[0, mine, hi] + fin[3]).astype(BF16)
        for s in sib + [s_b, s_a, s_oa, s_ob, s_sa, s_sb]:
            s.wait_send()
        if last_layer:
            gu.drain()
        s_o[l].drain()
        g_down[l].drain()
        if last_layer:
            for gth in (g_qkv[l], g_o[l], g_up[l]):
                gth.drain()
        sent_away(p, kv, qh, kv_sems, loc_heads)
        o_away(p, obuf, o_sems, head_w)
        took(kc_hbm.at[l], c_sems.at[0])
        took(vc_hbm.at[l], c_sems.at[1])

    def turn_back(j, carry):
        xt[rows(j * LANES, LANES), :] = hid[:, rows(j * LANES, LANES)].T
        return carry
    lax.fori_loop(0, width // LANES, turn_back, 0)
    for d, to in zip([lax.rem(p.me + k, n_dev) for k in range(1, n_dev)], devs):
        remote(xt.at[rows(d * piece_w, piece_w)], yt_hbm.at[:, rows(p.me * n_row, n_row)], y_sems.at[0], y_sems.at[1], to).start()
    pltpu.make_async_copy(xt.at[rows(p.me * piece_w, piece_w)], yt_hbm.at[:, rows(p.me * n_row, n_row)], y_sems.at[1]).start()
    took(xt_hbm.at[:, pl.ds(0, (n_dev - 1) * n_row)], x_sems.at[0])
    took(vbuf.at[pl.ds(0, n_dev - 1)], v_sems.at[0])
    took(bup.at[:, pl.ds(0, (num_tx - 1) * bup_w)], b_sems.at[0])
    took(yt_hbm, y_sems.at[1])
    took(xt.at[pl.ds(0, (n_dev - 1) * piece_w)], y_sems.at[0])


def sent_away(p, kv, qh, kv_sems, loc_heads):
    stays = p.c == p.y // loc_heads
    n_tok = kv.shape[1]
    n_q = qh.shape[0]

    @pl.when(stays)
    def _():
        took(kv.at[0, pl.ds(0, n_tok * 3 // 4)], kv_sems.at[0])
        took(qh.at[pl.ds(0, n_q * 3 // 4)], kv_sems.at[2])

    @pl.when(jnp.logical_not(stays))
    def _():
        took(kv.at[0], kv_sems.at[0])
        took(qh, kv_sems.at[2])


def o_away(p, obuf, o_sems, head_w):
    stays = lax.rem(p.x, 2) == p.c

    @pl.when(stays)
    def _():
        took(obuf.at[:, pl.ds(0, obuf.shape[1] - head_w)], o_sems.at[0])

    @pl.when(jnp.logical_not(stays))
    def _():
        took(obuf, o_sems.at[0])


def decoder(num_tx, num_ty, xt, vec, bup, wq, wk, wv, wo, wu, wd, bqkv, cos2, sin2, start, head_w):
    n_layers = wq.shape[0]
    n_dev = num_tx * num_ty
    n_chip = num_ty // 2
    piece_w, n_tok = xt.shape
    width = piece_w * n_dev
    n_row = n_tok // n_dev
    blk = 2 * n_row
    loc_w = wq.shape[2]
    loc_heads = loc_w // head_w
    tok_loc = n_tok // num_tx
    ff = wu.shape[2]
    col_w = wd.shape[2]
    half_w = width // 2
    n_q = n_tok // (2 * blk)
    vm = pl.BlockSpec(memory_space=pltpu.VMEM)
    hb = pl.BlockSpec(memory_space=pl.ANY)
    V = pltpu.VMEM
    dma = pltpu.SemaphoreType.DMA
    cache = jax.ShapeDtypeStruct((n_layers, tok_loc, loc_w), BF16)
    go = jax.ShapeDtypeStruct((n_layers, num_tx, wo.shape[1] * num_ty, col_w), BF16)
    CG, RG = ColumnGather.SEMS, RingGather.SEMS
    return pl.pallas_call(
        functools.partial(decoder_kernel, num_tx, num_ty, n_layers),
        out_shape=(jax.ShapeDtypeStruct((piece_w, n_tok), BF16), cache, cache, go),
        in_specs=[hb, vm, vm] + [hb] * 6 + [vm] * 4,
        out_specs=(hb,) * 4,
        scratch_shapes=[V((width, n_row), BF16), V((n_dev,) + vec.shape, F32), V((vec.shape[0], width), F32),
                        V((bup.shape[0], ff), F32),
                        V((n_layers, width, 3 * loc_w), BF16), V((n_layers, width, ff), BF16),
                        V((n_layers, num_tx, ff, col_w), BF16), V((2, width, col_w), BF16),
                        V((n_chip, blk, width), BF16), V((n_row, width), BF16), V((n_row, width), BF16),
                        V((n_chip, loc_heads, 3, blk, head_w), BF16), V((2, n_tok, head_w), BF16), V((n_q * blk, head_w), BF16),
                        V((n_q, blk, head_w), BF16), V((n_row, width), BF16), V((n_chip, blk, ff), BF16),
                        V((n_chip, blk, width), F32), V((n_chip, n_row, width), F32),
                        V((2, n_row, half_w), F32), V((4, n_row, half_w), F32),
                        dma((2,)), dma((2,)), dma((2,)), dma((2,)), dma((2, RG)), dma((2, RG)), dma((2, 3 * CG)), dma((2, CG)),
                        dma((2, RG)), dma((2, CG)), dma((2, CG)), dma((6,)), dma((2,)), dma((2, RS_SEMS)), dma((2,)), dma((2,))],
        compiler_params=pltpu.CompilerParams(collective_id=1, has_side_effects=True, vmem_limit_bytes=63 << 20),
        name="decoder",
    )(xt, vec, bup, wq, wk, wv, wo, wu, wd, bqkv, cos2, sin2, start)[:3]


def solution(mesh):
    num_tx = mesh.shape['tx']
    num_ty = mesh.shape['ty']
    width_spec = P('dp', ('tx', 'ty'))
    vec_spec = P(None, ('tx', 'ty'))
    proj_spec = P(None, 'tx', 'ty', None)
    head_spec = P(None, 'ty', None)
    cache_spec = P(None, ('dp', 'tx'), 'ty', None)
    in_specs = (width_spec, P('dp'), P('dp'), vec_spec, vec_spec, proj_spec, head_spec, proj_spec, head_spec,
                proj_spec, head_spec, P(None, 'ty', None, 'tx'), vec_spec, vec_spec, vec_spec,
                P(None, 'tx', 'ty'), P(None, ('ty', 'tx')), P(None, 'ty', 'tx'), vec_spec)
    out_specs = (width_spec, cache_spec, cache_spec)

    def device_fn(x_loc, seg_all, pos_all, ln1_gain, ln1_bias, w_q, b_q, w_k, b_k, w_v, b_v, w_o, b_o,
                  ln2_gain, ln2_bias, w_up, b_up, w_down, b_down):
        n_tok, piece_w = x_loc.shape
        tok_loc = n_tok // num_tx
        L, d_rows, loc_heads, head_dim = w_q.shape
        blk = 2 * tok_loc // num_ty
        core = lax.axis_index('ty') % 2
        q_start = lax.axis_index('tx') * tok_loc
        pos_q = lax.dynamic_slice_in_dim(pos_all, q_start, tok_loc, 0)
        inv_freq = jnp.exp(jnp.arange(head_dim // 2, dtype=F32) * (-2.0 * math.log(ROPE_THETA) / head_dim))
        angles = pos_q.astype(F32)[:, None] * inv_freq[None, :]
        cos_t, sin_t = jnp.cos(angles), jnp.sin(angles)
        cos2 = jnp.concatenate([cos_t, cos_t], axis=1)
        sin2 = jnp.concatenate([-sin_t, sin_t], axis=1)
        start = (jnp.arange(n_tok, dtype=jnp.int32) - pos_all).reshape(-1, 2, blk)
        start = lax.dynamic_index_in_dim(start, core, 1, keepdims=False).reshape(-1, 1)
        vec = jnp.concatenate([ln1_gain, ln1_bias, ln2_gain, ln2_bias, b_o, b_down], axis=0).astype(F32)
        vec = jnp.pad(vec, ((0, -vec.shape[0] % 8), (0, LANES - piece_w)))
        bup = jnp.pad(b_up.astype(F32), ((0, -L % 8), (0, 0)))
        bqkv = jnp.concatenate([b.reshape(L, -1) for b in (b_q, b_k, b_v)], axis=1).astype(F32)
        yt, k, v = decoder(num_tx, num_ty, x_loc.T, vec, bup, *[w.reshape(L, d_rows, -1) for w in (w_q, w_k, w_v)],
                           w_o.reshape(L, -1, w_o.shape[-1]), w_up, w_down, bqkv, cos2, sin2, start, head_dim)
        shape = (L, tok_loc, loc_heads, head_dim)
        return yt.T, k.reshape(shape), v.reshape(shape)

    return jax.shard_map(device_fn, mesh=mesh, in_specs=in_specs, out_specs=out_specs, check_vma=False)
```

```python
import math
import functools
import jax
import jax.numpy as jnp
from jax import lax
from jax.experimental import pallas as pl
from jax.experimental.pallas import tpu as pltpu
from jax.sharding import PartitionSpec as P

MESH = pl.DeviceIdType.MESH
F32 = jnp.float32
BF16 = jnp.bfloat16
ROPE_THETA = 100000.0
LOG2E = 1.4426950408889634
LANES = 128
BK = 1024


def rows_norm(x_f32, gain, bias):
    width = x_f32.shape[-1]
    mean = jnp.sum(x_f32, axis=-1, keepdims=True) / width
    var = jnp.sum(x_f32 * x_f32, axis=-1, keepdims=True) / width - mean * mean
    normed = (x_f32 - mean) * lax.rsqrt(var + 1e-5)
    return (normed * gain + bias).astype(BF16)


def gelu_tanh(x):
    return 0.5 * x * (1.0 + jnp.tanh(0.7978845608028654 * (x + 0.044715 * (x * x * x))))


def rows(at, n):
    return pl.ds(pl.multiple_of(at, n), n)


class Place:
    def __init__(self, num_tx, num_ty):
        self.num_tx, self.num_ty, self.n_chip = num_tx, num_ty, num_ty // 2
        self.y = lax.axis_index('tx')
        self.ty = lax.axis_index('ty')
        self.x = self.ty // 2
        self.c = lax.rem(self.ty, 2)
        self.me = self.y * num_ty + self.ty
        self.sib = self.at(self.y, self.x * 2 + 1 - self.c)
        self.right, self.left = self.beside(1), self.beside(self.n_chip - 1)
        self.above, self.below = self.over(1), self.over(num_tx - 1)

    def at(self, y, ty):
        return {'tx': y, 'ty': ty}

    def chip(self, k):
        return lax.rem(self.x + k, self.n_chip)

    def side(self, k):
        return lax.rem(self.y + k, self.num_tx)

    def beside(self, k):
        return self.at(self.y, self.chip(k) * 2 + self.c)

    def over(self, k):
        return self.at(self.side(k), self.ty)


def remote(src, dst, send_sem, recv_sem, to):
    return pltpu.make_async_remote_copy(src_ref=src, dst_ref=dst, send_sem=send_sem, recv_sem=recv_sem, device_id=to,
                                        device_id_type=MESH)


def copy_or_send(here, src, dst, send_sem, recv_sem, to):
    @pl.when(here)
    def _():
        pltpu.make_async_copy(src, dst, recv_sem).start()

    @pl.when(jnp.logical_not(here))
    def _():
        remote(src, dst, send_sem, recv_sem, to).start()


def took(ref, sem):
    pltpu.make_async_copy(ref, ref, sem).wait()


class RingGather:
    SEMS = 14

    def __init__(self, p, view, sems):
        self.p = p
        self.view = view
        self.sems = sems
        x, c, d = p.x, p.c, 1 - p.c
        far, left, right = p.chip(2), p.chip(p.n_chip - 1), p.chip(1)
        self.plan = [(x, 0, p.right, left), (x, 1, p.left, right), (x, 1, p.right, left), (x, 0, p.left, right),
                     (left, 0, p.right, far), (right, 1, p.left, far),
                     (x, 0, p.sib, x), (x, 1, p.sib, x), (left, 0, p.sib, left), (left, 1, p.sib, left),
                     (right, 0, p.sib, right), (right, 1, p.sib, right), (far, 0, p.sib, far), (far, 1, p.sib, far)]

    def out(self, i):
        chip, half, to, _ = self.plan[i]
        ref = self.view(chip, self.p.c, half)
        return remote(ref, ref, self.sems.at[0, i], self.sems.at[1, i], to)

    def arrived(self, i):
        _, half, to, chip = self.plan[i]
        core = self.p.c if i < 6 else 1 - self.p.c
        ref = self.view(chip, core, half)
        remote(ref, ref, self.sems.at[0, i], self.sems.at[1, i], to).wait_recv()

    def start(self):
        for i in (6, 7, 0, 1, 2, 3):
            self.out(i).start()

    def own(self):
        self.arrived(6)
        self.arrived(7)

    def relay(self):
        self.arrived(0)
        self.out(4).start()
        self.arrived(1)
        self.out(5).start()
        self.out(8).start()
        self.out(11).start()

    def near(self):
        self.arrived(2)
        self.out(9).start()
        self.arrived(3)
        self.out(10).start()

    def near_right(self):
        self.arrived(10)
        self.arrived(11)

    def near_left(self):
        self.arrived(8)
        self.arrived(9)

    def far(self):
        self.arrived(4)
        self.out(12).start()
        self.arrived(5)
        self.out(13).start()

    def far_done(self):
        self.arrived(12)
        self.arrived(13)

    def drain(self):
        for i in range(self.SEMS):
            self.out(i).wait_send()


class ColumnGather:
    SEMS = 8

    def __init__(self, p, pieces, sems):
        self.p = p
        self.pieces = pieces
        self.sems = sems

    def copy(self, n, i):
        p = self.p
        src, dst = self.pieces[n]
        up, down = p.side(1), p.side(p.num_tx - 1)
        half, to = ((0, p.above), (1, p.below), (1, p.above), (0, p.below), (0, p.above), (1, p.below))[i]
        here = src(half) if i < 4 else dst(down if i == 4 else up, half)
        there = dst((p.y, p.y, p.y, p.y, down, up)[i], half)
        return remote(here, there, self.sems.at[0, n * self.SEMS + i], self.sems.at[1, n * self.SEMS + i], to)

    def arrived(self, n, i):
        p = self.p
        src, dst = self.pieces[n]
        up, down, far = p.side(1), p.side(p.num_tx - 1), p.side(2)
        half, frm = ((0, down), (1, up), (1, down), (0, up), (0, far), (1, far))[i]
        remote(src(half), dst(frm, half), self.sems.at[0, n * self.SEMS + i], self.sems.at[1, n * self.SEMS + i],
               p.above).wait_recv()

    def own(self, n, half):
        src, dst = self.pieces[n]
        return pltpu.make_async_copy(src(half), dst(self.p.y, half), self.sems.at[1, n * self.SEMS + 6 + half])

    def start_first(self):
        for i in (0, 1):
            for n in range(len(self.pieces)):
                self.copy(n, i).start()

    def start_second(self):
        for i in (2, 3):
            for n in range(len(self.pieces)):
                self.copy(n, i).start()
        for n in range(len(self.pieces)):
            self.own(n, 0).start()
            self.own(n, 1).start()

    def start(self):
        self.start_first()
        self.start_second()

    def relay(self):
        for n in range(len(self.pieces)):
            self.arrived(n, 0)
            self.copy(n, 4).start()
            self.arrived(n, 1)
            self.copy(n, 5).start()

    def shard(self, k):
        for n in range(len(self.pieces)):
            if k == 0:
                self.own(n, 0).wait()
                self.own(n, 1).wait()
            elif k == 2:
                self.arrived(n, 4)
                self.arrived(n, 5)
            else:
                self.arrived(n, 3 if k == 1 else 2)

    def finish(self):
        for k in (0, 1, 3, 2):
            self.shard(k)

    def drain(self):
        for n in range(len(self.pieces)):
            for i in range(6):
                self.copy(n, i).wait_send()


S_DIRECT_R, S_DIRECT_L, S_FAR_R, S_FAR_L, S_SUM_R, S_SUM_L = range(6)


def decoder_kernel(num_tx, num_ty, n_layers,
                   xt_hbm, g1_ref, b1_ref, g2_ref, b2_ref, bo_ref, bd_ref, bup_ref, bq_ref, bk_ref, bv_ref, pos_ref,
                   wq_hbm, wk_hbm, wv_hbm, wo_hbm, wu_hbm, wd_hbm,
                   yt_hbm, kc_hbm, vc_hbm, go_hbm,
                   xt, vrow, vloc, vbuf, vec, bloc, bup, raw, ws, w, wu, wd, wo, cs, a_all, hid, st, cst, kv, vt, qh, ob, obuf,
                   g, full, sibin, far_in, fin,
                   x_sems, v_sems, b_sems, y_sems, a_sems, u_sems, wq_sems, wo_sems, wx_sems, wu_sems, wd_sems,
                   kv_sems, o_sems, p_sems, r_sems, l_sems, c_sems):
    p = Place(num_tx, num_ty)
    n_dev = num_tx * num_ty
    n_chip, x, y, c, ty = p.n_chip, p.x, p.y, p.c, p.ty
    n_row, width = hid.shape
    blk = 2 * n_row
    half_row = n_row // 2
    loc_heads, head_w = wq_hbm.shape[2], wq_hbm.shape[3]
    loc_w = loc_heads * head_w
    col_w = wd.shape[3]
    piece_w = xt_hbm.shape[0]
    last = n_chip - 1
    mine, other = rows(c * n_row, n_row), rows((1 - c) * n_row, n_row)

    barrier = pltpu.get_barrier_semaphore()
    ids = [lax.rem(p.me + k, n_dev) for k in range(1, n_dev)]
    devs = [p.at(d // num_ty, lax.rem(d, num_ty)) for d in ids]
    for to in devs:
        pl.semaphore_signal(barrier, inc=1, device_id=to, device_id_type=MESH)

    def load_raw(l):
        return [pltpu.make_async_copy(src.at[l], raw.at[i], l_sems.at[i]) for i, src in enumerate((wq_hbm, wk_hbm, wv_hbm))]

    def flatten(l):
        for i, ld in enumerate(load_raw(l)):
            ld.wait()
            ws[l, i] = raw[i].reshape(ws.shape[2], loc_w)
    for ld in load_raw(0):
        ld.start()
    vrow[...] = jnp.zeros_like(vrow)
    for i, ref in enumerate((g1_ref, b1_ref, g2_ref, b2_ref, bo_ref, bd_ref)):
        vrow[i * n_layers:(i + 1) * n_layers, :piece_w] = ref[...].astype(F32)
    vloc[...] = vrow[...].astype(BF16)
    bloc[...] = jnp.zeros_like(bloc)
    bloc[:n_layers, :] = bup_ref[...].astype(F32)
    flatten(0)
    pl.semaphore_wait(barrier, n_dev - 1)

    def halves(ref, l, n):
        return lambda h: ref.at[l, pl.ds(h * n, n)]

    def shard_rows(dst, l, n_shard, n, cols):
        return lambda ys, h: dst.at[l, rows(ys * n_shard + h * n, n), cols]

    qkv_rows = ws.shape[2]
    up_rows = wu_hbm.shape[1]
    down_rows = wd_hbm.shape[1]
    o_rows = wo_hbm.shape[1]

    def gather_qkv(l):
        n = qkv_rows // 2
        return ColumnGather(p, [((lambda h, i=i: ws.at[l, i, pl.ds(h * n, n)]),
                                 shard_rows(w, l, qkv_rows, n, pl.ds(i * loc_w, loc_w))) for i in range(3)], wq_sems)

    def gather_up(l):
        n = up_rows // 2
        return ColumnGather(p, [(halves(wu_hbm, l, n), shard_rows(wu, l, up_rows, n, slice(None)))], wu_sems)

    def gather_down(l):
        n = down_rows // 2
        return ColumnGather(p, [(halves(wd_hbm, l, n), lambda ys, h: wd.at[l, ys, pl.ds(h * n, n)])], wd_sems)

    def gather_o(l):
        n = o_rows // 2
        return ColumnGather(p, [(halves(wo_hbm, l, n), lambda ys, h: go_hbm.at[l, ys, rows(ty * o_rows + h * n, n)])], wo_sems)

    def spread_o(l):
        n = num_tx // 2
        return RingGather(p, lambda chip, core, h: go_hbm.at[l, pl.ds(h * n, n), rows((chip * 2 + core) * o_rows, o_rows)],
                          wx_sems)

    g_qkv = [gather_qkv(l) for l in range(n_layers)]
    g_up = [gather_up(l) for l in range(n_layers)]
    g_down = [gather_down(l) for l in range(n_layers)]
    g_o = [gather_o(l) for l in range(n_layers)]
    s_o = [spread_o(l) for l in range(n_layers)]

    for d, to in zip(ids, devs):
        remote(xt_hbm.at[:, rows(d * n_row, n_row)], xt.at[rows(p.me * piece_w, piece_w)], x_sems.at[0], x_sems.at[1], to).start()
        remote(vloc, vbuf.at[p.me], v_sems.at[0], v_sems.at[1], to).start()
    g_qkv[0].start()
    pltpu.make_async_copy(xt_hbm.at[:, rows(p.me * n_row, n_row)], xt.at[rows(p.me * piece_w, piece_w)], x_sems.at[1]).start()
    pltpu.make_async_copy(vloc, vbuf.at[p.me], v_sems.at[1]).start()
    bup_w = bup_ref.shape[1]
    for k in range(1, num_tx):
        remote(bloc, bup.at[:, rows(y * bup_w, bup_w)], b_sems.at[0], b_sems.at[1], p.over(k)).start()
    pltpu.make_async_copy(bloc, bup.at[:, rows(y * bup_w, bup_w)], b_sems.at[1]).start()
    for l in range(1, n_layers):
        for ld in load_raw(l):
            ld.start()
        flatten(l)

    lane = lax.broadcasted_iota(jnp.int32, (1, head_w), 1)
    inv_freq = jnp.exp(lax.rem(lane, head_w // 2).astype(F32) * (-2.0 * math.log(ROPE_THETA) / head_w))
    sign = jnp.where(lane < head_w // 2, -1.0, 1.0)

    def angles(k, carry):
        pos = pos_ref[pl.ds(y * n_chip + k, 1), :].astype(F32)
        ang = jnp.broadcast_to(pos, (head_w, blk)).T * inv_freq
        cs[0, rows(k * blk, blk), :] = jnp.cos(ang)
        cs[1, rows(k * blk, blk), :] = jnp.sin(ang) * sign
        return carry
    lax.fori_loop(0, n_chip, angles, 0)
    took(vbuf, v_sems.at[1])
    per = LANES // piece_w
    for j in range(width // LANES):
        vec[:, j * LANES:(j + 1) * LANES] = jnp.concatenate(
            [vbuf[per * j + i][:, :piece_w].astype(F32) for i in range(per)], axis=1)
    took(xt, x_sems.at[1])

    def turn(j, carry):
        hid[:, rows(j * LANES, LANES)] = xt[rows(j * LANES, LANES), :].T
        return carry
    lax.fori_loop(0, width // LANES, turn, 0)

    def vector(i, l):
        return vec[i * n_layers + l:i * n_layers + l + 1, :]

    def row_gather(sems):
        return RingGather(p, lambda chip, core, h: a_all.at[chip, rows(core * n_row + h * half_row, half_row)], sems)

    def order(n):
        return n + n // 2 - 2 * (n // 3)

    def each(n_from, n_to, body, hooks):
        def step(n, carry):
            for at_n, hook in hooks.items():
                @pl.when(n == at_n)
                def _():
                    for h in hook:
                        h()
            body(order(n))
            return carry
        lax.fori_loop(n_from, n_to, step, 0)

    def project(l, k):
        slot = p.chip(k)
        at_row = rows(slot * blk, blk)
        acc = jnp.dot(a_all[slot], w[l], preferred_element_type=F32)
        cos_t, sin_t = cs[0, at_row, :], cs[1, at_row, :]
        for i, bias in enumerate((bq_ref, bk_ref, bv_ref)):
            parts = []
            for h in range(loc_heads):
                lo = i * loc_w + h * head_w
                v = acc[:, lo:lo + head_w] + bias[l, h:h + 1, :].astype(F32)
                if i < 2:
                    v = v * cos_t + pltpu.roll(v, head_w // 2, 1) * sin_t
                parts.append(v.astype(BF16))
                st[k, h, i] = parts[-1]
            if i > 0:
                cst[k, i - 1] = jnp.concatenate(parts, axis=1).reshape(blk, loc_heads, head_w)
        at_tok = rows((y * n_chip + slot) * blk, blk)
        par = lax.rem(slot, 2)
        at_q = rows((y * (n_chip // 2) + slot // 2) * blk, blk)
        for h in range(loc_heads):
            yd = c * loc_heads + h
            for r in range(2):
                copy_or_send(jnp.logical_and(yd == y, c == r), st.at[k, h, 1 + r], kv.at[r, at_tok], kv_sems.at[0],
                             kv_sems.at[1], p.at(yd, x * 2 + r))
            copy_or_send(jnp.logical_and(yd == y, c == par), st.at[k, h, 0], qh.at[at_q], kv_sems.at[2], kv_sems.at[3],
                         p.at(yd, x * 2 + par))
        pltpu.make_async_copy(cst.at[k, 0], kc_hbm.at[l, at_row], c_sems.at[0]).start()
        pltpu.make_async_copy(cst.at[k, 1], vc_hbm.at[l, at_row], c_sems.at[1]).start()

    n_q = ob.shape[0]
    q_grp = 2 * blk
    n_grp = n_q * blk // q_grp
    n_sub = BK // blk

    def attend(hooks):
        def step(n, carry):
            grp = n_grp - 1 - n
            q = qh[rows(grp * q_grp, q_grp), :]
            q_col = lax.broadcasted_iota(jnp.int32, (1, blk), 1)
            at_q = [(2 * (2 * grp + i) + c) for i in range(2)]
            q_pos = jnp.concatenate([q_col + b * blk for b in at_q], axis=1)
            first = q_pos - jnp.concatenate([pos_ref[pl.ds(b, 1), :] for b in at_q], axis=1)
            key = lax.broadcasted_iota(jnp.int32, (blk, q_grp), 0)

            def score(j, m, diag):
                s = lax.dot_general(kv[0, rows(j * BK, BK), :], q, (((1,), (1,)), ((), ())),
                                    preferred_element_type=F32) * head_w ** -0.5
                for i in range(n_sub):
                    k_pos = key + (j * BK + i * blk)
                    ok = k_pos >= first
                    if diag:
                        ok = jnp.logical_and(ok, k_pos <= q_pos)
                    part = jnp.where(ok, s[i * blk:(i + 1) * blk], -1e30)
                    full[j, :, i * q_grp:(i + 1) * q_grp] = part
                    m = jnp.maximum(m, jnp.max(part.reshape(blk // 8, 8, q_grp), axis=0))
                return m
            m = lax.fori_loop(0, grp, lambda j, m: score(j, m, False), jnp.full((8, q_grp), -1e30, F32))
            m = jnp.max(score(grp, m, True), axis=0, keepdims=True)

            def expo(j, t):
                for i in range(n_sub):
                    e = jnp.exp(full[j, :, i * q_grp:(i + 1) * q_grp] - m)
                    full[j, :, i * q_grp:(i + 1) * q_grp] = e
                    t = t + jnp.sum(e.reshape(blk // 8, 8, q_grp), axis=0)
                return t
            t = lax.fori_loop(0, grp + 1, expo, jnp.zeros((8, q_grp), F32))
            inv = 1.0 / jnp.sum(t, axis=0, keepdims=True)

            def apply(j, acc):
                prob = jnp.concatenate([(full[j, :, i * q_grp:(i + 1) * q_grp] * inv).astype(BF16) for i in range(n_sub)], axis=0)
                return acc + jnp.dot(vt[:, rows(j * BK, BK)], prob, preferred_element_type=F32)
            out = lax.fori_loop(0, grp + 1, apply, jnp.zeros((head_w, q_grp), F32)).T.astype(BF16)
            cols_o = rows((x * num_tx + y) * head_w, head_w)
            for i, b in enumerate(at_q):
                ob[2 * grp + i] = out[i * blk:(i + 1) * blk]
                yt, xd = b // n_chip, lax.rem(b, n_chip)
                for r in range(2):
                    here = jnp.logical_and(jnp.logical_and(yt == y, xd == x), c == r)
                    copy_or_send(here, ob.at[2 * grp + i, pl.ds(r * n_row, n_row)], obuf.at[:, cols_o], o_sems.at[0],
                                 o_sems.at[1], p.at(yt, xd * 2 + r))
            for at_n, hook in hooks.items():
                @pl.when(n == at_n)
                def _():
                    for h in hook:
                        h()
            return carry
        lax.fori_loop(0, n_grp, step, 0)

    def up(l, k):
        slot = p.chip(k)

        def part(n, carry):
            cc = rows(n * 512, 512)
            h = jnp.dot(a_all[slot], wu[l, :, cc], preferred_element_type=F32) + bup[l:l + 1, cc]
            g[k, :, cc] = gelu_tanh(h).astype(BF16)
            return carry
        lax.fori_loop(0, wu.shape[2] // 512, part, 0)

    blocks = (0, 1, last, 2)
    cols = [rows(p.side(k) * col_w, col_w) for k in blocks]
    top, bottom = rows(c * n_row, half_row), rows(c * n_row + half_row, half_row)

    def to_sibling(k, j):
        i = k * num_tx + j
        return remote(full.at[k, other, cols[j]], sibin.at[k, :, cols[j]], p_sems.at[0, i], p_sems.at[1, i], p.sib)

    def rs(kind, j):
        k, part, dst, to = ((1, bottom, fin.at[0], p.right), (last, top, fin.at[1], p.left), (2, top, far_in.at[0], p.right),
                            (2, bottom, far_in.at[1], p.left), (1, top, fin.at[2], p.right),
                            (last, bottom, fin.at[3], p.left))[kind]
        i = kind * num_tx + j
        return remote(full.at[k, part, cols[j]], dst.at[:, cols[j]], r_sems.at[0, i], r_sems.at[1, i], to)

    def partials(l, j):
        def part(n, carry):
            k = order(lax.rem(n + 1, n_chip))
            full[k, :, cols[j]] = jnp.dot(g[k], wd[l, p.side(blocks[j])], preferred_element_type=F32)
            to_sibling(k, j).start()
            return carry
        lax.fori_loop(0, n_chip, part, 0)

    def pair_sum(k, j):
        to_sibling(k, j).wait_recv()
        full[k, mine, cols[j]] = full[k, mine, cols[j]] + sibin[k, :, cols[j]]

    def send_partials(j):
        pair_sum(1, j)
        rs(S_DIRECT_R, j).start()
        pair_sum(last, j)
        rs(S_DIRECT_L, j).start()
        pair_sum(2, j)
        rs(S_FAR_R, j).start()
        rs(S_FAR_L, j).start()
        pair_sum(0, j)

    def pass_on(j):
        rs(S_FAR_R, j).wait_recv()
        full[1, top, cols[j]] = full[1, top, cols[j]] + far_in[0, :, cols[j]]
        rs(S_SUM_R, j).start()
        rs(S_FAR_L, j).wait_recv()
        full[last, bottom, cols[j]] = full[last, bottom, cols[j]] + far_in[1, :, cols[j]]
        rs(S_SUM_L, j).start()

    def complete(l, j):
        cc = cols[j]
        bias = vec[5 * n_layers + l:5 * n_layers + l + 1, cc]
        for kind in (S_DIRECT_R, S_DIRECT_L, S_SUM_R, S_SUM_L):
            rs(kind, j).wait_recv()
        for part, out, ins in ((top, pl.ds(0, half_row), (1, 2)), (bottom, pl.ds(half_row, half_row), (0, 3))):
            tot = full[0, part, cc] + fin[ins[0], :, cc] + fin[ins[1], :, cc]
            hid[out, cc] = (hid[out, cc].astype(F32) + tot + bias).astype(BF16)

    def give_back(j):
        row = p.side(blocks[j])

        def turn_back(n, carry):
            at_c = rows(row * col_w + n * LANES, LANES)
            xt[at_c, :] = hid[:, at_c].T
            return carry
        lax.fori_loop(0, col_w // LANES, turn_back, 0)
        for k in range(num_ty):
            to_ty = lax.rem(ty + k, num_ty)
            copy_or_send(jnp.logical_and(row == y, k == 0), xt.at[rows((row * num_ty + to_ty) * piece_w, piece_w)],
                         yt_hbm.at[:, rows(p.me * n_row, n_row)], y_sems.at[0], y_sems.at[1], p.at(row, to_ty))

    for l in range(n_layers):
        first_layer, last_layer = l == 0, l == n_layers - 1
        a_all[x, mine, :] = rows_norm(hid[...].astype(F32), vector(0, l), vector(1, l))
        ga = row_gather(a_sems)
        ga.start()
        if first_layer:
            g_qkv[l].relay()
            g_o[l].start()
            ga.relay()
            ga.own()
            ga.near()
            ga.near_right()
            ga.near_left()
            ga.far()
            ga.far_done()
            ga.drain()
            g_qkv[l].finish()
            each(0, n_chip, lambda k: project(l, k), {1: [g_o[l].relay]})
        else:
            ga.relay()
            ga.own()
            g_qkv[l].finish()
            each(0, last, lambda k: project(l, k), {1: [ga.near, ga.near_right, ga.near_left, g_o[l].relay]})
            ga.far()
            ga.far_done()
            ga.drain()
            project(l, 2)
        g_up[l].start_first()
        g_o[l].finish()
        s_o[l].start()
        role = kv.at[c]
        took(role, kv_sems.at[1])
        forward = remote(role, role, kv_sems.at[4], kv_sems.at[5], p.sib)
        forward.start()
        s_o[l].relay()
        took(qh, kv_sems.at[3])
        remote(kv.at[1 - c], kv.at[1 - c], kv_sems.at[4], kv_sems.at[5], p.sib).wait_recv()
        forward.wait_send()

        def turn_v(n, carry):
            vt[:, rows(n * LANES, LANES)] = kv[1, rows(n * LANES, LANES), :].T
            return carry
        lax.fori_loop(0, vt.shape[1] // LANES, turn_v, 0)
        attend({1: [s_o[l].near]})
        g_up[l].start_second()
        g_up[l].relay()
        g_down[l].start()
        s_o[l].far()
        s_o[l].own()
        s_o[l].near_right()
        s_o[l].near_left()
        s_o[l].far_done()
        n_step = wo.shape[2]
        per_col = col_w // n_step

        def load_o(t):
            return pltpu.make_async_copy(go_hbm.at[l, t // per_col, :, rows(lax.rem(t, per_col) * n_step, n_step)],
                                         wo.at[lax.rem(t, 2)], l_sems.at[lax.rem(t, 2)])
        load_o(0).start()
        load_o(1).start()
        took(obuf, o_sems.at[1])

        def out_product(t, carry):
            load_o(t).wait()
            cc = rows(t * n_step, n_step)
            bias = vec[4 * n_layers + l:4 * n_layers + l + 1, cc]
            hid[:, cc] = (hid[:, cc].astype(F32) + jnp.dot(obuf[...], wo[lax.rem(t, 2)], preferred_element_type=F32)
                          + bias).astype(BF16)

            @pl.when(t + 2 < width // n_step)
            def _():
                load_o(t + 2).start()
            return carry
        lax.fori_loop(0, width // n_step, out_product, 0)
        a_all[x, mine, :] = rows_norm(hid[...].astype(F32), vector(2, l), vector(3, l))
        gu = row_gather(u_sems)
        gu.start()
        if first_layer:
            took(bup, b_sems.at[1])
        gu.own()
        gu.relay()
        g_up[l].finish()
        each(0, n_chip, lambda k: up(l, k), {1: [gu.near, gu.near_right, gu.near_left], last: [gu.far, gu.far_done]})
        gu.drain()
        g_down[l].relay()
        if not last_layer:
            g_qkv[l].drain()
            g_o[l].drain()
            g_qkv[l + 1].start()
        for j in range(num_tx):
            if j == num_tx - 1:
                pass_on(j - 1)
            g_down[l].shard(blocks[j])
            partials(l, j)
            send_partials(j)
            if 0 < j < num_tx - 1:
                pass_on(j - 1)
            if j > 1:
                complete(l, j - 2)
                if last_layer:
                    give_back(j - 2)
        if not last_layer:
            g_qkv[l + 1].relay()
            g_o[l + 1].start()
        pass_on(num_tx - 1)
        for j in range(num_tx - 2, num_tx):
            complete(l, j)
            if last_layer:
                give_back(j)
        for j in range(num_tx):
            for k in range(n_chip):
                to_sibling(k, j).wait_send()
            for kind in range(6):
                rs(kind, j).wait_send()
        s_o[l].drain()
        g_up[l].drain()
        g_down[l].drain()
        if last_layer:
            g_qkv[l].drain()
            g_o[l].drain()
        sent_away(p, kv, qh, kv_sems, loc_heads)
        o_away(p, obuf, o_sems, head_w)
        took(kc_hbm.at[l], c_sems.at[0])
        took(vc_hbm.at[l], c_sems.at[1])

    took(xt_hbm.at[:, pl.ds(0, (n_dev - 1) * n_row)], x_sems.at[0])
    took(vbuf.at[pl.ds(0, n_dev - 1)], v_sems.at[0])
    took(bup.at[:, pl.ds(0, (num_tx - 1) * bup_w)], b_sems.at[0])
    took(yt_hbm, y_sems.at[1])
    took(xt.at[pl.ds(0, (n_dev - 1) * piece_w)], y_sems.at[0])


def sent_away(p, kv, qh, kv_sems, loc_heads):
    stays = p.c == p.y // loc_heads
    n_tok = kv.shape[1]
    n_q = qh.shape[0]

    @pl.when(stays)
    def _():
        took(kv.at[0, pl.ds(0, n_tok * 3 // 4)], kv_sems.at[0])
        took(qh.at[pl.ds(0, n_q * 3 // 4)], kv_sems.at[2])

    @pl.when(jnp.logical_not(stays))
    def _():
        took(kv.at[0], kv_sems.at[0])
        took(qh, kv_sems.at[2])


def o_away(p, obuf, o_sems, head_w):
    stays = lax.rem(p.x, 2) == p.c

    @pl.when(stays)
    def _():
        took(obuf.at[:, pl.ds(0, obuf.shape[1] - head_w)], o_sems.at[0])

    @pl.when(jnp.logical_not(stays))
    def _():
        took(obuf, o_sems.at[0])


def decoder(num_tx, num_ty, xt, vectors, b_up, b_qkv, pos, wq, wk, wv, wo, wu, wd):
    n_layers, d_rows, loc_heads, head_w = wq.shape
    n_dev = num_tx * num_ty
    n_chip = num_ty // 2
    piece_w, n_tok = xt.shape
    width = piece_w * n_dev
    n_row = n_tok // n_dev
    blk = 2 * n_row
    loc_w = loc_heads * head_w
    tok_loc = n_tok // num_tx
    ff = wu.shape[2]
    col_w = wd.shape[2]
    n_q = n_tok // (2 * blk)
    n_vec = -(-len(vectors) * n_layers // 16) * 16
    vm = pl.BlockSpec(memory_space=pltpu.VMEM)
    hb = pl.BlockSpec(memory_space=pl.ANY)
    V = pltpu.VMEM
    dma = pltpu.SemaphoreType.DMA
    cache = jax.ShapeDtypeStruct((n_layers, tok_loc, loc_heads, head_w), BF16)
    go = jax.ShapeDtypeStruct((n_layers, num_tx, wo.shape[1] * num_ty, col_w), BF16)
    CG, RG = ColumnGather.SEMS, RingGather.SEMS
    return pl.pallas_call(
        functools.partial(decoder_kernel, num_tx, num_ty, n_layers),
        out_shape=(jax.ShapeDtypeStruct((piece_w, n_tok), BF16), cache, cache, go),
        in_specs=[hb] + [vm] * 11 + [hb] * 6,
        out_specs=(hb,) * 4,
        scratch_shapes=[V((width, n_row), BF16), V((n_vec, LANES), F32), V((n_vec, LANES), BF16), V((n_dev, n_vec, LANES), BF16),
                        V((n_vec, width), F32), V((8, b_up.shape[1]), F32), V((8, ff), F32),
                        V((3, d_rows, loc_heads, head_w), BF16), V((n_layers, 3, d_rows, loc_w), BF16),
                        V((n_layers, width, 3 * loc_w), BF16), V((n_layers, width, ff), BF16),
                        V((n_layers, num_tx, ff, col_w), BF16), V((2, width, col_w // 2), BF16),
                        V((2, tok_loc, head_w), F32),
                        V((n_chip, blk, width), BF16), V((n_row, width), BF16),
                        V((n_chip, loc_heads, 3, blk, head_w), BF16), V((n_chip, 2, blk, loc_heads, head_w), BF16),
                        V((2, n_tok, head_w), BF16), V((head_w, n_tok), BF16), V((n_q * blk, head_w), BF16),
                        V((n_q, blk, head_w), BF16), V((n_row, width), BF16), V((n_chip, blk, ff), BF16),
                        V((n_chip, blk, width), F32), V((n_chip, n_row, width), F32),
                        V((2, n_row // 2, width), F32), V((4, n_row // 2, width), F32),
                        dma((2,)), dma((2,)), dma((2,)), dma((2,)), dma((2, RG)), dma((2, RG)), dma((2, 3 * CG)), dma((2, CG)),
                        dma((2, RG)), dma((2, CG)), dma((2, CG)), dma((6,)), dma((2,)), dma((2, n_chip * num_tx)),
                        dma((2, 6 * num_tx)), dma((3,)), dma((2,))],
        compiler_params=pltpu.CompilerParams(collective_id=1, has_side_effects=True, vmem_limit_bytes=63 << 20),
        name="decoder",
    )(xt, *vectors, b_up, *b_qkv, pos, wq, wk, wv, wo, wu, wd)[:3]


def solution(mesh):
    num_tx = mesh.shape['tx']
    num_ty = mesh.shape['ty']
    width_spec = P('dp', ('tx', 'ty'))
    vec_spec = P(None, ('tx', 'ty'))
    proj_spec = P(None, 'tx', 'ty', None)
    head_spec = P(None, 'ty', None)
    cache_spec = P(None, ('dp', 'tx'), 'ty', None)
    in_specs = (width_spec, P('dp'), P('dp'), vec_spec, vec_spec, proj_spec, head_spec, proj_spec, head_spec,
                proj_spec, head_spec, P(None, 'ty', None, 'tx'), vec_spec, vec_spec, vec_spec,
                P(None, 'tx', 'ty'), P(None, ('ty', 'tx')), P(None, 'ty', 'tx'), vec_spec)
    out_specs = (width_spec, cache_spec, cache_spec)

    def device_fn(x_loc, seg_all, pos_all, ln1_gain, ln1_bias, w_q, b_q, w_k, b_k, w_v, b_v, w_o, b_o,
                  ln2_gain, ln2_bias, w_up, b_up, w_down, b_down):
        n_tok = x_loc.shape[0]
        blk = 2 * n_tok // (num_tx * num_ty)
        yt, k, v = decoder(num_tx, num_ty, x_loc.T, (ln1_gain, ln1_bias, ln2_gain, ln2_bias, b_o, b_down), b_up,
                           (b_q, b_k, b_v), pos_all.reshape(-1, blk), w_q, w_k, w_v,
                           w_o.reshape(w_o.shape[0], -1, w_o.shape[-1]), w_up, w_down)
        return yt.T, k, v

    return jax.shard_map(device_fn, mesh=mesh, in_specs=in_specs, out_specs=out_specs, check_vma=False)
```

```python
import math
import functools
import jax
import jax.numpy as jnp
from jax import lax
from jax.experimental import pallas as pl
from jax.experimental.pallas import tpu as pltpu
from jax.sharding import PartitionSpec as P

MESH = pl.DeviceIdType.MESH
F32 = jnp.float32
BF16 = jnp.bfloat16
ROPE_THETA = 100000.0
LOG2E = 1.4426950408889634
LANES = 128
BK = 1024


def rows_norm(x_f32, gain, bias):
    width = x_f32.shape[-1]
    mean = jnp.sum(x_f32, axis=-1, keepdims=True) / width
    var = jnp.sum(x_f32 * x_f32, axis=-1, keepdims=True) / width - mean * mean
    normed = (x_f32 - mean) * lax.rsqrt(var + 1e-5)
    return (normed * gain + bias).astype(BF16)


def gelu_tanh(x):
    return 0.5 * x * (1.0 + jnp.tanh(0.7978845608028654 * (x + 0.044715 * (x * x * x))))


def rows(at, n):
    return pl.ds(pl.multiple_of(at, n), n)


class Place:
    def __init__(self, num_tx, num_ty):
        self.num_tx, self.num_ty, self.n_chip = num_tx, num_ty, num_ty // 2
        self.y = lax.axis_index('tx')
        self.ty = lax.axis_index('ty')
        self.x = self.ty // 2
        self.c = lax.rem(self.ty, 2)
        self.me = self.y * num_ty + self.ty
        self.sib = self.at(self.y, self.x * 2 + 1 - self.c)
        self.right, self.left = self.beside(1), self.beside(self.n_chip - 1)
        self.above, self.below = self.over(1), self.over(num_tx - 1)

    def at(self, y, ty):
        return {'tx': y, 'ty': ty}

    def chip(self, k):
        return lax.rem(self.x + k, self.n_chip)

    def side(self, k):
        return lax.rem(self.y + k, self.num_tx)

    def beside(self, k):
        return self.at(self.y, self.chip(k) * 2 + self.c)

    def over(self, k):
        return self.at(self.side(k), self.ty)


def remote(src, dst, send_sem, recv_sem, to):
    return pltpu.make_async_remote_copy(src_ref=src, dst_ref=dst, send_sem=send_sem, recv_sem=recv_sem, device_id=to,
                                        device_id_type=MESH)


def copy_or_send(here, src, dst, send_sem, recv_sem, to):
    @pl.when(here)
    def _():
        pltpu.make_async_copy(src, dst, recv_sem).start()

    @pl.when(jnp.logical_not(here))
    def _():
        remote(src, dst, send_sem, recv_sem, to).start()


def took(ref, sem):
    pltpu.make_async_copy(ref, ref, sem).wait()


class RingGather:
    SEMS = 14

    def __init__(self, p, view, sems):
        self.p = p
        self.view = view
        self.sems = sems
        x, c, d = p.x, p.c, 1 - p.c
        far, left, right = p.chip(2), p.chip(p.n_chip - 1), p.chip(1)
        self.plan = [(x, 0, p.right, left), (x, 1, p.left, right), (x, 1, p.right, left), (x, 0, p.left, right),
                     (left, 0, p.right, far), (right, 1, p.left, far),
                     (x, 0, p.sib, x), (x, 1, p.sib, x), (left, 0, p.sib, left), (left, 1, p.sib, left),
                     (right, 0, p.sib, right), (right, 1, p.sib, right), (far, 0, p.sib, far), (far, 1, p.sib, far)]

    def out(self, i):
        chip, half, to, _ = self.plan[i]
        ref = self.view(chip, self.p.c, half)
        return remote(ref, ref, self.sems.at[0, i], self.sems.at[1, i], to)

    def arrived(self, i):
        _, half, to, chip = self.plan[i]
        core = self.p.c if i < 6 else 1 - self.p.c
        ref = self.view(chip, core, half)
        remote(ref, ref, self.sems.at[0, i], self.sems.at[1, i], to).wait_recv()

    def start(self):
        for i in (6, 7, 0, 1, 2, 3):
            self.out(i).start()

    def own(self):
        self.arrived(6)
        self.arrived(7)

    def relay(self):
        self.arrived(0)
        self.out(4).start()
        self.arrived(1)
        self.out(5).start()
        self.out(8).start()
        self.out(11).start()

    def near(self):
        self.arrived(2)
        self.out(9).start()
        self.arrived(3)
        self.out(10).start()

    def near_right(self):
        self.arrived(10)
        self.arrived(11)

    def near_left(self):
        self.arrived(8)
        self.arrived(9)

    def far(self):
        self.arrived(4)
        self.out(12).start()
        self.arrived(5)
        self.out(13).start()

    def far_done(self):
        self.arrived(12)
        self.arrived(13)

    def drain(self):
        for i in range(self.SEMS):
            self.out(i).wait_send()


class ColumnGather:
    SEMS = 8

    def __init__(self, p, pieces, sems, early=0):
        self.p = p
        self.pieces = pieces
        self.sems = sems
        self.early = early

    def copy(self, n, i):
        p = self.p
        src, dst = self.pieces[n]
        up, down = p.side(1), p.side(p.num_tx - 1)
        half, to = ((0, p.above), (1, p.below), (1, p.above), (0, p.below), (0, p.above), (1, p.below))[i]
        here = src(half) if i < 4 else dst(down if i == 4 else up, half)
        there = dst((p.y, p.y, p.y, p.y, down, up)[i], half)
        return remote(here, there, self.sems.at[0, n * self.SEMS + i], self.sems.at[1, n * self.SEMS + i], to)

    def arrived(self, n, i):
        p = self.p
        src, dst = self.pieces[n]
        up, down, far = p.side(1), p.side(p.num_tx - 1), p.side(2)
        half, frm = ((0, down), (1, up), (1, down), (0, up), (0, far), (1, far))[i]
        remote(src(half), dst(frm, half), self.sems.at[0, n * self.SEMS + i], self.sems.at[1, n * self.SEMS + i],
               p.above).wait_recv()

    def own(self, n, half):
        src, dst = self.pieces[n]
        return pltpu.make_async_copy(src(half), dst(self.p.y, half), self.sems.at[1, n * self.SEMS + 6 + half])

    def start_first(self):
        for i in (0, 1):
            for n in range(len(self.pieces)):
                self.copy(n, i).start()
        self.rest(range(self.early))

    def start_second(self):
        self.rest(range(self.early, len(self.pieces)))

    def rest(self, which):
        for i in (2, 3):
            for n in which:
                self.copy(n, i).start()
        for n in which:
            self.own(n, 0).start()
            self.own(n, 1).start()

    def start(self):
        self.start_first()
        self.start_second()

    def relay(self):
        for n in range(len(self.pieces)):
            self.arrived(n, 0)
            self.copy(n, 4).start()
            self.arrived(n, 1)
            self.copy(n, 5).start()

    def shard(self, k):
        for n in range(len(self.pieces)):
            if k == 0:
                self.own(n, 0).wait()
                self.own(n, 1).wait()
            elif k == 2:
                self.arrived(n, 4)
                self.arrived(n, 5)
            else:
                self.arrived(n, 3 if k == 1 else 2)

    def finish(self):
        for k in (0, 1, 3, 2):
            self.shard(k)

    def drain(self):
        for n in range(len(self.pieces)):
            for i in range(6):
                self.copy(n, i).wait_send()


S_DIRECT_R, S_DIRECT_L, S_FAR_R, S_FAR_L, S_SUM_R, S_SUM_L = range(6)


def decoder_kernel(num_tx, num_ty, n_layers,
                   xt_hbm, g1_ref, b1_ref, g2_ref, b2_ref, bo_ref, bd_ref, bup_ref, bq_ref, bk_ref, bv_ref, pos_ref,
                   wq_hbm, wk_hbm, wv_hbm, wo_hbm, wu_hbm, wd_hbm,
                   yt_ref, kc_ref, vc_ref,
                   xt, vrow, vloc, vbuf, vec, bloc, bup, raw, ws, w, wu, wd, wo, cs, a_all, hid, st, sv, kt, vt, qh, ob, obuf,
                   g, full, sibin, far_in, fin,
                   x_sems, v_sems, b_sems, y_sems, a_sems, u_sems, wq_sems, wo_sems, wx_sems, wu_sems, wd_sems,
                   kv_sems, o_sems, p_sems, r_sems, l_sems):
    p = Place(num_tx, num_ty)
    n_dev = num_tx * num_ty
    n_chip, x, y, c, ty = p.n_chip, p.x, p.y, p.c, p.ty
    n_row, width = hid.shape
    blk = 2 * n_row
    half_row = n_row // 2
    loc_heads, head_w = wq_hbm.shape[2], wq_hbm.shape[3]
    loc_w = loc_heads * head_w
    col_w = wd.shape[2]
    piece_w = xt_hbm.shape[0]
    last = n_chip - 1
    mine, other = rows(c * n_row, n_row), rows((1 - c) * n_row, n_row)

    barrier = pltpu.get_barrier_semaphore()
    ids = [lax.rem(p.me + k, n_dev) for k in range(1, n_dev)]
    devs = [p.at(d // num_ty, lax.rem(d, num_ty)) for d in ids]
    for to in devs:
        pl.semaphore_signal(barrier, inc=1, device_id=to, device_id_type=MESH)

    def load_raw(l):
        return [pltpu.make_async_copy(src.at[l], raw.at[i], l_sems.at[i]) for i, src in enumerate((wq_hbm, wk_hbm, wv_hbm))]

    def flatten(l):
        for i, ld in enumerate(load_raw(l)):
            ld.wait()
            ws[l, i] = raw[i].reshape(ws.shape[2], loc_w)
    for ld in load_raw(0):
        ld.start()
    vrow[...] = jnp.zeros_like(vrow)
    for i, ref in enumerate((g1_ref, b1_ref, g2_ref, b2_ref, bo_ref, bd_ref)):
        vrow[i * n_layers:(i + 1) * n_layers, :piece_w] = ref[...].astype(F32)
    vloc[...] = vrow[...].astype(BF16)
    bloc[...] = jnp.zeros_like(bloc)
    bloc[:n_layers, :] = bup_ref[...].astype(F32)
    flatten(0)
    pl.semaphore_wait(barrier, n_dev - 1)

    def halves(ref, l, n):
        return lambda h: ref.at[l, pl.ds(h * n, n)]

    def shard_rows(dst, n_shard, n, at_cols):
        return lambda ys, h: dst.at[rows(ys * n_shard + h * n, n), at_cols]

    qkv_rows = ws.shape[2]
    up_rows = wu_hbm.shape[1]
    down_rows = wd_hbm.shape[1]
    o_rows = wo_hbm.shape[1]

    def gather_qkv(l):
        n = qkv_rows // 2
        return ColumnGather(p, [((lambda h, i=i: ws.at[l, i, pl.ds(h * n, n)]),
                                 shard_rows(w, qkv_rows, n, pl.ds(i * loc_w, loc_w))) for i in range(3)], wq_sems)

    def gather_up(l):
        n, half = up_rows // 2, wu.shape[1] // 2
        return ColumnGather(p, [((lambda h, at_c=at_c: wu_hbm.at[l, pl.ds(h * n, n), at_c]), shard_rows(wu, up_rows, n, at_c))
                                for at_c in (pl.ds(0, half), pl.ds(half, half))], wu_sems, early=1)

    def gather_down(l):
        n = down_rows // 2
        return ColumnGather(p, [(halves(wd_hbm, l, n), lambda ys, h: wd.at[ys, pl.ds(h * n, n)])], wd_sems)

    def gather_o(l):
        n = o_rows // 2
        return ColumnGather(p, [(halves(wo_hbm, l, n), lambda ys, h: wo.at[ys, rows(ty * o_rows + h * n, n)])], wo_sems)

    def spread_o(l):
        n = num_tx // 2
        return RingGather(p, lambda chip, core, h: wo.at[pl.ds(h * n, n), rows((chip * 2 + core) * o_rows, o_rows)], wx_sems)

    g_qkv = [gather_qkv(l) for l in range(n_layers)]
    g_up = [gather_up(l) for l in range(n_layers)]
    g_down = [gather_down(l) for l in range(n_layers)]
    g_o = [gather_o(l) for l in range(n_layers)]
    s_o = [spread_o(l) for l in range(n_layers)]

    for d, to in zip(ids, devs):
        remote(xt_hbm.at[:, rows(d * n_row, n_row)], xt.at[rows(p.me * piece_w, piece_w)], x_sems.at[0], x_sems.at[1], to).start()
        remote(vloc, vbuf.at[p.me], v_sems.at[0], v_sems.at[1], to).start()
    g_o[0].start()
    g_qkv[0].start_first()
    pltpu.make_async_copy(xt_hbm.at[:, rows(p.me * n_row, n_row)], xt.at[rows(p.me * piece_w, piece_w)], x_sems.at[1]).start()
    pltpu.make_async_copy(vloc, vbuf.at[p.me], v_sems.at[1]).start()
    bup_w = bup_ref.shape[1]
    for k in range(1, num_tx):
        remote(bloc, bup.at[:, rows(y * bup_w, bup_w)], b_sems.at[0], b_sems.at[1], p.over(k)).start()
    pltpu.make_async_copy(bloc, bup.at[:, rows(y * bup_w, bup_w)], b_sems.at[1]).start()
    for l in range(1, n_layers):
        for ld in load_raw(l):
            ld.start()
        flatten(l)

    lane = lax.broadcasted_iota(jnp.int32, (1, head_w), 1)
    inv_freq = jnp.exp(lax.rem(lane, head_w // 2).astype(F32) * (-2.0 * math.log(ROPE_THETA) / head_w))
    sign = jnp.where(lane < head_w // 2, -1.0, 1.0)

    def angles(k, carry):
        pos = pos_ref[pl.ds(y * n_chip + k, 1), :].astype(F32)
        ang = jnp.broadcast_to(pos, (head_w, blk)).T * inv_freq
        cs[0, rows(k * blk, blk), :] = jnp.cos(ang)
        cs[1, rows(k * blk, blk), :] = jnp.sin(ang) * sign
        return carry
    lax.fori_loop(0, n_chip, angles, 0)
    took(vbuf, v_sems.at[1])
    per = LANES // piece_w
    for j in range(width // LANES):
        vec[:, j * LANES:(j + 1) * LANES] = jnp.concatenate(
            [vbuf[per * j + i][:, :piece_w].astype(F32) for i in range(per)], axis=1)
    took(xt, x_sems.at[1])

    def turn(j, carry):
        hid[:, rows(j * LANES, LANES)] = xt[rows(j * LANES, LANES), :].T
        return carry
    lax.fori_loop(0, width // LANES, turn, 0)

    def vector(i, l):
        return vec[i * n_layers + l:i * n_layers + l + 1, :]

    def row_gather(sems):
        return RingGather(p, lambda chip, core, h: a_all.at[chip, rows(core * n_row + h * half_row, half_row)], sems)

    def order(n):
        return n + n // 2 - 2 * (n // 3)

    def each(n_from, n_to, body, hooks):
        def step(n, carry):
            for at_n, hook in hooks.items():
                @pl.when(n == at_n)
                def _():
                    for h in hook:
                        h()
            body(order(n))
            return carry
        lax.fori_loop(n_from, n_to, step, 0)

    def project(l, k):
        slot = p.chip(k)
        at_row = rows(slot * blk, blk)
        acc = jnp.dot(a_all[slot], w[...], preferred_element_type=F32)
        cos_t, sin_t = cs[0, at_row, :], cs[1, at_row, :]
        for i, bias in enumerate((bq_ref, bk_ref, bv_ref)):
            parts = []
            for h in range(loc_heads):
                lo = i * loc_w + h * head_w
                v = acc[:, lo:lo + head_w] + bias[l, h:h + 1, :].astype(F32)
                if i < 2:
                    v = v * cos_t + pltpu.roll(v, head_w // 2, 1) * sin_t
                v = v.astype(BF16)
                parts.append(v)
                if i < 2:
                    st[k, h, i] = v
                else:
                    sv[k, h] = v.T
            if i > 0:
                (kc_ref, vc_ref)[i - 1][l, at_row] = jnp.concatenate(parts, axis=1).reshape(blk, loc_heads, head_w)
        at_tok = rows((y * n_chip + slot) * blk, blk)
        par = lax.rem(slot, 2)
        at_q = rows((y * (n_chip // 2) + slot // 2) * blk, blk)
        for h in range(loc_heads):
            yd = c * loc_heads + h
            for r, (src, dst) in enumerate(((st.at[k, h, 1], kt.at[at_tok]), (sv.at[k, h], vt.at[:, at_tok]))):
                copy_or_send(jnp.logical_and(yd == y, c == r), src, dst, kv_sems.at[0], kv_sems.at[1], p.at(yd, x * 2 + r))
            copy_or_send(jnp.logical_and(yd == y, c == par), st.at[k, h, 0], qh.at[at_q], kv_sems.at[2], kv_sems.at[3],
                         p.at(yd, x * 2 + par))

    n_q = ob.shape[0]
    q_grp = 2 * blk
    n_grp = n_q * blk // q_grp
    n_sub = BK // blk

    def attend(hooks):
        def step(n, carry):
            grp = n_grp - 1 - n
            q = qh[rows(grp * q_grp, q_grp), :]
            q_col = lax.broadcasted_iota(jnp.int32, (1, blk), 1)
            at_q = [(2 * (2 * grp + i) + c) for i in range(2)]
            q_pos = jnp.concatenate([q_col + b * blk for b in at_q], axis=1)
            first = q_pos - jnp.concatenate([pos_ref[pl.ds(b, 1), :] for b in at_q], axis=1)
            key = lax.broadcasted_iota(jnp.int32, (blk, q_grp), 0)
            scale = head_w ** -0.5 * LOG2E

            def score(j, m, diag):
                s = lax.dot_general(kt[rows(j * BK, BK), :], q, (((1,), (1,)), ((), ())), preferred_element_type=F32)
                for i in range(n_sub):
                    k_pos = key + (j * BK + i * blk)
                    ok = k_pos >= first
                    if diag:
                        ok = jnp.logical_and(ok, k_pos <= q_pos)
                    part = jnp.where(ok, s[i * blk:(i + 1) * blk], -1e30)
                    full[j, :, i * q_grp:(i + 1) * q_grp] = part
                    m = jnp.maximum(m, jnp.max(part.reshape(blk // 8, 8, q_grp), axis=0))
                return m
            m = lax.fori_loop(0, grp, lambda j, m: score(j, m, False), jnp.full((8, q_grp), -1e30, F32))
            m = jnp.max(score(grp, m, True), axis=0, keepdims=True)

            def expo(j, t):
                for i in range(n_sub):
                    e = jnp.exp2((full[j, :, i * q_grp:(i + 1) * q_grp] - m) * scale)
                    full[j, :, i * q_grp:(i + 1) * q_grp] = e
                    t = t + jnp.sum(e.reshape(blk // 8, 8, q_grp), axis=0)
                return t
            t = lax.fori_loop(0, grp + 1, expo, jnp.zeros((8, q_grp), F32))
            inv = 1.0 / jnp.sum(t, axis=0, keepdims=True)

            def apply(j, acc):
                prob = jnp.concatenate([(full[j, :, i * q_grp:(i + 1) * q_grp] * inv).astype(BF16) for i in range(n_sub)], axis=0)
                return acc + jnp.dot(vt[:, rows(j * BK, BK)], prob, preferred_element_type=F32)
            out = lax.fori_loop(0, grp + 1, apply, jnp.zeros((head_w, q_grp), F32)).T.astype(BF16)
            cols_o = rows((x * num_tx + y) * head_w, head_w)
            for i, b in enumerate(at_q):
                ob[2 * grp + i] = out[i * blk:(i + 1) * blk]
                yt, xd = b // n_chip, lax.rem(b, n_chip)
                for r in range(2):
                    here = jnp.logical_and(jnp.logical_and(yt == y, xd == x), c == r)
                    copy_or_send(here, ob.at[2 * grp + i, pl.ds(r * n_row, n_row)], obuf.at[:, cols_o], o_sems.at[0],
                                 o_sems.at[1], p.at(yt, xd * 2 + r))
            for at_n, hook in hooks.items():
                @pl.when(n == at_n)
                def _():
                    for h in hook:
                        h()
            return carry
        lax.fori_loop(0, n_grp, step, 0)

    def up(l, k):
        slot = p.chip(k)

        def part(n, carry):
            cc = rows(n * 512, 512)
            h = jnp.dot(a_all[slot], wu[:, cc], preferred_element_type=F32) + bup[l:l + 1, cc]
            g[k, :, cc] = gelu_tanh(h).astype(BF16)
            return carry
        lax.fori_loop(0, wu.shape[1] // 512, part, 0)

    blocks = (0, 1, last, 2)
    cols = [rows(p.side(k) * col_w, col_w) for k in blocks]
    top, bottom = rows(c * n_row, half_row), rows(c * n_row + half_row, half_row)

    def to_sibling(k, j):
        i = k * num_tx + j
        return remote(full.at[k, other, cols[j]], sibin.at[k, :, cols[j]], p_sems.at[0, i], p_sems.at[1, i], p.sib)

    def rs(kind, j):
        k, part, dst, to = ((1, bottom, fin.at[0], p.right), (last, top, fin.at[1], p.left), (2, top, far_in.at[0], p.right),
                            (2, bottom, far_in.at[1], p.left), (1, top, fin.at[2], p.right),
                            (last, bottom, fin.at[3], p.left))[kind]
        i = kind * num_tx + j
        return remote(full.at[k, part, cols[j]], dst.at[:, cols[j]], r_sems.at[0, i], r_sems.at[1, i], to)

    def partials(j):
        def part(n, carry):
            k = order(lax.rem(n + 1, n_chip))
            full[k, :, cols[j]] = jnp.dot(g[k], wd[p.side(blocks[j])], preferred_element_type=F32)
            to_sibling(k, j).start()
            return carry
        lax.fori_loop(0, n_chip, part, 0)

    def pair_sum(k, j):
        to_sibling(k, j).wait_recv()
        full[k, mine, cols[j]] = full[k, mine, cols[j]] + sibin[k, :, cols[j]]

    def send_partials(j):
        pair_sum(1, j)
        rs(S_DIRECT_R, j).start()
        pair_sum(last, j)
        rs(S_DIRECT_L, j).start()
        pair_sum(2, j)
        rs(S_FAR_R, j).start()
        rs(S_FAR_L, j).start()
        pair_sum(0, j)

    def pass_on(j):
        rs(S_FAR_R, j).wait_recv()
        full[1, top, cols[j]] = full[1, top, cols[j]] + far_in[0, :, cols[j]]
        rs(S_SUM_R, j).start()
        rs(S_FAR_L, j).wait_recv()
        full[last, bottom, cols[j]] = full[last, bottom, cols[j]] + far_in[1, :, cols[j]]
        rs(S_SUM_L, j).start()

    def complete(l, j):
        cc = cols[j]
        bias = vec[5 * n_layers + l:5 * n_layers + l + 1, cc]
        for kind in (S_DIRECT_R, S_DIRECT_L, S_SUM_R, S_SUM_L):
            rs(kind, j).wait_recv()
        for part, out, ins in ((top, pl.ds(0, half_row), (1, 2)), (bottom, pl.ds(half_row, half_row), (0, 3))):
            tot = full[0, part, cc] + fin[ins[0], :, cc] + fin[ins[1], :, cc]
            hid[out, cc] = (hid[out, cc].astype(F32) + tot + bias).astype(BF16)

    def give_back(j):
        row = p.side(blocks[j])

        def turn_back(n, carry):
            at_c = rows(row * col_w + n * LANES, LANES)
            xt[at_c, :] = hid[:, at_c].T
            return carry
        lax.fori_loop(0, col_w // LANES, turn_back, 0)
        for k in range(num_ty):
            to_ty = lax.rem(ty + k, num_ty)
            copy_or_send(jnp.logical_and(row == y, k == 0), xt.at[rows((row * num_ty + to_ty) * piece_w, piece_w)],
                         yt_ref.at[:, rows(p.me * n_row, n_row)], y_sems.at[0], y_sems.at[1], p.at(row, to_ty))

    def start_forward():
        @pl.when(c == 0)
        def _():
            remote(kt, kt, kv_sems.at[4], kv_sems.at[5], p.sib).start()

        @pl.when(c != 0)
        def _():
            remote(vt, vt, kv_sems.at[4], kv_sems.at[5], p.sib).start()

    for l in range(n_layers):
        first_layer, last_layer = l == 0, l == n_layers - 1
        a_all[x, mine, :] = rows_norm(hid[...].astype(F32), vector(0, l), vector(1, l))
        ga = row_gather(a_sems)
        ga.start()
        if first_layer:
            g_o[l].relay()
            g_qkv[l].start_second()
            ga.relay()
            g_qkv[l].relay()
            ga.own()
            ga.near()
            g_o[l].finish()
            s_o[l].start()
            ga.near_right()
            ga.near_left()
            ga.far()
            ga.far_done()
            ga.drain()
            g_qkv[l].finish()
            each(0, n_chip, lambda k: project(l, k), {})
        else:
            g_qkv[l].relay()
            ga.relay()
            ga.own()
            g_o[l].finish()
            s_o[l].start()
            g_qkv[l].finish()
            each(0, last, lambda k: project(l, k), {1: [ga.near, ga.near_right, ga.near_left]})
            ga.far()
            ga.far_done()
            ga.drain()
            project(l, 2)
        g_up[l].start_first()
        s_o[l].relay()
        took(kt, kv_sems.at[1])
        start_forward()
        took(qh, kv_sems.at[3])
        took(kt, kv_sems.at[5])
        took(kt, kv_sems.at[4])
        attend({0: [s_o[l].near]})
        g_up[l].start_second()
        g_up[l].relay()
        g_qkv[l].drain()
        g_down[l].start()
        s_o[l].far()
        s_o[l].own()
        s_o[l].near_right()
        s_o[l].near_left()
        s_o[l].far_done()
        took(obuf, o_sems.at[1])

        def out_product(t, carry):
            cc = rows(t * col_w, col_w)
            bias = vec[4 * n_layers + l:4 * n_layers + l + 1, cc]
            hid[:, cc] = (hid[:, cc].astype(F32) + jnp.dot(obuf[...], wo[t], preferred_element_type=F32) + bias).astype(BF16)
            return carry
        lax.fori_loop(0, num_tx, out_product, 0)
        a_all[x, mine, :] = rows_norm(hid[...].astype(F32), vector(2, l), vector(3, l))
        gu = row_gather(u_sems)
        gu.start()
        if first_layer:
            took(bup, b_sems.at[1])
        gu.own()
        gu.relay()
        g_up[l].finish()
        each(0, n_chip, lambda k: up(l, k), {1: [gu.near, gu.near_right, gu.near_left], last: [gu.far, gu.far_done]})
        gu.drain()
        s_o[l].drain()
        g_o[l].drain()
        g_up[l].drain()
        g_down[l].relay()
        if not last_layer:
            g_qkv[l + 1].start_first()
        for j in range(num_tx):
            g_down[l].shard(blocks[j])
            if j == num_tx - 1 and not last_layer:
                g_o[l + 1].start()
            partials(j)
            send_partials(j)
            if j > 0:
                pass_on(j - 1)
            if j > 1:
                complete(l, j - 2)
                if last_layer:
                    give_back(j - 2)
        if not last_layer:
            g_o[l + 1].relay()
            g_qkv[l + 1].start_second()
        pass_on(num_tx - 1)
        for j in range(num_tx - 2, num_tx):
            complete(l, j)
            if last_layer:
                give_back(j)
        for j in range(num_tx):
            for k in range(n_chip):
                to_sibling(k, j).wait_send()
            for kind in range(6):
                rs(kind, j).wait_send()
        g_down[l].drain()
        sent_away(p, kt, qh, kv_sems, loc_heads)
        o_away(p, obuf, o_sems, head_w)

    took(xt_hbm.at[:, pl.ds(0, (n_dev - 1) * n_row)], x_sems.at[0])
    took(vbuf.at[pl.ds(0, n_dev - 1)], v_sems.at[0])
    took(bup.at[:, pl.ds(0, (num_tx - 1) * bup_w)], b_sems.at[0])
    took(yt_ref, y_sems.at[1])
    took(xt.at[pl.ds(0, (n_dev - 1) * piece_w)], y_sems.at[0])


def sent_away(p, kt, qh, kv_sems, loc_heads):
    stays = p.c == p.y // loc_heads
    n_tok = kt.shape[0]
    n_q = qh.shape[0]

    @pl.when(stays)
    def _():
        took(kt.at[pl.ds(0, n_tok * 3 // 4)], kv_sems.at[0])
        took(qh.at[pl.ds(0, n_q * 3 // 4)], kv_sems.at[2])

    @pl.when(jnp.logical_not(stays))
    def _():
        took(kt, kv_sems.at[0])
        took(qh, kv_sems.at[2])


def o_away(p, obuf, o_sems, head_w):
    stays = lax.rem(p.x, 2) == p.c

    @pl.when(stays)
    def _():
        took(obuf.at[:, pl.ds(0, obuf.shape[1] - head_w)], o_sems.at[0])

    @pl.when(jnp.logical_not(stays))
    def _():
        took(obuf, o_sems.at[0])


def decoder(num_tx, num_ty, xt, vectors, b_up, b_qkv, pos, wq, wk, wv, wo, wu, wd):
    n_layers, d_rows, loc_heads, head_w = wq.shape
    n_dev = num_tx * num_ty
    n_chip = num_ty // 2
    piece_w, n_tok = xt.shape
    width = piece_w * n_dev
    n_row = n_tok // n_dev
    blk = 2 * n_row
    loc_w = loc_heads * head_w
    tok_loc = n_tok // num_tx
    ff = wu.shape[2]
    col_w = wd.shape[2]
    n_q = n_tok // (2 * blk)
    n_vec = -(-len(vectors) * n_layers // 16) * 16
    vm = pl.BlockSpec(memory_space=pltpu.VMEM)
    hb = pl.BlockSpec(memory_space=pl.ANY)
    V = pltpu.VMEM
    dma = pltpu.SemaphoreType.DMA
    cache = jax.ShapeDtypeStruct((n_layers, tok_loc, loc_heads, head_w), BF16)
    CG, RG = ColumnGather.SEMS, RingGather.SEMS
    return pl.pallas_call(
        functools.partial(decoder_kernel, num_tx, num_ty, n_layers),
        out_shape=(jax.ShapeDtypeStruct((piece_w, n_tok), BF16), cache, cache),
        in_specs=[hb] + [vm] * 11 + [hb] * 6,
        out_specs=(vm,) * 3,
        scratch_shapes=[V((width, n_row), BF16), V((n_vec, LANES), F32), V((n_vec, LANES), BF16), V((n_dev, n_vec, LANES), BF16),
                        V((n_vec, width), F32), V((8, b_up.shape[1]), F32), V((8, ff), F32),
                        V((3, d_rows, loc_heads, head_w), BF16), V((n_layers, 3, d_rows, loc_w), BF16),
                        V((width, 3 * loc_w), BF16), V((width, ff), BF16), V((num_tx, ff, col_w), BF16),
                        V((num_tx, width, col_w), BF16), V((2, tok_loc, head_w), F32),
                        V((n_chip, blk, width), BF16), V((n_row, width), BF16),
                        V((n_chip, loc_heads, 2, blk, head_w), BF16), V((n_chip, loc_heads, head_w, blk), BF16),
                        V((n_tok, head_w), BF16), V((head_w, n_tok), BF16), V((n_q * blk, head_w), BF16),
                        V((n_q, blk, head_w), BF16), V((n_row, width), BF16), V((n_chip, blk, ff), BF16),
                        V((n_chip, blk, width), F32), V((n_chip, n_row, width), F32),
                        V((2, n_row // 2, width), F32), V((4, n_row // 2, width), F32),
                        dma((2,)), dma((2,)), dma((2,)), dma((2,)), dma((2, RG)), dma((2, RG)), dma((2, 3 * CG)), dma((2, CG)),
                        dma((2, RG)), dma((2, 2 * CG)), dma((2, CG)), dma((6,)), dma((2,)), dma((2, n_chip * num_tx)),
                        dma((2, 6 * num_tx)), dma((3,))],
        compiler_params=pltpu.CompilerParams(collective_id=1, has_side_effects=True, vmem_limit_bytes=63 << 20),
        name="decoder",
    )(xt, *vectors, b_up, *b_qkv, pos, wq, wk, wv, wo, wu, wd)


def solution(mesh):
    num_tx = mesh.shape['tx']
    num_ty = mesh.shape['ty']
    width_spec = P('dp', ('tx', 'ty'))
    vec_spec = P(None, ('tx', 'ty'))
    proj_spec = P(None, 'tx', 'ty', None)
    head_spec = P(None, 'ty', None)
    cache_spec = P(None, ('dp', 'tx'), 'ty', None)
    in_specs = (width_spec, P('dp'), P('dp'), vec_spec, vec_spec, proj_spec, head_spec, proj_spec, head_spec,
                proj_spec, head_spec, P(None, 'ty', None, 'tx'), vec_spec, vec_spec, vec_spec,
                P(None, 'tx', 'ty'), P(None, ('ty', 'tx')), P(None, 'ty', 'tx'), vec_spec)
    out_specs = (width_spec, cache_spec, cache_spec)

    def device_fn(x_loc, seg_all, pos_all, ln1_gain, ln1_bias, w_q, b_q, w_k, b_k, w_v, b_v, w_o, b_o,
                  ln2_gain, ln2_bias, w_up, b_up, w_down, b_down):
        n_tok = x_loc.shape[0]
        blk = 2 * n_tok // (num_tx * num_ty)
        yt, k, v = decoder(num_tx, num_ty, x_loc.T, (ln1_gain, ln1_bias, ln2_gain, ln2_bias, b_o, b_down), b_up,
                           (b_q, b_k, b_v), pos_all.reshape(-1, blk), w_q, w_k, w_v,
                           w_o.reshape(w_o.shape[0], -1, w_o.shape[-1]), w_up, w_down)
        return yt.T, k, v

    return jax.shard_map(device_fn, mesh=mesh, in_specs=in_specs, out_specs=out_specs, check_vma=False)
```

```python
import math
import functools
import jax
import jax.numpy as jnp
from jax import lax
from jax.experimental import pallas as pl
from jax.experimental.pallas import tpu as pltpu
from jax.sharding import PartitionSpec as P

MESH = pl.DeviceIdType.MESH
F32 = jnp.float32
BF16 = jnp.bfloat16
ROPE_THETA = 100000.0
LOG2E = 1.4426950408889634
LANES = 128
BK = 1024
SEND, RECV = 0, 1


def rows_norm(x_f32, gain, bias):
    width = x_f32.shape[-1]
    mean = jnp.sum(x_f32, axis=-1, keepdims=True) / width
    var = jnp.sum(x_f32 * x_f32, axis=-1, keepdims=True) / width - mean * mean
    normed = (x_f32 - mean) * lax.rsqrt(var + 1e-5)
    return (normed * gain + bias).astype(BF16)


def gelu_tanh(x):
    return 0.5 * x * (1.0 + jnp.tanh(0.7978845608028654 * (x + 0.044715 * (x * x * x))))


def rows(at, n):
    return pl.ds(pl.multiple_of(at, n), n)


class Place:
    def __init__(self, num_tx, num_ty):
        self.num_tx, self.num_ty, self.n_chip = num_tx, num_ty, num_ty // 2
        self.y = lax.axis_index('tx')
        self.ty = lax.axis_index('ty')
        self.x = self.ty // 2
        self.c = lax.rem(self.ty, 2)
        self.me = self.y * num_ty + self.ty
        self.sib = self.at(self.y, self.x * 2 + 1 - self.c)
        self.right, self.left = self.beside(1), self.beside(self.n_chip - 1)
        self.above, self.below = self.over(1), self.over(num_tx - 1)

    def at(self, y, ty):
        return {'tx': y, 'ty': ty}

    def chip(self, k):
        return lax.rem(self.x + k, self.n_chip)

    def side(self, k):
        return lax.rem(self.y + k, self.num_tx)

    def beside(self, k):
        return self.at(self.y, self.chip(k) * 2 + self.c)

    def over(self, k):
        return self.at(self.side(k), self.ty)


def remote(src, dst, send_sem, recv_sem, to):
    return pltpu.make_async_remote_copy(src_ref=src, dst_ref=dst, send_sem=send_sem, recv_sem=recv_sem, device_id=to,
                                        device_id_type=MESH)


def copy_or_send(here, src, dst, send_sem, recv_sem, to):
    @pl.when(here)
    def _():
        pltpu.make_async_copy(src, dst, recv_sem).start()

    @pl.when(jnp.logical_not(here))
    def _():
        remote(src, dst, send_sem, recv_sem, to).start()


def took(ref, sem):
    pltpu.make_async_copy(ref, ref, sem).wait()


class RingGather:
    SEMS = 14

    def __init__(self, p, view, sems):
        self.p = p
        self.view = view
        self.sems = sems
        x, c, d = p.x, p.c, 1 - p.c
        far, left, right = p.chip(2), p.chip(p.n_chip - 1), p.chip(1)
        self.plan = [(x, 0, p.right, left), (x, 1, p.left, right), (x, 1, p.right, left), (x, 0, p.left, right),
                     (left, 0, p.right, far), (right, 1, p.left, far),
                     (x, 0, p.sib, x), (x, 1, p.sib, x), (left, 0, p.sib, left), (left, 1, p.sib, left),
                     (right, 0, p.sib, right), (right, 1, p.sib, right), (far, 0, p.sib, far), (far, 1, p.sib, far)]

    def out(self, i):
        chip, half, to, _ = self.plan[i]
        ref = self.view(chip, self.p.c, half)
        return remote(ref, ref, self.sems.at[SEND, i], self.sems.at[RECV, i], to)

    def arrived(self, i):
        _, half, to, chip = self.plan[i]
        core = self.p.c if i < 6 else 1 - self.p.c
        ref = self.view(chip, core, half)
        remote(ref, ref, self.sems.at[SEND, i], self.sems.at[RECV, i], to).wait_recv()

    def start_first(self):
        for i in (6, 7, 0, 1):
            self.out(i).start()

    def start_second(self):
        for i in (2, 3):
            self.out(i).start()

    def start(self):
        self.start_first()
        self.start_second()

    def own(self):
        self.arrived(6)
        self.arrived(7)

    def relay(self):
        self.arrived(0)
        self.out(4).start()
        self.arrived(1)
        self.out(5).start()
        self.out(8).start()
        self.out(11).start()

    def near(self):
        self.arrived(2)
        self.out(9).start()
        self.arrived(3)
        self.out(10).start()

    def near_right(self):
        self.arrived(10)
        self.arrived(11)

    def near_left(self):
        self.arrived(8)
        self.arrived(9)

    def far(self):
        self.arrived(4)
        self.out(12).start()
        self.arrived(5)
        self.out(13).start()

    def far_done(self):
        self.arrived(12)
        self.arrived(13)

    def drain(self):
        for i in range(self.SEMS):
            self.out(i).wait_send()


class ColumnGather:
    SEMS = 8

    def __init__(self, p, pieces, sems, early=0):
        self.p = p
        self.pieces = pieces
        self.sems = sems
        self.early = early

    def copy(self, n, i):
        p = self.p
        src, dst = self.pieces[n]
        up, down = p.side(1), p.side(p.num_tx - 1)
        half, to = ((0, p.above), (1, p.below), (1, p.above), (0, p.below), (0, p.above), (1, p.below))[i]
        here = src(half) if i < 4 else dst(down if i == 4 else up, half)
        there = dst((p.y, p.y, p.y, p.y, down, up)[i], half)
        return remote(here, there, self.sems.at[SEND, n * self.SEMS + i], self.sems.at[RECV, n * self.SEMS + i], to)

    def arrived(self, n, i):
        p = self.p
        src, dst = self.pieces[n]
        up, down, far = p.side(1), p.side(p.num_tx - 1), p.side(2)
        half, frm = ((0, down), (1, up), (1, down), (0, up), (0, far), (1, far))[i]
        remote(src(half), dst(frm, half), self.sems.at[SEND, n * self.SEMS + i], self.sems.at[RECV, n * self.SEMS + i],
               p.above).wait_recv()

    def own(self, n, half):
        src, dst = self.pieces[n]
        return pltpu.make_async_copy(src(half), dst(self.p.y, half), self.sems.at[RECV, n * self.SEMS + 6 + half])

    def start_first(self):
        for i in (0, 1):
            for n in range(len(self.pieces)):
                self.copy(n, i).start()
        self.rest(range(self.early))

    def start_second(self):
        self.rest(range(self.early, len(self.pieces)))

    def rest(self, which):
        for i in (2, 3):
            for n in which:
                self.copy(n, i).start()
        for n in which:
            self.own(n, 0).start()
            self.own(n, 1).start()

    def start(self):
        self.start_first()
        self.start_second()

    def relay(self, which=None):
        for n in range(len(self.pieces)) if which is None else which:
            self.arrived(n, 0)
            self.copy(n, 4).start()
            self.arrived(n, 1)
            self.copy(n, 5).start()

    def step(self, j, which=None):
        for n in range(len(self.pieces)) if which is None else which:
            if j == 0:
                self.own(n, 0).wait()
                self.own(n, 1).wait()
            elif j > 1:
                self.arrived(n, 2 * j - 2)
                self.arrived(n, 2 * j - 1)

    def piece(self, n):
        for j in range(4):
            self.step(j, [n])

    def finish(self):
        for j in range(4):
            self.step(j)

    def drain(self):
        for n in range(len(self.pieces)):
            for i in range(6):
                self.copy(n, i).wait_send()


S_DIRECT_R, S_DIRECT_L, S_FAR_R, S_FAR_L, S_SUM_R, S_SUM_L = range(6)


def decoder_kernel(num_tx, num_ty, n_layers,
                   xt_hbm, g1_ref, b1_ref, g2_ref, b2_ref, bo_ref, bd_ref, bup_ref, bq_ref, bk_ref, bv_ref, pos_hbm,
                   wq_hbm, wk_hbm, wv_hbm, wo_hbm, wu_hbm, wd_hbm,
                   yt_hbm, kc_hbm, vc_hbm, go_hbm,
                   pos, xt, vrow, vloc, vbuf, vec, bloc, bup, raw, ws, w, wu, wd, wo, cs, a_all, hid, st, sv, kc, vc, kt, vt, qh, ob, obuf,
                   g, full, sibin, far_in, fin,
                   x_sems, v_sems, b_sems, y_sems, a_sems, u_sems, wq_sems, wo_sems, wx_sems, wu_sems, wd_sems,
                   kv_sems, o_sems, p_sems, r_sems, l_sems, c_sems):
    p = Place(num_tx, num_ty)
    n_dev = num_tx * num_ty
    n_chip, x, y, c, ty = p.n_chip, p.x, p.y, p.c, p.ty
    n_row, width = hid.shape
    blk = 2 * n_row
    half_row = n_row // 2
    loc_heads, head_w = wq_hbm.shape[2], wq_hbm.shape[3]
    loc_w = loc_heads * head_w
    col_w = wd.shape[2]
    piece_w = xt_hbm.shape[0]
    last = n_chip - 1
    mine, other = rows(c * n_row, n_row), rows((1 - c) * n_row, n_row)

    barrier = pltpu.get_barrier_semaphore()
    ids = [lax.rem(p.me + k, n_dev) for k in range(1, n_dev)]
    devs = [p.at(d // num_ty, lax.rem(d, num_ty)) for d in ids]
    for to in devs:
        pl.semaphore_signal(barrier, inc=1, device_id=to, device_id_type=MESH)

    def load_raw(l):
        return [pltpu.make_async_copy(src.at[l], raw.at[i], l_sems.at[i]) for i, src in enumerate((wq_hbm, wk_hbm, wv_hbm))]

    def flatten(l):
        for i, ld in enumerate(load_raw(l)):
            ld.wait()
            ws[l, i] = raw[i].reshape(ws.shape[2], loc_w)
    for ld in load_raw(0):
        ld.start()
    load_pos = pltpu.make_async_copy(pos_hbm, pos, l_sems.at[3])
    load_pos.start()
    vrow[...] = jnp.zeros_like(vrow)
    for i, ref in enumerate((g1_ref, b1_ref, g2_ref, b2_ref, bo_ref, bd_ref)):
        vrow[i * n_layers:(i + 1) * n_layers, :piece_w] = ref[...].astype(F32)
    vloc[...] = vrow[...].astype(BF16)
    bloc[...] = jnp.zeros_like(bloc)
    bloc[:n_layers, :] = bup_ref[...].astype(F32)
    pl.semaphore_wait(barrier, n_dev - 1)

    def halves(ref, l, n):
        return lambda h: ref.at[l, pl.ds(h * n, n)]

    def shard_rows(dst, n_shard, n, at_cols):
        return lambda ys, h: dst.at[rows(ys * n_shard + h * n, n), at_cols]

    qkv_rows = ws.shape[2]
    up_rows = wu_hbm.shape[1]
    o_rows = wo_hbm.shape[1]

    def gather_qkv(l):
        n = qkv_rows // 2
        return ColumnGather(p, [((lambda h, i=i: ws.at[l, i, pl.ds(h * n, n)]),
                                 shard_rows(w, qkv_rows, n, pl.ds(i * loc_w, loc_w))) for i in range(3)], wq_sems)

    def gather_up(l):
        n, half = up_rows // 2, wu.shape[1] // 2
        return ColumnGather(p, [((lambda h, at_c=at_c: wu_hbm.at[l, pl.ds(h * n, n), at_c]), shard_rows(wu, up_rows, n, at_c))
                                for at_c in (pl.ds(0, half), pl.ds(half, half))], wu_sems, early=1)

    def gather_down(l):
        n = col_w // 2
        return ColumnGather(p, [((lambda h: wd_hbm.at[l, :, pl.ds(h * n, n)]), lambda ys, h: wd.at[ys, :, pl.ds(h * n, n)])],
                            wd_sems)

    def whole_o(l):
        return wo if l == 0 else go_hbm.at[l - 1]

    def gather_o(l):
        n = o_rows // 2
        return ColumnGather(p, [(halves(wo_hbm, l, n), lambda ys, h: whole_o(l).at[ys, rows(ty * o_rows + h * n, n)])],
                            wo_sems.at[l])

    def spread_o(l):
        n = num_tx // 2
        return RingGather(p, lambda chip, core, h: whole_o(l).at[pl.ds(h * n, n), rows((chip * 2 + core) * o_rows, o_rows)],
                          wx_sems.at[l])

    g_qkv = [gather_qkv(l) for l in range(n_layers)]
    g_up = [gather_up(l) for l in range(n_layers)]
    g_down = [gather_down(l) for l in range(n_layers)]
    g_o = [gather_o(l) for l in range(n_layers)]
    s_o = [spread_o(l) for l in range(n_layers)]

    for d, to in zip(ids, devs):
        remote(xt_hbm.at[:, rows(d * n_row, n_row)], xt.at[rows(p.me * piece_w, piece_w)], x_sems.at[SEND], x_sems.at[RECV], to).start()
        remote(vloc, vbuf.at[p.me], v_sems.at[SEND], v_sems.at[RECV], to).start()
    g_o[0].start()
    flatten(0)
    g_qkv[0].start_first()
    pltpu.make_async_copy(xt_hbm.at[:, rows(p.me * n_row, n_row)], xt.at[rows(p.me * piece_w, piece_w)], x_sems.at[RECV]).start()
    pltpu.make_async_copy(vloc, vbuf.at[p.me], v_sems.at[RECV]).start()
    bup_w = bup_ref.shape[1]
    for k in range(1, num_tx):
        remote(bloc, bup.at[:, rows(y * bup_w, bup_w)], b_sems.at[SEND], b_sems.at[RECV], p.over(k)).start()
    pltpu.make_async_copy(bloc, bup.at[:, rows(y * bup_w, bup_w)], b_sems.at[RECV]).start()
    for l in range(1, n_layers):
        for ld in load_raw(l):
            ld.start()
        flatten(l)

    load_pos.wait()
    lane = lax.broadcasted_iota(jnp.int32, (1, head_w), 1)
    inv_freq = jnp.exp(lax.rem(lane, head_w // 2).astype(F32) * (-2.0 * math.log(ROPE_THETA) / head_w))
    sign = jnp.where(lane < head_w // 2, -1.0, 1.0)

    def positions(b):
        return pos[rows(b * blk, blk)].reshape(1, blk)

    def angles(k, carry):
        ang = jnp.broadcast_to(positions(y * n_chip + k).astype(F32), (head_w, blk)).T * inv_freq
        cs[0, rows(k * blk, blk), :] = jnp.cos(ang)
        cs[1, rows(k * blk, blk), :] = jnp.sin(ang) * sign
        return carry
    lax.fori_loop(0, n_chip, angles, 0)
    took(vbuf, v_sems.at[RECV])
    per = LANES // piece_w
    for j in range(width // LANES):
        vec[:, j * LANES:(j + 1) * LANES] = jnp.concatenate(
            [vbuf[per * j + i][:, :piece_w].astype(F32) for i in range(per)], axis=1)
    took(xt, x_sems.at[RECV])

    def turn(j, carry):
        hid[:, rows(j * LANES, LANES)] = xt[rows(j * LANES, LANES), :].T
        return carry
    lax.fori_loop(0, width // LANES, turn, 0)

    def vector(i, l):
        return vec[i * n_layers + l:i * n_layers + l + 1, :]

    def row_gather(sems):
        return RingGather(p, lambda chip, core, h: a_all.at[chip, rows(core * n_row + h * half_row, half_row)], sems)

    def order(n):
        return n + n // 2 - 2 * (n // 3)

    def each(n_from, n_to, body, hooks):
        def step(n, carry):
            for at_n, hook in hooks.items():
                @pl.when(n == at_n)
                def _():
                    for h in hook:
                        h()
            body(order(n))
            return carry
        lax.fori_loop(n_from, n_to, step, 0)

    def project(l, k):
        slot = p.chip(k)
        at_row = rows(slot * blk, blk)
        acc = jnp.dot(a_all[slot], w[...], preferred_element_type=F32)
        cos_t, sin_t = cs[0, at_row, :], cs[1, at_row, :]
        for i, bias in enumerate((bq_ref, bk_ref, bv_ref)):
            parts = []
            for h in range(loc_heads):
                lo = i * loc_w + h * head_w
                v = acc[:, lo:lo + head_w] + bias[l, h:h + 1, :].astype(F32)
                if i < 2:
                    v = v * cos_t + pltpu.roll(v, head_w // 2, 1) * sin_t
                v = v.astype(BF16)
                parts.append(v)
                if i < 2:
                    st[k, h, i] = v
                else:
                    sv[k, h] = v.T
            if i > 0:
                (kc, vc)[i - 1][l, at_row] = jnp.concatenate(parts, axis=1).reshape(blk, loc_heads, head_w)
        at_tok = rows((y * n_chip + slot) * blk, blk)
        par = lax.rem(slot, 2)
        at_q = rows((y * (n_chip // 2) + slot // 2) * blk, blk)
        for h in range(loc_heads):
            yd = c * loc_heads + h
            for r, (src, dst) in enumerate(((st.at[k, h, 1], kt.at[at_tok]), (sv.at[k, h], vt.at[:, at_tok]))):
                copy_or_send(jnp.logical_and(yd == y, c == r), src, dst, kv_sems.at[SEND], kv_sems.at[RECV], p.at(yd, x * 2 + r))
            copy_or_send(jnp.logical_and(yd == y, c == par), st.at[k, h, 0], qh.at[at_q], kv_sems.at[2], kv_sems.at[3],
                         p.at(yd, x * 2 + par))

    n_q = ob.shape[0]
    q_grp = 2 * blk
    n_grp = n_q * blk // q_grp
    n_sub = BK // blk

    def attend(hooks):
        def step(n, carry):
            grp = n_grp - 1 - n
            q = qh[rows(grp * q_grp, q_grp), :]
            q_col = lax.broadcasted_iota(jnp.int32, (1, blk), 1)
            at_q = [(2 * (2 * grp + i) + c) for i in range(2)]
            q_pos = jnp.concatenate([q_col + b * blk for b in at_q], axis=1)
            first = q_pos - jnp.concatenate([positions(b) for b in at_q], axis=1)
            key = lax.broadcasted_iota(jnp.int32, (blk, q_grp), 0)
            scale = head_w ** -0.5 * LOG2E

            def score(j, m, diag):
                s = lax.dot_general(kt[rows(j * BK, BK), :], q, (((1,), (1,)), ((), ())), preferred_element_type=F32)
                for i in range(n_sub):
                    k_pos = key + (j * BK + i * blk)
                    ok = k_pos >= first
                    if diag:
                        ok = jnp.logical_and(ok, k_pos <= q_pos)
                    part = jnp.where(ok, s[i * blk:(i + 1) * blk], -1e30)
                    full[j, :, i * q_grp:(i + 1) * q_grp] = part
                    m = jnp.maximum(m, jnp.max(part.reshape(blk // 8, 8, q_grp), axis=0))
                return m
            m = lax.fori_loop(0, grp, lambda j, m: score(j, m, False), jnp.full((8, q_grp), -1e30, F32))
            m = jnp.max(score(grp, m, True), axis=0, keepdims=True)

            def expo(j, t):
                for i in range(n_sub):
                    e = jnp.exp2((full[j, :, i * q_grp:(i + 1) * q_grp] - m) * scale)
                    full[j, :, i * q_grp:(i + 1) * q_grp] = e
                    t = t + jnp.sum(e.reshape(blk // 8, 8, q_grp), axis=0)
                return t
            t = lax.fori_loop(0, grp + 1, expo, jnp.zeros((8, q_grp), F32))
            inv = 1.0 / jnp.sum(t, axis=0, keepdims=True)

            def apply(j, acc):
                prob = jnp.concatenate([(full[j, :, i * q_grp:(i + 1) * q_grp] * inv).astype(BF16) for i in range(n_sub)], axis=0)
                return acc + jnp.dot(vt[:, rows(j * BK, BK)], prob, preferred_element_type=F32)
            out = lax.fori_loop(0, grp + 1, apply, jnp.zeros((head_w, q_grp), F32)).T.astype(BF16)
            cols_o = rows((x * num_tx + y) * head_w, head_w)
            for i, b in enumerate(at_q):
                ob[2 * grp + i] = out[i * blk:(i + 1) * blk]
                yt, xd = b // n_chip, lax.rem(b, n_chip)
                for r in range(2):
                    here = jnp.logical_and(jnp.logical_and(yt == y, xd == x), c == r)
                    copy_or_send(here, ob.at[2 * grp + i, pl.ds(r * n_row, n_row)], obuf.at[:, cols_o], o_sems.at[SEND],
                                 o_sems.at[RECV], p.at(yt, xd * 2 + r))
            for at_n, hook in hooks.items():
                @pl.when(n == at_n)
                def _():
                    for h in hook:
                        h()
            return carry
        lax.fori_loop(0, n_grp, step, 0)

    def up(l, k, n):
        half = wu.shape[1] // 2
        cc = pl.ds(n * half, half)
        h = jnp.dot(a_all[p.chip(k)], wu[:, cc], preferred_element_type=F32) + bup[l:l + 1, cc]
        g[k, :, cc] = gelu_tanh(h).astype(BF16)

    half_col = col_w // 2
    below, above, far_side = p.side(num_tx - 1), p.side(1), p.side(2)
    blocks = (((y, 0), (y, 1)), ((below, 0), (above, 1)), ((below, 1), (above, 0)), ((far_side, 0), (far_side, 1)))
    cols = [[rows(t * col_w + h * half_col, half_col) for t, h in pair] for pair in blocks]
    top, bottom = rows(c * n_row, half_row), rows(c * n_row + half_row, half_row)

    def to_sibling(k, j):
        out = []
        for i in range(2):
            at_s = (k * num_tx + j) * 2 + i
            out.append(remote(full.at[k, other, cols[j][i]], sibin.at[k, :, cols[j][i]], p_sems.at[SEND, at_s], p_sems.at[RECV, at_s],
                              p.sib))
        return out

    def rs(kind, j):
        k, part, dst, to = ((1, bottom, fin.at[0], p.right), (last, top, fin.at[1], p.left), (2, top, far_in.at[0], p.right),
                            (2, bottom, far_in.at[1], p.left), (1, top, fin.at[2], p.right),
                            (last, bottom, fin.at[3], p.left))[kind]
        out = []
        for i in range(2):
            at_s = (kind * num_tx + j) * 2 + i
            out.append(remote(full.at[k, part, cols[j][i]], dst.at[:, cols[j][i]], r_sems.at[SEND, at_s], r_sems.at[RECV, at_s], to))
        return out

    def start(copies):
        for cp in copies:
            cp.start()

    def landed(copies):
        for cp in copies:
            cp.wait_recv()

    def partial(k, j):
        for i, (t, h) in enumerate(blocks[j]):
            full[k, :, cols[j][i]] = jnp.dot(g[k], wd[t, :, h * half_col:(h + 1) * half_col], preferred_element_type=F32)
        start(to_sibling(k, j))

    def pair_sum(k, j):
        landed(to_sibling(k, j))
        for cc in cols[j]:
            full[k, mine, cc] = full[k, mine, cc] + sibin[k, :, cc]

    def send_near(j):
        pair_sum(1, j)
        start(rs(S_DIRECT_R, j))
        pair_sum(last, j)
        start(rs(S_DIRECT_L, j))

    def send_far(j):
        pair_sum(2, j)
        start(rs(S_FAR_R, j))
        start(rs(S_FAR_L, j))
        pair_sum(0, j)

    def pass_on(j):
        landed(rs(S_FAR_R, j))
        for cc in cols[j]:
            full[1, top, cc] = full[1, top, cc] + far_in[0, :, cc]
        start(rs(S_SUM_R, j))
        landed(rs(S_FAR_L, j))
        for cc in cols[j]:
            full[last, bottom, cc] = full[last, bottom, cc] + far_in[1, :, cc]
        start(rs(S_SUM_L, j))

    def complete(l, j):
        for kind in (S_DIRECT_R, S_DIRECT_L, S_SUM_R, S_SUM_L):
            landed(rs(kind, j))
        for cc in cols[j]:
            bias = vec[5 * n_layers + l:5 * n_layers + l + 1, cc]
            for part, out, ins in ((top, pl.ds(0, half_row), (1, 2)), (bottom, pl.ds(half_row, half_row), (0, 3))):
                tot = full[0, part, cc] + fin[ins[0], :, cc] + fin[ins[1], :, cc]
                hid[out, cc] = (hid[out, cc].astype(F32) + tot + bias).astype(BF16)

    def give_back(j):
        for t, h in blocks[j]:
            for n in range(half_col // LANES):
                at_c = rows(t * col_w + h * half_col + n * LANES, LANES)
                xt[at_c, :] = hid[:, at_c].T
            for k in range(num_ty // 2):
                to_ty = h * (num_ty // 2) + k
                copy_or_send(jnp.logical_and(t == y, ty == to_ty), xt.at[rows((t * num_ty + to_ty) * piece_w, piece_w)],
                             yt_hbm.at[:, rows(p.me * n_row, n_row)], y_sems.at[SEND], y_sems.at[RECV], p.at(t, to_ty))

    def start_forward():
        @pl.when(c == 0)
        def _():
            remote(kt, kt, kv_sems.at[4], kv_sems.at[5], p.sib).start()

        @pl.when(c != 0)
        def _():
            remote(vt, vt, kv_sems.at[4], kv_sems.at[5], p.sib).start()

    for l in range(n_layers):
        first_layer, last_layer = l == 0, l == n_layers - 1
        a_all[x, mine, :] = rows_norm(hid[...].astype(F32), vector(0, l), vector(1, l))
        ga = row_gather(a_sems)
        ga.start()
        ahead = [] if last_layer else [g_o[l + 1].relay]
        if first_layer:
            g_o[l].relay()
            g_qkv[l].start_second()
            ga.relay()
            g_qkv[l].relay()
            if not last_layer:
                g_o[l + 1].start()
            ga.own()
            ga.near()
            g_o[l].finish()
            s_o[l].start()
            ga.near_right()
            ga.near_left()
            ga.far()
            ga.far_done()
            ga.drain()
            g_qkv[l].finish()
            each(0, n_chip, lambda k: project(l, k), {2: ahead})
            s_o[l].relay()
        else:
            if not last_layer:
                g_o[l + 1].start()
            ga.relay()
            ga.own()
            s_o[l].start_second()
            s_o[l].relay()
            g_qkv[l].finish()
            each(0, last, lambda k: project(l, k), {1: [ga.near, ga.near_right, ga.near_left], 2: ahead})
            ga.far()
            ga.far_done()
            ga.drain()
            project(l, 2)
        for i, (src, dst) in enumerate(((kc, kc_hbm), (vc, vc_hbm))):
            pltpu.make_async_copy(src.at[l], dst.at[l], c_sems.at[i]).start()
        if not last_layer:
            g_o[l + 1].finish()
            s_o[l + 1].start_first()
        sent_away(p, kt, qh, kv_sems, loc_heads)
        g_up[l].start_first()
        took(kt, kv_sems.at[RECV])
        start_forward()
        took(qh, kv_sems.at[3])
        took(kt, kv_sems.at[5])
        took(kt, kv_sems.at[4])
        attend({0: [s_o[l].near]})
        g_up[l].relay([0])
        g_up[l].start_second()
        g_up[l].relay([1])
        g_qkv[l].drain()
        g_down[l].start()
        s_o[l].far()
        s_o[l].own()
        s_o[l].near_right()
        s_o[l].near_left()
        s_o[l].far_done()
        load_o = [] if first_layer else [pltpu.make_async_copy(whole_o(l).at[t], wo.at[t], l_sems.at[t]) for t in range(num_tx)]
        for ld in load_o:
            ld.start()
        took(obuf, o_sems.at[RECV])
        for ld in load_o:
            ld.wait()

        def out_product(t, carry):
            cc = rows(t * col_w, col_w)
            bias = vec[4 * n_layers + l:4 * n_layers + l + 1, cc]
            hid[:, cc] = (hid[:, cc].astype(F32) + jnp.dot(obuf[...], wo[t], preferred_element_type=F32) + bias).astype(BF16)
            return carry
        lax.fori_loop(0, num_tx, out_product, 0)
        a_all[x, mine, :] = rows_norm(hid[...].astype(F32), vector(2, l), vector(3, l))
        gu = row_gather(u_sems)
        gu.start()
        if first_layer:
            took(bup, b_sems.at[RECV])
        gu.own()
        gu.relay()
        g_up[l].piece(0)
        each(0, last, lambda k: up(l, k, 0), {1: [gu.near, gu.near_right, gu.near_left]})
        if not first_layer:
            gu.far()
            gu.far_done()
            up(l, 2, 0)
        g_up[l].piece(1)
        g_down[l].step(0)

        def near_partial(n, carry):
            up(l, order(n), 1)
            partial(order(n), 0)
            return carry
        lax.fori_loop(1, last, near_partial, 0)
        if first_layer:
            gu.far()
            gu.far_done()
            up(l, 2, 0)
        up(l, 2, 1)
        gu.drain()
        s_o[l].drain()
        g_o[l].drain()
        g_up[l].drain()
        send_near(0)
        partial(2, 0)
        up(l, 0, 1)
        partial(0, 0)
        g_down[l].relay()
        if not last_layer:
            g_qkv[l + 1].start()
        send_far(0)
        for j in range(1, num_tx):
            g_down[l].step(j)

            def each_partial(n, carry):
                partial(order(lax.rem(n + 1, n_chip)), j)
                return carry
            lax.fori_loop(0, n_chip, each_partial, 0)
            send_near(j)
            send_far(j)
            pass_on(j - 1)
            if j > 1:
                complete(l, j - 2)
                if last_layer:
                    give_back(j - 2)
        pass_on(num_tx - 1)
        if not last_layer:
            g_qkv[l + 1].relay()
        for j in range(num_tx - 2, num_tx):
            complete(l, j)
            if last_layer:
                give_back(j)
        for j in range(num_tx):
            for k in range(n_chip):
                for cp in to_sibling(k, j):
                    cp.wait_send()
            for kind in range(6):
                for cp in rs(kind, j):
                    cp.wait_send()
        g_down[l].drain()
        o_away(p, obuf, o_sems, head_w)

    took(kc_hbm, c_sems.at[SEND])
    took(vc_hbm, c_sems.at[RECV])
    took(xt_hbm.at[:, pl.ds(0, (n_dev - 1) * n_row)], x_sems.at[SEND])
    took(vbuf.at[pl.ds(0, n_dev - 1)], v_sems.at[SEND])
    took(bup.at[:, pl.ds(0, (num_tx - 1) * bup_w)], b_sems.at[SEND])
    took(yt_hbm, y_sems.at[RECV])
    took(xt.at[pl.ds(0, (n_dev - 1) * piece_w)], y_sems.at[SEND])


def sent_away(p, kt, qh, kv_sems, loc_heads):
    stays = p.c == p.y // loc_heads
    n_tok = kt.shape[0]
    n_q = qh.shape[0]

    @pl.when(stays)
    def _():
        took(kt.at[pl.ds(0, n_tok * 3 // 4)], kv_sems.at[SEND])
        took(qh.at[pl.ds(0, n_q * 3 // 4)], kv_sems.at[2])

    @pl.when(jnp.logical_not(stays))
    def _():
        took(kt, kv_sems.at[SEND])
        took(qh, kv_sems.at[2])


def o_away(p, obuf, o_sems, head_w):
    stays = lax.rem(p.x, 2) == p.c

    @pl.when(stays)
    def _():
        took(obuf.at[:, pl.ds(0, obuf.shape[1] - head_w)], o_sems.at[SEND])

    @pl.when(jnp.logical_not(stays))
    def _():
        took(obuf, o_sems.at[SEND])


def decoder(num_tx, num_ty, xt, vectors, b_up, b_qkv, pos, wq, wk, wv, wo, wu, wd):
    n_layers, d_rows, loc_heads, head_w = wq.shape
    n_dev = num_tx * num_ty
    n_chip = num_ty // 2
    piece_w, n_tok = xt.shape
    width = piece_w * n_dev
    n_row = n_tok // n_dev
    blk = 2 * n_row
    loc_w = loc_heads * head_w
    tok_loc = n_tok // num_tx
    ff = wu.shape[2]
    col_w = wd.shape[2]
    n_q = n_tok // (2 * blk)
    n_vec = -(-len(vectors) * n_layers // 16) * 16
    vm = pl.BlockSpec(memory_space=pltpu.VMEM)
    hb = pl.BlockSpec(memory_space=pl.ANY)
    V = pltpu.VMEM
    dma = pltpu.SemaphoreType.DMA
    ends = dma((2,))
    cache = jax.ShapeDtypeStruct((n_layers, tok_loc, loc_heads, head_w), BF16)
    CG, RG = ColumnGather.SEMS, RingGather.SEMS
    return pl.pallas_call(
        functools.partial(decoder_kernel, num_tx, num_ty, n_layers),
        out_shape=(jax.ShapeDtypeStruct((piece_w, n_tok), BF16), cache, cache,
                   jax.ShapeDtypeStruct((max(n_layers - 1, 1), num_tx, width, col_w), BF16)),
        in_specs=[hb] + [vm] * 10 + [hb] * 7,
        out_specs=(hb,) * 4,
        scratch_shapes=[V((n_tok,), jnp.int32), V((width, n_row), BF16), V((n_vec, LANES), F32), V((n_vec, LANES), BF16), V((n_dev, n_vec, LANES), BF16),
                        V((n_vec, width), F32), V((8, b_up.shape[1]), F32), V((8, ff), F32),
                        V((3, d_rows, loc_heads, head_w), BF16), V((n_layers, 3, d_rows, loc_w), BF16),
                        V((width, 3 * loc_w), BF16), V((width, ff), BF16), V((num_tx, ff, col_w), BF16),
                        V((num_tx, width, col_w), BF16), V((2, tok_loc, head_w), F32),
                        V((n_chip, blk, width), BF16), V((n_row, width), BF16),
                        V((n_chip, loc_heads, 2, blk, head_w), BF16), V((n_chip, loc_heads, head_w, blk), BF16), V(cache.shape, BF16),
                        V(cache.shape, BF16),
                        V((n_tok, head_w), BF16), V((head_w, n_tok), BF16), V((n_q * blk, head_w), BF16),
                        V((n_q, blk, head_w), BF16), V((n_row, width), BF16), V((n_chip, blk, ff), BF16),
                        V((n_chip, blk, width), F32), V((n_chip, n_row, width), F32),
                        V((2, n_row // 2, width), F32), V((4, n_row // 2, width), F32),
                        ends, ends, ends, ends, dma((2, RG)), dma((2, RG)), dma((2, 3 * CG)),
                        dma((n_layers, 2, CG)), dma((n_layers, 2, RG)), dma((2, 2 * CG)), dma((2, CG)), dma((6,)), ends, dma((2, 2 * n_chip * num_tx)),
                        dma((2, 12 * num_tx)), dma((4,)), ends],
        compiler_params=pltpu.CompilerParams(collective_id=1, has_side_effects=True, vmem_limit_bytes=63 << 20),
        name="decoder",
    )(xt, *vectors, b_up, *b_qkv, pos, wq, wk, wv, wo, wu, wd)[:3]


def hand_over_kernel(n, *refs):
    src, dst, buf, sems = refs[:n], refs[n:2 * n], refs[2 * n:3 * n], refs[3 * n]
    copies = []
    for i in range(n):
        step = src[i].shape[0] // 2
        for h in range(2):
            part = pl.ds(h * step, step)
            copies.append((pltpu.make_async_copy(src[i].at[part], buf[i].at[part], sems.at[SEND, 2 * i + h]),
                           pltpu.make_async_copy(buf[i].at[part], dst[i].at[part], sems.at[RECV, 2 * i + h])))
    for load, _ in copies:
        load.start()
    for load, store in copies:
        load.wait()
        store.start()
    for _, store in copies:
        store.wait()


def hand_over(arrays):
    n = len(arrays)
    hb = pl.BlockSpec(memory_space=pl.ANY)
    return pl.pallas_call(
        functools.partial(hand_over_kernel, n),
        out_shape=tuple(jax.ShapeDtypeStruct(a.shape, a.dtype) for a in arrays),
        in_specs=[hb] * n,
        out_specs=(hb,) * n,
        scratch_shapes=[pltpu.VMEM(a.shape, a.dtype) for a in arrays] + [pltpu.SemaphoreType.DMA((2, 2 * n))],
        name="hand_over",
    )(*arrays)


def solution(mesh):
    num_tx = mesh.shape['tx']
    num_ty = mesh.shape['ty']
    width_spec = P('dp', ('tx', 'ty'))
    vec_spec = P(None, ('tx', 'ty'))
    proj_spec = P(None, 'tx', 'ty', None)
    head_spec = P(None, 'ty', None)
    cache_spec = P(None, ('dp', 'tx'), 'ty', None)
    in_specs = (width_spec, P('dp'), P('dp'), vec_spec, vec_spec, proj_spec, head_spec, proj_spec, head_spec,
                proj_spec, head_spec, P(None, 'ty', None, 'tx'), vec_spec, vec_spec, vec_spec,
                P(None, 'tx', 'ty'), P(None, ('ty', 'tx')), P(None, 'ty', 'tx'), vec_spec)
    out_specs = (width_spec, cache_spec, cache_spec)

    def device_fn(x_loc, seg_all, pos_all, ln1_gain, ln1_bias, w_q, b_q, w_k, b_k, w_v, b_v, w_o, b_o,
                  ln2_gain, ln2_bias, w_up, b_up, w_down, b_down):
        yt, k, v = decoder(num_tx, num_ty, x_loc.T, (ln1_gain, ln1_bias, ln2_gain, ln2_bias, b_o, b_down), b_up,
                           (b_q, b_k, b_v), pos_all, w_q, w_k, w_v,
                           w_o.reshape(w_o.shape[0], -1, w_o.shape[-1]), w_up, w_down)
        yt, k, v = hand_over((yt, k, v))
        return yt.T, k, v

    return jax.shard_map(device_fn, mesh=mesh, in_specs=in_specs, out_specs=out_specs, check_vma=False)
```

```python
import math
import functools
import jax
import jax.numpy as jnp
from jax import lax
from jax.experimental import pallas as pl
from jax.experimental.pallas import tpu as pltpu
from jax.sharding import PartitionSpec as P

MESH = pl.DeviceIdType.MESH
F32 = jnp.float32
BF16 = jnp.bfloat16
ROPE_THETA = 100000.0
LOG2E = 1.4426950408889634
LANES = 128
BK = 1024
SEND, RECV = 0, 1


def rows_norm(x_f32, gain, bias):
    width = x_f32.shape[-1]
    mean = jnp.sum(x_f32, axis=-1, keepdims=True) / width
    var = jnp.sum(x_f32 * x_f32, axis=-1, keepdims=True) / width - mean * mean
    normed = (x_f32 - mean) * lax.rsqrt(var + 1e-5)
    return (normed * gain + bias).astype(BF16)


def gelu_tanh(x):
    return 0.5 * x * (1.0 + jnp.tanh(0.7978845608028654 * (x + 0.044715 * (x * x * x))))


def rows(at, n):
    return pl.ds(pl.multiple_of(at, n), n)


class Place:
    def __init__(self, num_tx, num_ty):
        self.num_tx, self.num_ty, self.n_chip = num_tx, num_ty, num_ty // 2
        self.y = lax.axis_index('tx')
        self.ty = lax.axis_index('ty')
        self.x = self.ty // 2
        self.c = lax.rem(self.ty, 2)
        self.me = self.y * num_ty + self.ty
        self.sib = self.at(self.y, self.x * 2 + 1 - self.c)
        self.right, self.left = self.beside(1), self.beside(self.n_chip - 1)
        self.above, self.below = self.over(1), self.over(num_tx - 1)

    def at(self, y, ty):
        return {'tx': y, 'ty': ty}

    def chip(self, k):
        return lax.rem(self.x + k, self.n_chip)

    def side(self, k):
        return lax.rem(self.y + k, self.num_tx)

    def beside(self, k):
        return self.at(self.y, self.chip(k) * 2 + self.c)

    def over(self, k):
        return self.at(self.side(k), self.ty)


def remote(src, dst, send_sem, recv_sem, to):
    return pltpu.make_async_remote_copy(src_ref=src, dst_ref=dst, send_sem=send_sem, recv_sem=recv_sem, device_id=to,
                                        device_id_type=MESH)


def copy_or_send(here, src, dst, send_sem, recv_sem, to):
    @pl.when(here)
    def _():
        pltpu.make_async_copy(src, dst, recv_sem).start()

    @pl.when(jnp.logical_not(here))
    def _():
        remote(src, dst, send_sem, recv_sem, to).start()


def took(ref, sem):
    pltpu.make_async_copy(ref, ref, sem).wait()


class RingGather:
    SEMS = 14

    def __init__(self, p, view, sems):
        self.p = p
        self.view = view
        self.sems = sems
        x, c, d = p.x, p.c, 1 - p.c
        far, left, right = p.chip(2), p.chip(p.n_chip - 1), p.chip(1)
        self.plan = [(x, 0, p.right, left), (x, 1, p.left, right), (x, 1, p.right, left), (x, 0, p.left, right),
                     (left, 0, p.right, far), (right, 1, p.left, far),
                     (x, 0, p.sib, x), (x, 1, p.sib, x), (left, 0, p.sib, left), (left, 1, p.sib, left),
                     (right, 0, p.sib, right), (right, 1, p.sib, right), (far, 0, p.sib, far), (far, 1, p.sib, far)]

    def out(self, i):
        chip, half, to, _ = self.plan[i]
        ref = self.view(chip, self.p.c, half)
        return remote(ref, ref, self.sems.at[SEND, i], self.sems.at[RECV, i], to)

    def arrived(self, i):
        _, half, to, chip = self.plan[i]
        core = self.p.c if i < 6 else 1 - self.p.c
        ref = self.view(chip, core, half)
        remote(ref, ref, self.sems.at[SEND, i], self.sems.at[RECV, i], to).wait_recv()

    def start_first(self):
        for i in (6, 7, 0, 1):
            self.out(i).start()

    def start_second(self):
        for i in (2, 3):
            self.out(i).start()

    def start(self):
        self.start_first()
        self.start_second()

    def own(self):
        self.arrived(6)
        self.arrived(7)

    def relay(self):
        self.arrived(0)
        self.out(4).start()
        self.arrived(1)
        self.out(5).start()
        self.out(8).start()
        self.out(11).start()

    def near(self):
        self.arrived(2)
        self.out(9).start()
        self.arrived(3)
        self.out(10).start()

    def near_right(self):
        self.arrived(10)
        self.arrived(11)

    def near_left(self):
        self.arrived(8)
        self.arrived(9)

    def far(self):
        self.arrived(4)
        self.out(12).start()
        self.arrived(5)
        self.out(13).start()

    def far_done(self):
        self.arrived(12)
        self.arrived(13)

    def drain(self):
        for i in range(self.SEMS):
            self.out(i).wait_send()


class ColumnGather:
    SEMS = 8

    def __init__(self, p, pieces, sems, early=0):
        self.p = p
        self.pieces = pieces
        self.sems = sems
        self.early = early

    def copy(self, n, i):
        p = self.p
        src, dst = self.pieces[n]
        up, down = p.side(1), p.side(p.num_tx - 1)
        half, to = ((0, p.above), (1, p.below), (1, p.above), (0, p.below), (0, p.above), (1, p.below))[i]
        here = src(half) if i < 4 else dst(down if i == 4 else up, half)
        there = dst((p.y, p.y, p.y, p.y, down, up)[i], half)
        return remote(here, there, self.sems.at[SEND, n * self.SEMS + i], self.sems.at[RECV, n * self.SEMS + i], to)

    def arrived(self, n, i):
        p = self.p
        src, dst = self.pieces[n]
        up, down, far = p.side(1), p.side(p.num_tx - 1), p.side(2)
        half, frm = ((0, down), (1, up), (1, down), (0, up), (0, far), (1, far))[i]
        remote(src(half), dst(frm, half), self.sems.at[SEND, n * self.SEMS + i], self.sems.at[RECV, n * self.SEMS + i],
               p.above).wait_recv()

    def own(self, n, half):
        src, dst = self.pieces[n]
        return pltpu.make_async_copy(src(half), dst(self.p.y, half), self.sems.at[RECV, n * self.SEMS + 6 + half])

    def start_piece(self, n):
        for i in (0, 1):
            self.copy(n, i).start()

    def start_first(self, n_from=0):
        for i in (0, 1):
            for n in range(n_from, len(self.pieces)):
                self.copy(n, i).start()
        self.rest(range(self.early))

    def start_second(self):
        self.rest(range(self.early, len(self.pieces)))

    def rest(self, which):
        for i in (2, 3):
            for n in which:
                self.copy(n, i).start()
        for n in which:
            self.own(n, 0).start()
            self.own(n, 1).start()

    def start(self):
        self.start_first()
        self.start_second()

    def relay(self, which=None):
        for n in range(len(self.pieces)) if which is None else which:
            self.arrived(n, 0)
            self.copy(n, 4).start()
            self.arrived(n, 1)
            self.copy(n, 5).start()

    def step(self, j, which=None):
        for n in range(len(self.pieces)) if which is None else which:
            if j == 0:
                self.own(n, 0).wait()
                self.own(n, 1).wait()
            elif j > 1:
                self.arrived(n, 2 * j - 2)
                self.arrived(n, 2 * j - 1)

    def piece(self, n):
        for j in range(4):
            self.step(j, [n])

    def finish(self):
        for j in range(4):
            self.step(j)

    def drain(self):
        for n in range(len(self.pieces)):
            for i in range(6):
                self.copy(n, i).wait_send()


S_DIRECT_R, S_DIRECT_L, S_FAR_R, S_FAR_L, S_SUM_R, S_SUM_L = range(6)


def decoder_kernel(num_tx, num_ty, n_layers,
                   xt_hbm, g1_ref, b1_ref, g2_ref, b2_ref, bo_ref, bd_ref, bup_ref, bq_ref, bk_ref, bv_ref, pos_hbm,
                   wq_hbm, wk_hbm, wv_hbm, wo_hbm, wu_hbm, wd_hbm,
                   yt_hbm, kc_hbm, vc_hbm, go_hbm,
                   pos, xt, vrow, vloc, vbuf, vec, bloc, bup, raw, ws, w, wu, wd, wo, cs, a_all, hid, st, sv, kc, vc, kt, vt, qh, ob, obuf,
                   g, full, sibin, far_in, fin,
                   x_sems, v_sems, b_sems, y_sems, a_sems, u_sems, wq_sems, wo_sems, wx_sems, wu_sems, wd_sems,
                   kv_sems, o_sems, p_sems, r_sems, l_sems, c_sems):
    p = Place(num_tx, num_ty)
    n_dev = num_tx * num_ty
    n_chip, x, y, c, ty = p.n_chip, p.x, p.y, p.c, p.ty
    n_row, width = hid.shape
    blk = 2 * n_row
    half_row = n_row // 2
    loc_heads, head_w = wq_hbm.shape[2], wq_hbm.shape[3]
    loc_w = loc_heads * head_w
    col_w = wd.shape[2]
    piece_w = xt_hbm.shape[0]
    last = n_chip - 1
    mine, other = rows(c * n_row, n_row), rows((1 - c) * n_row, n_row)

    barrier = pltpu.get_barrier_semaphore()
    ids = [lax.rem(p.me + k, n_dev) for k in range(1, n_dev)]
    devs = [p.at(d // num_ty, lax.rem(d, num_ty)) for d in ids]
    for to in devs:
        pl.semaphore_signal(barrier, inc=1, device_id=to, device_id_type=MESH)

    def load_raw(l):
        return [pltpu.make_async_copy(src.at[l], raw.at[i], l_sems.at[i]) for i, src in enumerate((wq_hbm, wk_hbm, wv_hbm))]

    def flatten(l):
        for i, ld in enumerate(load_raw(l)):
            ld.wait()
            ws[l, i] = raw[i].reshape(ws.shape[2], loc_w)
    for ld in load_raw(0):
        ld.start()
    load_pos = pltpu.make_async_copy(pos_hbm, pos, l_sems.at[3])
    load_pos.start()
    vrow[...] = jnp.zeros_like(vrow)
    for i, ref in enumerate((g1_ref, b1_ref, g2_ref, b2_ref, bo_ref, bd_ref)):
        vrow[i * n_layers:(i + 1) * n_layers, :piece_w] = ref[...].astype(F32)
    vloc[...] = vrow[...].astype(BF16)
    bloc[...] = jnp.zeros_like(bloc)
    bloc[:n_layers, :] = bup_ref[...].astype(F32)
    pl.semaphore_wait(barrier, n_dev - 1)

    def halves(ref, l, n):
        return lambda h: ref.at[l, pl.ds(h * n, n)]

    def shard_rows(dst, n_shard, n, at_cols):
        return lambda ys, h: dst.at[rows(ys * n_shard + h * n, n), at_cols]

    qkv_rows = ws.shape[2]
    up_rows = wu_hbm.shape[1]
    o_rows = wo_hbm.shape[1]

    def gather_qkv(l):
        n = qkv_rows // 2
        return ColumnGather(p, [((lambda h, i=i: ws.at[l, i, pl.ds(h * n, n)]),
                                 shard_rows(w, qkv_rows, n, pl.ds(i * loc_w, loc_w))) for i in range(3)], wq_sems)

    def gather_up(l):
        n, half = up_rows // 2, wu.shape[1] // 2
        return ColumnGather(p, [((lambda h, at_c=at_c: wu_hbm.at[l, pl.ds(h * n, n), at_c]), shard_rows(wu, up_rows, n, at_c))
                                for at_c in (pl.ds(0, half), pl.ds(half, half))], wu_sems, early=1)

    def gather_down(l):
        n = col_w // 2
        return ColumnGather(p, [((lambda h: wd_hbm.at[l, :, pl.ds(h * n, n)]), lambda ys, h: wd.at[ys, :, pl.ds(h * n, n)])],
                            wd_sems)

    def whole_o(l):
        return wo if l == 0 else go_hbm.at[l - 1]

    def gather_o(l):
        n = o_rows // 2
        return ColumnGather(p, [(halves(wo_hbm, l, n), lambda ys, h: whole_o(l).at[ys, rows(ty * o_rows + h * n, n)])],
                            wo_sems.at[l])

    def spread_o(l):
        n = num_tx // 2
        return RingGather(p, lambda chip, core, h: whole_o(l).at[pl.ds(h * n, n), rows((chip * 2 + core) * o_rows, o_rows)],
                          wx_sems.at[l])

    g_qkv = [gather_qkv(l) for l in range(n_layers)]
    g_up = [gather_up(l) for l in range(n_layers)]
    g_down = [gather_down(l) for l in range(n_layers)]
    g_o = [gather_o(l) for l in range(n_layers)]
    s_o = [spread_o(l) for l in range(n_layers)]

    for k in range(1, num_tx):
        remote(vloc, vbuf.at[y, ty], v_sems.at[SEND], v_sems.at[RECV], p.over(k)).start()
    for d, to in zip(ids, devs):
        remote(xt_hbm.at[:, rows(d * n_row, n_row)], xt.at[rows(p.me * piece_w, piece_w)], x_sems.at[SEND], x_sems.at[RECV], to).start()
    g_o[0].start()
    flatten(0)
    g_qkv[0].start_first()
    pltpu.make_async_copy(xt_hbm.at[:, rows(p.me * n_row, n_row)], xt.at[rows(p.me * piece_w, piece_w)], x_sems.at[RECV]).start()
    pltpu.make_async_copy(vloc, vbuf.at[y, ty], v_sems.at[RECV]).start()
    bup_w = bup_ref.shape[1]
    for k in range(1, num_tx):
        remote(bloc, bup.at[:, rows(y * bup_w, bup_w)], b_sems.at[SEND], b_sems.at[RECV], p.over(k)).start()
    pltpu.make_async_copy(bloc, bup.at[:, rows(y * bup_w, bup_w)], b_sems.at[RECV]).start()
    column = vbuf.at[:, ty]
    took(column, v_sems.at[RECV])
    for k in range(1, num_ty):
        remote(column, column, v_sems.at[2], v_sems.at[3], p.at(y, lax.rem(ty + k, num_ty))).start()
    for l in range(1, n_layers):
        for ld in load_raw(l):
            ld.start()
        flatten(l)

    load_pos.wait()
    lane = lax.broadcasted_iota(jnp.int32, (1, head_w), 1)
    inv_freq = jnp.exp(lax.rem(lane, head_w // 2).astype(F32) * (-2.0 * math.log(ROPE_THETA) / head_w))
    sign = jnp.where(lane < head_w // 2, -1.0, 1.0)

    def positions(b):
        return pos[rows(b * blk, blk)].reshape(1, blk)

    def angles(k, carry):
        ang = jnp.broadcast_to(positions(y * n_chip + k).astype(F32), (head_w, blk)).T * inv_freq
        cs[0, rows(k * blk, blk), :] = jnp.cos(ang)
        cs[1, rows(k * blk, blk), :] = jnp.sin(ang) * sign
        return carry
    lax.fori_loop(0, n_chip, angles, 0)
    took(vbuf.at[:, pl.ds(1, num_ty - 1)], v_sems.at[3])
    per = LANES // piece_w
    for j in range(width // LANES):
        vec[:, j * LANES:(j + 1) * LANES] = jnp.concatenate(
            [vbuf[(per * j + i) // num_ty, (per * j + i) % num_ty][:, :piece_w].astype(F32) for i in range(per)], axis=1)
    took(xt, x_sems.at[RECV])

    def turn(j, carry):
        hid[:, rows(j * LANES, LANES)] = xt[rows(j * LANES, LANES), :].T
        return carry
    lax.fori_loop(0, width // LANES, turn, 0)

    def vector(i, l):
        return vec[i * n_layers + l:i * n_layers + l + 1, :]

    def row_gather(sems):
        return RingGather(p, lambda chip, core, h: a_all.at[chip, rows(core * n_row + h * half_row, half_row)], sems)

    def order(n):
        return n + n // 2 - 2 * (n // 3)

    def each(n_from, n_to, body, hooks):
        def step(n, carry):
            for at_n, hook in hooks.items():
                @pl.when(n == at_n)
                def _():
                    for h in hook:
                        h()
            body(order(n))
            return carry
        lax.fori_loop(n_from, n_to, step, 0)

    def project(l, k):
        slot = p.chip(k)
        at_row = rows(slot * blk, blk)
        acc = jnp.dot(a_all[slot], w[...], preferred_element_type=F32)
        cos_t, sin_t = cs[0, at_row, :], cs[1, at_row, :]
        for i, bias in enumerate((bq_ref, bk_ref, bv_ref)):
            parts = []
            for h in range(loc_heads):
                lo = i * loc_w + h * head_w
                v = acc[:, lo:lo + head_w] + bias[l, h:h + 1, :].astype(F32)
                if i < 2:
                    v = v * cos_t + pltpu.roll(v, head_w // 2, 1) * sin_t
                v = v.astype(BF16)
                parts.append(v)
                if i < 2:
                    st[k, h, i] = v
                else:
                    sv[k, h] = v.T
            if i > 0:
                (kc, vc)[i - 1][l, at_row] = jnp.concatenate(parts, axis=1).reshape(blk, loc_heads, head_w)
        at_tok = rows((y * n_chip + slot) * blk, blk)
        par = lax.rem(slot, 2)
        at_q = rows((y * (n_chip // 2) + slot // 2) * blk, blk)
        for h in range(loc_heads):
            yd = c * loc_heads + h
            for r, (src, dst) in enumerate(((st.at[k, h, 1], kt.at[at_tok]), (sv.at[k, h], vt.at[:, at_tok]))):
                copy_or_send(jnp.logical_and(yd == y, c == r), src, dst, kv_sems.at[SEND], kv_sems.at[RECV], p.at(yd, x * 2 + r))
            copy_or_send(jnp.logical_and(yd == y, c == par), st.at[k, h, 0], qh.at[at_q], kv_sems.at[2], kv_sems.at[3],
                         p.at(yd, x * 2 + par))

    n_q = ob.shape[0]
    q_grp = 2 * blk
    n_grp = n_q * blk // q_grp
    n_sub = BK // blk

    def attend(hooks):
        def step(n, carry):
            grp = n_grp - 1 - n
            q = qh[rows(grp * q_grp, q_grp), :]
            q_col = lax.broadcasted_iota(jnp.int32, (1, blk), 1)
            at_q = [(2 * (2 * grp + i) + c) for i in range(2)]
            q_pos = jnp.concatenate([q_col + b * blk for b in at_q], axis=1)
            first = q_pos - jnp.concatenate([positions(b) for b in at_q], axis=1)
            key = lax.broadcasted_iota(jnp.int32, (blk, q_grp), 0)
            scale = head_w ** -0.5 * LOG2E

            def score(j, m, diag):
                s = lax.dot_general(kt[rows(j * BK, BK), :], q, (((1,), (1,)), ((), ())), preferred_element_type=F32)
                for i in range(n_sub):
                    k_pos = key + (j * BK + i * blk)
                    ok = k_pos >= first
                    if diag:
                        ok = jnp.logical_and(ok, k_pos <= q_pos)
                    part = jnp.where(ok, s[i * blk:(i + 1) * blk], -1e30)
                    full[j, :, i * q_grp:(i + 1) * q_grp] = part
                    m = jnp.maximum(m, jnp.max(part.reshape(blk // 8, 8, q_grp), axis=0))
                return m
            m = lax.fori_loop(0, grp, lambda j, m: score(j, m, False), jnp.full((8, q_grp), -1e30, F32))
            m = jnp.max(score(grp, m, True), axis=0, keepdims=True)

            def expo(j, t):
                for i in range(n_sub):
                    e = jnp.exp2((full[j, :, i * q_grp:(i + 1) * q_grp] - m) * scale)
                    full[j, :, i * q_grp:(i + 1) * q_grp] = e
                    t = t + jnp.sum(e.reshape(blk // 8, 8, q_grp), axis=0)
                return t
            t = lax.fori_loop(0, grp + 1, expo, jnp.zeros((8, q_grp), F32))
            inv = 1.0 / jnp.sum(t, axis=0, keepdims=True)

            def apply(j, acc):
                prob = jnp.concatenate([(full[j, :, i * q_grp:(i + 1) * q_grp] * inv).astype(BF16) for i in range(n_sub)], axis=0)
                return acc + jnp.dot(vt[:, rows(j * BK, BK)], prob, preferred_element_type=F32)
            out = lax.fori_loop(0, grp + 1, apply, jnp.zeros((head_w, q_grp), F32)).T.astype(BF16)
            cols_o = rows((x * num_tx + y) * head_w, head_w)
            for i, b in enumerate(at_q):
                ob[2 * grp + i] = out[i * blk:(i + 1) * blk]
                yt, xd = b // n_chip, lax.rem(b, n_chip)
                for r in range(2):
                    here = jnp.logical_and(jnp.logical_and(yt == y, xd == x), c == r)
                    copy_or_send(here, ob.at[2 * grp + i, pl.ds(r * n_row, n_row)], obuf.at[:, cols_o], o_sems.at[SEND],
                                 o_sems.at[RECV], p.at(yt, xd * 2 + r))
            for at_n, hook in hooks.items():
                @pl.when(n == at_n)
                def _():
                    for h in hook:
                        h()
            return carry
        lax.fori_loop(0, n_grp, step, 0)

    def up(l, k, n):
        half = wu.shape[1] // 2
        cc = pl.ds(n * half, half)
        h = jnp.dot(a_all[p.chip(k)], wu[:, cc], preferred_element_type=F32) + bup[l:l + 1, cc]
        g[k, :, cc] = gelu_tanh(h).astype(BF16)

    half_col = col_w // 2
    below, above, far_side = p.side(num_tx - 1), p.side(1), p.side(2)
    blocks = (((y, 0), (y, 1)), ((below, 0), (above, 1)), ((below, 1), (above, 0)), ((far_side, 0), (far_side, 1)))
    cols = [[rows(t * col_w + h * half_col, half_col) for t, h in pair] for pair in blocks]
    top, bottom = rows(c * n_row, half_row), rows(c * n_row + half_row, half_row)

    def to_sibling(k, j):
        out = []
        for i in range(2):
            at_s = (k * num_tx + j) * 2 + i
            out.append(remote(full.at[k, other, cols[j][i]], sibin.at[k, :, cols[j][i]], p_sems.at[SEND, at_s], p_sems.at[RECV, at_s],
                              p.sib))
        return out

    def rs(kind, j):
        k, part, dst, to = ((1, bottom, fin.at[0], p.right), (last, top, fin.at[1], p.left), (2, top, far_in.at[0], p.right),
                            (2, bottom, far_in.at[1], p.left), (1, top, fin.at[2], p.right),
                            (last, bottom, fin.at[3], p.left))[kind]
        out = []
        for i in range(2):
            at_s = (kind * num_tx + j) * 2 + i
            out.append(remote(full.at[k, part, cols[j][i]], dst.at[:, cols[j][i]], r_sems.at[SEND, at_s], r_sems.at[RECV, at_s], to))
        return out

    def start(copies):
        for cp in copies:
            cp.start()

    def landed(copies):
        for cp in copies:
            cp.wait_recv()

    def partial(k, j):
        for i, (t, h) in enumerate(blocks[j]):
            full[k, :, cols[j][i]] = jnp.dot(g[k], wd[t, :, h * half_col:(h + 1) * half_col], preferred_element_type=F32)
        start(to_sibling(k, j))

    def pair_sum(k, j):
        landed(to_sibling(k, j))
        for cc in cols[j]:
            full[k, mine, cc] = full[k, mine, cc] + sibin[k, :, cc]

    def send_near(j):
        pair_sum(1, j)
        start(rs(S_DIRECT_R, j))
        pair_sum(last, j)
        start(rs(S_DIRECT_L, j))

    def send_far(j):
        pair_sum(2, j)
        start(rs(S_FAR_R, j))
        start(rs(S_FAR_L, j))

    def pass_on(j):
        for i, cc in enumerate(cols[j]):
            rs(S_FAR_R, j)[i].wait_recv()
            full[1, top, cc] = full[1, top, cc] + far_in[0, :, cc]
            rs(S_SUM_R, j)[i].start()
            rs(S_FAR_L, j)[i].wait_recv()
            full[last, bottom, cc] = full[last, bottom, cc] + far_in[1, :, cc]
            rs(S_SUM_L, j)[i].start()

    def complete(l, j):
        pair_sum(0, j)
        for kind in (S_DIRECT_R, S_DIRECT_L, S_SUM_R, S_SUM_L):
            landed(rs(kind, j))
        for cc in cols[j]:
            bias = vec[5 * n_layers + l:5 * n_layers + l + 1, cc]
            for part, out, ins in ((top, pl.ds(0, half_row), (1, 2)), (bottom, pl.ds(half_row, half_row), (0, 3))):
                tot = full[0, part, cc] + fin[ins[0], :, cc] + fin[ins[1], :, cc]
                hid[out, cc] = (hid[out, cc].astype(F32) + tot + bias).astype(BF16)

    def give_back(j):
        for t, h in blocks[j]:
            for n in range(half_col // LANES):
                at_c = rows(t * col_w + h * half_col + n * LANES, LANES)
                xt[at_c, :] = hid[:, at_c].T
            for k in range(num_ty // 2):
                to_ty = h * (num_ty // 2) + k
                copy_or_send(jnp.logical_and(t == y, ty == to_ty), xt.at[rows((t * num_ty + to_ty) * piece_w, piece_w)],
                             yt_hbm.at[:, rows(p.me * n_row, n_row)], y_sems.at[SEND], y_sems.at[RECV], p.at(t, to_ty))

    def start_forward():
        @pl.when(c == 0)
        def _():
            remote(kt, kt, kv_sems.at[4], kv_sems.at[5], p.sib).start()

        @pl.when(c != 0)
        def _():
            remote(vt, vt, kv_sems.at[4], kv_sems.at[5], p.sib).start()

    for l in range(n_layers):
        first_layer, last_layer = l == 0, l == n_layers - 1
        a_all[x, mine, :] = rows_norm(hid[...].astype(F32), vector(0, l), vector(1, l))
        ga = row_gather(a_sems)
        ga.start()
        ahead = [] if last_layer else [g_o[l + 1].relay]
        if first_layer:
            g_o[l].relay()
            g_qkv[l].start_second()
            ga.relay()
            g_qkv[l].relay()
            if not last_layer:
                g_o[l + 1].start()
            ga.own()
            ga.near()
            g_o[l].finish()
            s_o[l].start()
            ga.near_right()
            ga.near_left()
            ga.far()
            ga.far_done()
            ga.drain()
            g_qkv[l].finish()
            each(0, n_chip, lambda k: project(l, k), {2: ahead})
            s_o[l].relay()
        else:
            if not last_layer:
                g_o[l + 1].start()
            g_up[l].start_piece(0)
            ga.relay()
            ga.own()
            s_o[l].start_second()
            s_o[l].relay()
            g_qkv[l].finish()
            each(0, last, lambda k: project(l, k), {1: [ga.near, ga.near_right, ga.near_left], 2: ahead})
            ga.far()
            ga.far_done()
            ga.drain()
            project(l, 2)
        for i, (src, dst) in enumerate(((kc, kc_hbm), (vc, vc_hbm))):
            pltpu.make_async_copy(src.at[l], dst.at[l], c_sems.at[i]).start()
        if not last_layer:
            g_o[l + 1].finish()
            s_o[l + 1].start_first()
        sent_away(p, kt, qh, kv_sems, loc_heads)
        g_up[l].start_first(0 if first_layer else 1)
        took(kt, kv_sems.at[RECV])
        start_forward()
        took(qh, kv_sems.at[3])
        took(kt, kv_sems.at[5])
        took(kt, kv_sems.at[4])
        by_chip = [] if first_layer else [
            pltpu.make_async_copy(whole_o(l).at[:, at_r], wo.at[:, at_r], l_sems.at[i])
            for i, at_r in enumerate(rows(p.chip(k) * 2 * o_rows, 2 * o_rows) for k in range(n_chip))]

        def near_o():
            s_o[l].own()
            s_o[l].near_right()
            s_o[l].near_left()
            for k in (0, 1, last):
                for ld in by_chip[k:k + 1]:
                    ld.start()
        attend({0: [s_o[l].near], 1: [near_o, s_o[l].far]})
        g_up[l].relay([0])
        g_up[l].start_second()
        g_up[l].relay([1])
        g_qkv[l].drain()
        g_down[l].start()
        s_o[l].far_done()
        for ld in by_chip[2:3]:
            ld.start()
        took(obuf, o_sems.at[RECV])
        for ld in by_chip:
            ld.wait()

        def out_product(t, carry):
            cc = rows(t * col_w, col_w)
            bias = vec[4 * n_layers + l:4 * n_layers + l + 1, cc]
            hid[:, cc] = (hid[:, cc].astype(F32) + jnp.dot(obuf[...], wo[t], preferred_element_type=F32) + bias).astype(BF16)
            return carry
        lax.fori_loop(0, num_tx, out_product, 0)
        a_all[x, mine, :] = rows_norm(hid[...].astype(F32), vector(2, l), vector(3, l))
        gu = row_gather(u_sems)
        gu.start()
        if first_layer:
            took(bup, b_sems.at[RECV])
        gu.own()
        gu.relay()
        g_up[l].piece(0)
        each(0, last, lambda k: up(l, k, 0), {1: [gu.near, gu.near_right, gu.near_left]})
        if not first_layer:
            gu.far()
            gu.far_done()
            up(l, 2, 0)
        g_up[l].piece(1)
        g_down[l].step(0)

        def near_partial(n, carry):
            up(l, order(n), 1)
            partial(order(n), 0)
            return carry
        lax.fori_loop(1, last, near_partial, 0)
        if first_layer:
            gu.far()
            gu.far_done()
            up(l, 2, 0)
        up(l, 2, 1)
        gu.drain()
        s_o[l].drain()
        g_o[l].drain()
        g_up[l].drain()
        send_near(0)
        partial(2, 0)
        up(l, 0, 1)
        partial(0, 0)
        g_down[l].relay()
        if not last_layer:
            g_qkv[l + 1].start()
        send_far(0)
        for j in range(1, num_tx):
            g_down[l].step(j)

            def each_partial(n, carry):
                partial(lax.rem(2 + last * n, n_chip), j)
                return carry
            lax.fori_loop(0, n_chip, each_partial, 0)
            send_far(j)
            send_near(j)
            pass_on(j - 1)
            if j > 1:
                complete(l, j - 2)
                if last_layer:
                    give_back(j - 2)
        pass_on(num_tx - 1)
        if not last_layer:
            g_qkv[l + 1].relay()
        for j in range(num_tx - 2, num_tx):
            complete(l, j)
            if last_layer:
                give_back(j)
        for j in range(num_tx):
            for k in range(n_chip):
                for cp in to_sibling(k, j):
                    cp.wait_send()
            for kind in range(6):
                for cp in rs(kind, j):
                    cp.wait_send()
        g_down[l].drain()
        o_away(p, obuf, o_sems, head_w)

    took(kc_hbm, c_sems.at[SEND])
    took(vc_hbm, c_sems.at[RECV])
    took(xt_hbm.at[:, pl.ds(0, (n_dev - 1) * n_row)], x_sems.at[SEND])
    took(vbuf.at[pl.ds(0, num_tx - 1), 0], v_sems.at[SEND])
    took(vbuf.at[:, pl.ds(1, num_ty - 1)], v_sems.at[2])
    took(bup.at[:, pl.ds(0, (num_tx - 1) * bup_w)], b_sems.at[SEND])
    took(yt_hbm, y_sems.at[RECV])
    took(xt.at[pl.ds(0, (n_dev - 1) * piece_w)], y_sems.at[SEND])


def sent_away(p, kt, qh, kv_sems, loc_heads):
    stays = p.c == p.y // loc_heads
    n_tok = kt.shape[0]
    n_q = qh.shape[0]

    @pl.when(stays)
    def _():
        took(kt.at[pl.ds(0, n_tok * 3 // 4)], kv_sems.at[SEND])
        took(qh.at[pl.ds(0, n_q * 3 // 4)], kv_sems.at[2])

    @pl.when(jnp.logical_not(stays))
    def _():
        took(kt, kv_sems.at[SEND])
        took(qh, kv_sems.at[2])


def o_away(p, obuf, o_sems, head_w):
    stays = lax.rem(p.x, 2) == p.c

    @pl.when(stays)
    def _():
        took(obuf.at[:, pl.ds(0, obuf.shape[1] - head_w)], o_sems.at[SEND])

    @pl.when(jnp.logical_not(stays))
    def _():
        took(obuf, o_sems.at[SEND])


def decoder(num_tx, num_ty, xt, vectors, b_up, b_qkv, pos, wq, wk, wv, wo, wu, wd):
    n_layers, d_rows, loc_heads, head_w = wq.shape
    n_dev = num_tx * num_ty
    n_chip = num_ty // 2
    piece_w, n_tok = xt.shape
    width = piece_w * n_dev
    n_row = n_tok // n_dev
    blk = 2 * n_row
    loc_w = loc_heads * head_w
    tok_loc = n_tok // num_tx
    ff = wu.shape[2]
    col_w = wd.shape[2]
    n_q = n_tok // (2 * blk)
    n_vec = -(-len(vectors) * n_layers // 16) * 16
    vm = pl.BlockSpec(memory_space=pltpu.VMEM)
    hb = pl.BlockSpec(memory_space=pl.ANY)
    V = pltpu.VMEM
    dma = pltpu.SemaphoreType.DMA
    ends = dma((2,))
    cache = jax.ShapeDtypeStruct((n_layers, tok_loc, loc_heads, head_w), BF16)
    CG, RG = ColumnGather.SEMS, RingGather.SEMS
    return pl.pallas_call(
        functools.partial(decoder_kernel, num_tx, num_ty, n_layers),
        out_shape=(jax.ShapeDtypeStruct((piece_w, n_tok), BF16), cache, cache,
                   jax.ShapeDtypeStruct((max(n_layers - 1, 1), num_tx, width, col_w), BF16)),
        in_specs=[hb] + [vm] * 10 + [hb] * 7,
        out_specs=(hb,) * 4,
        scratch_shapes=[V((n_tok,), jnp.int32), V((width, n_row), BF16), V((n_vec, LANES), F32), V((n_vec, LANES), BF16), V((num_tx, num_ty, n_vec, LANES), BF16),
                        V((n_vec, width), F32), V((8, b_up.shape[1]), F32), V((8, ff), F32),
                        V((3, d_rows, loc_heads, head_w), BF16), V((n_layers, 3, d_rows, loc_w), BF16),
                        V((width, 3 * loc_w), BF16), V((width, ff), BF16), V((num_tx, ff, col_w), BF16),
                        V((num_tx, width, col_w), BF16), V((2, tok_loc, head_w), F32),
                        V((n_chip, blk, width), BF16), V((n_row, width), BF16),
                        V((n_chip, loc_heads, 2, blk, head_w), BF16), V((n_chip, loc_heads, head_w, blk), BF16), V(cache.shape, BF16),
                        V(cache.shape, BF16),
                        V((n_tok, head_w), BF16), V((head_w, n_tok), BF16), V((n_q * blk, head_w), BF16),
                        V((n_q, blk, head_w), BF16), V((n_row, width), BF16), V((n_chip, blk, ff), BF16),
                        V((n_chip, blk, width), F32), V((n_chip, n_row, width), F32),
                        V((2, n_row // 2, width), F32), V((4, n_row // 2, width), F32),
                        ends, dma((4,)), ends, ends, dma((2, RG)), dma((2, RG)), dma((2, 3 * CG)),
                        dma((n_layers, 2, CG)), dma((n_layers, 2, RG)), dma((2, 2 * CG)), dma((2, CG)), dma((6,)), ends, dma((2, 2 * n_chip * num_tx)),
                        dma((2, 12 * num_tx)), dma((4,)), ends],
        compiler_params=pltpu.CompilerParams(collective_id=1, has_side_effects=True, vmem_limit_bytes=63 << 20),
        name="decoder",
    )(xt, *vectors, b_up, *b_qkv, pos, wq, wk, wv, wo, wu, wd)[:3]


def hand_over_kernel(n, *refs):
    src, dst, buf, sems = refs[:n], refs[n:2 * n], refs[2 * n:3 * n], refs[3 * n]
    copies = []
    for i in range(n):
        step = src[i].shape[0] // 2
        for h in range(2):
            part = pl.ds(h * step, step)
            copies.append((pltpu.make_async_copy(src[i].at[part], buf[i].at[part], sems.at[SEND, 2 * i + h]),
                           pltpu.make_async_copy(buf[i].at[part], dst[i].at[part], sems.at[RECV, 2 * i + h])))
    for load, _ in copies:
        load.start()
    for load, store in copies:
        load.wait()
        store.start()
    for _, store in copies:
        store.wait()


def hand_over(arrays):
    n = len(arrays)
    hb = pl.BlockSpec(memory_space=pl.ANY)
    return pl.pallas_call(
        functools.partial(hand_over_kernel, n),
        out_shape=tuple(jax.ShapeDtypeStruct(a.shape, a.dtype) for a in arrays),
        in_specs=[hb] * n,
        out_specs=(hb,) * n,
        scratch_shapes=[pltpu.VMEM(a.shape, a.dtype) for a in arrays] + [pltpu.SemaphoreType.DMA((2, 2 * n))],
        name="hand_over",
    )(*arrays)


def solution(mesh):
    num_tx = mesh.shape['tx']
    num_ty = mesh.shape['ty']
    width_spec = P('dp', ('tx', 'ty'))
    vec_spec = P(None, ('tx', 'ty'))
    proj_spec = P(None, 'tx', 'ty', None)
    head_spec = P(None, 'ty', None)
    cache_spec = P(None, ('dp', 'tx'), 'ty', None)
    in_specs = (width_spec, P('dp'), P('dp'), vec_spec, vec_spec, proj_spec, head_spec, proj_spec, head_spec,
                proj_spec, head_spec, P(None, 'ty', None, 'tx'), vec_spec, vec_spec, vec_spec,
                P(None, 'tx', 'ty'), P(None, ('ty', 'tx')), P(None, 'ty', 'tx'), vec_spec)
    out_specs = (width_spec, cache_spec, cache_spec)

    def device_fn(x_loc, seg_all, pos_all, ln1_gain, ln1_bias, w_q, b_q, w_k, b_k, w_v, b_v, w_o, b_o,
                  ln2_gain, ln2_bias, w_up, b_up, w_down, b_down):
        yt, k, v = decoder(num_tx, num_ty, x_loc.T, (ln1_gain, ln1_bias, ln2_gain, ln2_bias, b_o, b_down), b_up,
                           (b_q, b_k, b_v), pos_all, w_q, w_k, w_v,
                           w_o.reshape(w_o.shape[0], -1, w_o.shape[-1]), w_up, w_down)
        yt, k, v = hand_over((yt, k, v))
        return yt.T, k, v

    return jax.shard_map(device_fn, mesh=mesh, in_specs=in_specs, out_specs=out_specs, check_vma=False)
```

```python
import math
import functools
import jax
import jax.numpy as jnp
from jax import lax
from jax.experimental import pallas as pl
from jax.experimental.pallas import tpu as pltpu
from jax.sharding import PartitionSpec as P

MESH = pl.DeviceIdType.MESH
F32 = jnp.float32
BF16 = jnp.bfloat16
ROPE_THETA = 100000.0
LOG2E = 1.4426950408889634
LANES = 128
BK = 1024
SEND, RECV = 0, 1


def rows_norm(x_f32, gain, bias):
    width = x_f32.shape[-1]
    mean = jnp.sum(x_f32, axis=-1, keepdims=True) / width
    var = jnp.sum(x_f32 * x_f32, axis=-1, keepdims=True) / width - mean * mean
    normed = (x_f32 - mean) * lax.rsqrt(var + 1e-5)
    return (normed * gain + bias).astype(BF16)


def gelu_tanh(x):
    return 0.5 * x * (1.0 + jnp.tanh(0.7978845608028654 * (x + 0.044715 * (x * x * x))))


def rows(at, n):
    return pl.ds(pl.multiple_of(at, n), n)


def unrolled_loop(n_from, n_to, body, value):
    for n in range(n_from, n_to):
        value = body(n, value)
    return value


class Place:
    def __init__(self, num_tx, num_ty):
        self.num_tx, self.num_ty, self.n_chip = num_tx, num_ty, num_ty // 2
        self.y = lax.axis_index('tx')
        self.ty = lax.axis_index('ty')
        self.x = self.ty // 2
        self.c = lax.rem(self.ty, 2)
        self.me = self.y * num_ty + self.ty
        self.sib = self.at(self.y, self.x * 2 + 1 - self.c)
        self.right, self.left = self.beside(1), self.beside(self.n_chip - 1)
        self.above, self.below = self.over(1), self.over(num_tx - 1)

    def at(self, y, ty):
        return {'tx': y, 'ty': ty}

    def chip(self, k):
        return lax.rem(self.x + k, self.n_chip)

    def side(self, k):
        return lax.rem(self.y + k, self.num_tx)

    def beside(self, k):
        return self.at(self.y, self.chip(k) * 2 + self.c)

    def over(self, k):
        return self.at(self.side(k), self.ty)


def remote(src, dst, send_sem, recv_sem, to):
    return pltpu.make_async_remote_copy(src_ref=src, dst_ref=dst, send_sem=send_sem, recv_sem=recv_sem, device_id=to,
                                        device_id_type=MESH)


def copy_or_send(here, src, dst, send_sem, recv_sem, to):
    @pl.when(here)
    def _():
        pltpu.make_async_copy(src, dst, recv_sem).start()

    @pl.when(jnp.logical_not(here))
    def _():
        remote(src, dst, send_sem, recv_sem, to).start()


def took(ref, sem):
    pltpu.make_async_copy(ref, ref, sem).wait()


class RingGather:
    SEMS = 14

    def __init__(self, p, view, sems):
        self.p = p
        self.view = view
        self.sems = sems
        x, c, d = p.x, p.c, 1 - p.c
        far, left, right = p.chip(2), p.chip(p.n_chip - 1), p.chip(1)
        self.plan = [(x, 0, p.right, left), (x, 1, p.left, right), (x, 1, p.right, left), (x, 0, p.left, right),
                     (left, 0, p.right, far), (right, 1, p.left, far),
                     (x, 0, p.sib, x), (x, 1, p.sib, x), (left, 0, p.sib, left), (left, 1, p.sib, left),
                     (right, 0, p.sib, right), (right, 1, p.sib, right), (far, 0, p.sib, far), (far, 1, p.sib, far)]

    def out(self, i):
        chip, half, to, _ = self.plan[i]
        ref = self.view(chip, self.p.c, half)
        return remote(ref, ref, self.sems.at[SEND, i], self.sems.at[RECV, i], to)

    def arrived(self, i):
        _, half, to, chip = self.plan[i]
        core = self.p.c if i < 6 else 1 - self.p.c
        ref = self.view(chip, core, half)
        remote(ref, ref, self.sems.at[SEND, i], self.sems.at[RECV, i], to).wait_recv()

    def start_first(self):
        for i in (6, 7, 0, 1):
            self.out(i).start()

    def start_second(self):
        for i in (2, 3):
            self.out(i).start()

    def start(self):
        self.start_first()
        self.start_second()

    def own(self):
        self.arrived(6)
        self.arrived(7)

    def relay(self):
        self.arrived(0)
        self.out(4).start()
        self.arrived(1)
        self.out(5).start()
        self.out(8).start()
        self.out(11).start()

    def near(self):
        self.arrived(2)
        self.out(9).start()
        self.arrived(3)
        self.out(10).start()

    def near_right(self):
        self.arrived(10)
        self.arrived(11)

    def near_left(self):
        self.arrived(8)
        self.arrived(9)

    def far(self):
        self.arrived(4)
        self.out(12).start()
        self.arrived(5)
        self.out(13).start()

    def far_done(self):
        self.arrived(12)
        self.arrived(13)

    def drain(self):
        for i in range(self.SEMS):
            self.out(i).wait_send()


class ColumnGather:
    SEMS = 8

    def __init__(self, p, pieces, sems, early=0):
        self.p = p
        self.pieces = pieces
        self.sems = sems
        self.early = early

    def copy(self, n, i):
        p = self.p
        src, dst = self.pieces[n]
        up, down = p.side(1), p.side(p.num_tx - 1)
        half, to = ((0, p.above), (1, p.below), (1, p.above), (0, p.below), (0, p.above), (1, p.below))[i]
        here = src(half) if i < 4 else dst(down if i == 4 else up, half)
        there = dst((p.y, p.y, p.y, p.y, down, up)[i], half)
        return remote(here, there, self.sems.at[SEND, n * self.SEMS + i], self.sems.at[RECV, n * self.SEMS + i], to)

    def arrived(self, n, i):
        p = self.p
        src, dst = self.pieces[n]
        up, down, far = p.side(1), p.side(p.num_tx - 1), p.side(2)
        half, frm = ((0, down), (1, up), (1, down), (0, up), (0, far), (1, far))[i]
        remote(src(half), dst(frm, half), self.sems.at[SEND, n * self.SEMS + i], self.sems.at[RECV, n * self.SEMS + i],
               p.above).wait_recv()

    def own(self, n, half):
        src, dst = self.pieces[n]
        return pltpu.make_async_copy(src(half), dst(self.p.y, half), self.sems.at[RECV, n * self.SEMS + 6 + half])

    def start_piece(self, n):
        for i in (0, 1):
            self.copy(n, i).start()

    def start_first(self, n_from=0):
        for i in (0, 1):
            for n in range(n_from, len(self.pieces)):
                self.copy(n, i).start()
        self.rest(range(self.early))

    def start_second(self):
        self.rest(range(self.early, len(self.pieces)))

    def rest(self, which):
        for i in (2, 3):
            for n in which:
                self.copy(n, i).start()
        for n in which:
            self.own(n, 0).start()
            self.own(n, 1).start()

    def start(self):
        self.start_first()
        self.start_second()

    def relay(self, which=None):
        for n in range(len(self.pieces)) if which is None else which:
            self.arrived(n, 0)
            self.copy(n, 4).start()
            self.arrived(n, 1)
            self.copy(n, 5).start()

    def step(self, j, which=None):
        for n in range(len(self.pieces)) if which is None else which:
            if j == 0:
                self.own(n, 0).wait()
                self.own(n, 1).wait()
            elif j > 1:
                self.arrived(n, 2 * j - 2)
                self.arrived(n, 2 * j - 1)

    def piece(self, n):
        for j in range(4):
            self.step(j, [n])

    def finish(self):
        for j in range(4):
            self.step(j)

    def drain(self):
        for n in range(len(self.pieces)):
            for i in range(6):
                self.copy(n, i).wait_send()


S_DIRECT_R, S_DIRECT_L, S_FAR_R, S_FAR_L, S_SUM_R, S_SUM_L = range(6)


def decoder_kernel(num_tx, num_ty, n_layers,
                   xt_hbm, g1_ref, b1_ref, g2_ref, b2_ref, bo_ref, bd_ref, bup_ref, bq_ref, bk_ref, bv_ref, pos_hbm,
                   wq_hbm, wk_hbm, wv_hbm, wo_hbm, wu_hbm, wd_hbm,
                   yt_hbm, kc_hbm, vc_hbm, go_hbm,
                   pos, xt, vrow, vloc, vbuf, vec, bloc, bup, raw, ws, w, wu, wd, wo, cs, a_all, hid, st, sv, kc, vc, kt, vt, qh, ob, obuf,
                   g, full, sibin, far_in, fin,
                   x_sems, v_sems, b_sems, y_sems, a_sems, u_sems, wq_sems, wo_sems, wx_sems, wu_sems, wd_sems,
                   kv_sems, o_sems, p_sems, r_sems, l_sems, c_sems):
    p = Place(num_tx, num_ty)
    n_dev = num_tx * num_ty
    n_chip, x, y, c, ty = p.n_chip, p.x, p.y, p.c, p.ty
    n_row, width = hid.shape
    blk = 2 * n_row
    half_row = n_row // 2
    loc_heads, head_w = wq_hbm.shape[2], wq_hbm.shape[3]
    loc_w = loc_heads * head_w
    col_w = wd.shape[2]
    piece_w = xt_hbm.shape[0]
    last = n_chip - 1
    mine, other = rows(c * n_row, n_row), rows((1 - c) * n_row, n_row)

    barrier = pltpu.get_barrier_semaphore()
    ids = [lax.rem(p.me + k, n_dev) for k in range(1, n_dev)]
    devs = [p.at(d // num_ty, lax.rem(d, num_ty)) for d in ids]
    for to in devs:
        pl.semaphore_signal(barrier, inc=1, device_id=to, device_id_type=MESH)

    def load_raw(l):
        return [pltpu.make_async_copy(src.at[l], raw.at[i], l_sems.at[i]) for i, src in enumerate((wq_hbm, wk_hbm, wv_hbm))]

    def flatten(l):
        for i, ld in enumerate(load_raw(l)):
            ld.wait()
            ws[l, i] = raw[i].reshape(ws.shape[2], loc_w)
    for ld in load_raw(0):
        ld.start()
    load_pos = pltpu.make_async_copy(pos_hbm, pos, l_sems.at[3])
    load_pos.start()
    vrow[...] = jnp.zeros_like(vrow)
    for i, ref in enumerate((g1_ref, b1_ref, g2_ref, b2_ref, bo_ref, bd_ref)):
        vrow[i * n_layers:(i + 1) * n_layers, :piece_w] = ref[...].astype(F32)
    vloc[...] = vrow[...].astype(BF16)
    bloc[...] = jnp.zeros_like(bloc)
    bloc[:n_layers, :] = bup_ref[...].astype(F32)
    pl.semaphore_wait(barrier, n_dev - 1)

    def halves(ref, l, n):
        return lambda h: ref.at[l, pl.ds(h * n, n)]

    def shard_rows(dst, n_shard, n, at_cols):
        return lambda ys, h: dst.at[rows(ys * n_shard + h * n, n), at_cols]

    qkv_rows = ws.shape[2]
    up_rows = wu_hbm.shape[1]
    o_rows = wo_hbm.shape[1]

    def gather_qkv(l):
        n = qkv_rows // 2
        return ColumnGather(p, [((lambda h, i=i: ws.at[l, i, pl.ds(h * n, n)]),
                                 shard_rows(w, qkv_rows, n, pl.ds(i * loc_w, loc_w))) for i in range(3)], wq_sems)

    def gather_up(l):
        n, half = up_rows // 2, wu.shape[1] // 2
        return ColumnGather(p, [((lambda h, at_c=at_c: wu_hbm.at[l, pl.ds(h * n, n), at_c]), shard_rows(wu, up_rows, n, at_c))
                                for at_c in (pl.ds(0, half), pl.ds(half, half))], wu_sems, early=1)

    def gather_down(l):
        n = col_w // 2
        return ColumnGather(p, [((lambda h: wd_hbm.at[l, :, pl.ds(h * n, n)]), lambda ys, h: wd.at[ys, :, pl.ds(h * n, n)])],
                            wd_sems)

    def whole_o(l):
        return wo if l == 0 else go_hbm.at[l - 1]

    def gather_o(l):
        n = o_rows // 2
        return ColumnGather(p, [(halves(wo_hbm, l, n), lambda ys, h: whole_o(l).at[ys, rows(ty * o_rows + h * n, n)])],
                            wo_sems.at[l])

    def spread_o(l):
        n = num_tx // 2
        return RingGather(p, lambda chip, core, h: whole_o(l).at[pl.ds(h * n, n), rows((chip * 2 + core) * o_rows, o_rows)],
                          wx_sems.at[l])

    g_qkv = [gather_qkv(l) for l in range(n_layers)]
    g_up = [gather_up(l) for l in range(n_layers)]
    g_down = [gather_down(l) for l in range(n_layers)]
    g_o = [gather_o(l) for l in range(n_layers)]
    s_o = [spread_o(l) for l in range(n_layers)]

    for k in range(1, num_tx):
        remote(vloc, vbuf.at[y, ty], v_sems.at[SEND], v_sems.at[RECV], p.over(k)).start()
    for d, to in zip(ids, devs):
        remote(xt_hbm.at[:, rows(d * n_row, n_row)], xt.at[rows(p.me * piece_w, piece_w)], x_sems.at[SEND], x_sems.at[RECV], to).start()
    g_o[0].start()
    flatten(0)
    g_qkv[0].start_first()
    pltpu.make_async_copy(xt_hbm.at[:, rows(p.me * n_row, n_row)], xt.at[rows(p.me * piece_w, piece_w)], x_sems.at[RECV]).start()
    pltpu.make_async_copy(vloc, vbuf.at[y, ty], v_sems.at[RECV]).start()
    bup_w = bup_ref.shape[1]
    for k in range(1, num_tx):
        remote(bloc, bup.at[:, rows(y * bup_w, bup_w)], b_sems.at[SEND], b_sems.at[RECV], p.over(k)).start()
    pltpu.make_async_copy(bloc, bup.at[:, rows(y * bup_w, bup_w)], b_sems.at[RECV]).start()
    column = vbuf.at[:, ty]
    took(column, v_sems.at[RECV])
    for k in range(1, num_ty):
        remote(column, column, v_sems.at[2], v_sems.at[3], p.at(y, lax.rem(ty + k, num_ty))).start()
    for l in range(1, n_layers):
        for ld in load_raw(l):
            ld.start()
        flatten(l)

    load_pos.wait()
    lane = lax.broadcasted_iota(jnp.int32, (1, head_w), 1)
    inv_freq = jnp.exp(lax.rem(lane, head_w // 2).astype(F32) * (-2.0 * math.log(ROPE_THETA) / head_w))
    sign = jnp.where(lane < head_w // 2, -1.0, 1.0)

    def positions(b):
        return pos[rows(b * blk, blk)].reshape(1, blk)

    def angles(k, carry):
        ang = jnp.broadcast_to(positions(y * n_chip + k).astype(F32), (head_w, blk)).T * inv_freq
        cs[0, rows(k * blk, blk), :] = jnp.cos(ang)
        cs[1, rows(k * blk, blk), :] = jnp.sin(ang) * sign
        return carry
    lax.fori_loop(0, n_chip, angles, 0)
    took(vbuf.at[:, pl.ds(1, num_ty - 1)], v_sems.at[3])
    per = LANES // piece_w
    for j in range(width // LANES):
        vec[:, j * LANES:(j + 1) * LANES] = jnp.concatenate(
            [vbuf[(per * j + i) // num_ty, (per * j + i) % num_ty][:, :piece_w].astype(F32) for i in range(per)], axis=1)
    took(xt, x_sems.at[RECV])

    def turn(j, carry):
        hid[:, rows(j * LANES, LANES)] = xt[rows(j * LANES, LANES), :].T
        return carry
    lax.fori_loop(0, width // LANES, turn, 0)

    def vector(i, l):
        return vec[i * n_layers + l:i * n_layers + l + 1, :]

    def row_gather(sems):
        return RingGather(p, lambda chip, core, h: a_all.at[chip, rows(core * n_row + h * half_row, half_row)], sems)

    def order(n):
        return n + n // 2 - 2 * (n // 3)

    def at_step(n, hooks):
        for at_n, hook in hooks.items():
            if isinstance(n, int):
                for h in hook if n == at_n else ():
                    h()
            else:
                @pl.when(n == at_n)
                def _():
                    for h in hook:
                        h()

    def each(n_from, n_to, body, hooks):
        def step(n, carry):
            at_step(n, hooks)
            body(order(n))
            return carry
        lax.fori_loop(n_from, n_to, step, 0)

    def project(l, k):
        slot = p.chip(k)
        at_row = rows(slot * blk, blk)
        acc = jnp.dot(a_all[slot], w[...], preferred_element_type=F32)
        cos_t, sin_t = cs[0, at_row, :], cs[1, at_row, :]
        for i, bias in enumerate((bq_ref, bk_ref, bv_ref)):
            parts = []
            for h in range(loc_heads):
                lo = i * loc_w + h * head_w
                v = acc[:, lo:lo + head_w] + bias[l, h:h + 1, :].astype(F32)
                if i < 2:
                    v = v * cos_t + pltpu.roll(v, head_w // 2, 1) * sin_t
                v = v.astype(BF16)
                parts.append(v)
                if i < 2:
                    st[k, h, i] = v
                else:
                    sv[k, h] = v.T
            if i > 0:
                (kc, vc)[i - 1][l, at_row] = jnp.concatenate(parts, axis=1).reshape(blk, loc_heads, head_w)
        at_tok = rows((y * n_chip + slot) * blk, blk)
        par = lax.rem(slot, 2)
        at_q = rows((y * (n_chip // 2) + slot // 2) * blk, blk)
        for h in range(loc_heads):
            yd = c * loc_heads + h
            for r, (src, dst) in enumerate(((st.at[k, h, 1], kt.at[at_tok]), (sv.at[k, h], vt.at[:, at_tok]))):
                copy_or_send(jnp.logical_and(yd == y, c == r), src, dst, kv_sems.at[SEND], kv_sems.at[RECV], p.at(yd, x * 2 + r))
            copy_or_send(jnp.logical_and(yd == y, c == par), st.at[k, h, 0], qh.at[at_q], kv_sems.at[2], kv_sems.at[3],
                         p.at(yd, x * 2 + par))

    n_q = ob.shape[0]
    q_grp = 2 * blk
    n_grp = n_q * blk // q_grp
    n_sub = BK // blk

    def attend(hooks, unrolled):
        def step(n, carry):
            loop = unrolled_loop if isinstance(n, int) else lax.fori_loop
            grp = n_grp - 1 - n
            q = qh[rows(grp * q_grp, q_grp), :]
            q_col = lax.broadcasted_iota(jnp.int32, (1, blk), 1)
            at_q = [(2 * (2 * grp + i) + c) for i in range(2)]
            q_pos = jnp.concatenate([q_col + b * blk for b in at_q], axis=1)
            first = q_pos - jnp.concatenate([positions(b) for b in at_q], axis=1)
            key = lax.broadcasted_iota(jnp.int32, (blk, q_grp), 0)
            scale = head_w ** -0.5 * LOG2E

            def score(j, m, diag):
                s = lax.dot_general(kt[rows(j * BK, BK), :], q, (((1,), (1,)), ((), ())), preferred_element_type=F32)
                for i in range(n_sub):
                    k_pos = key + (j * BK + i * blk)
                    ok = k_pos >= first
                    if diag:
                        ok = jnp.logical_and(ok, k_pos <= q_pos)
                    part = jnp.where(ok, s[i * blk:(i + 1) * blk], -1e30)
                    full[j, :, i * q_grp:(i + 1) * q_grp] = part
                    m = jnp.maximum(m, jnp.max(part.reshape(blk // 8, 8, q_grp), axis=0))
                return m
            m = loop(0, grp, lambda j, m: score(j, m, False), jnp.full((8, q_grp), -1e30, F32))
            m = jnp.max(score(grp, m, True), axis=0, keepdims=True)

            def expo(j, t):
                for i in range(n_sub):
                    e = jnp.exp2((full[j, :, i * q_grp:(i + 1) * q_grp] - m) * scale)
                    full[j, :, i * q_grp:(i + 1) * q_grp] = e
                    t = t + jnp.sum(e.reshape(blk // 8, 8, q_grp), axis=0)
                return t
            t = loop(0, grp + 1, expo, jnp.zeros((8, q_grp), F32))
            inv = 1.0 / jnp.sum(t, axis=0, keepdims=True)

            def apply(j, acc):
                prob = jnp.concatenate([(full[j, :, i * q_grp:(i + 1) * q_grp] * inv).astype(BF16) for i in range(n_sub)], axis=0)
                return acc + jnp.dot(vt[:, rows(j * BK, BK)], prob, preferred_element_type=F32)
            out = loop(0, grp + 1, apply, jnp.zeros((head_w, q_grp), F32)).T.astype(BF16)
            cols_o = rows((x * num_tx + y) * head_w, head_w)
            for i, b in enumerate(at_q):
                ob[2 * grp + i] = out[i * blk:(i + 1) * blk]
                yt, xd = b // n_chip, lax.rem(b, n_chip)
                for r in range(2):
                    here = jnp.logical_and(jnp.logical_and(yt == y, xd == x), c == r)
                    copy_or_send(here, ob.at[2 * grp + i, pl.ds(r * n_row, n_row)], obuf.at[:, cols_o], o_sems.at[SEND],
                                 o_sems.at[RECV], p.at(yt, xd * 2 + r))
            at_step(n, hooks)
            return carry
        if unrolled:
            step(0, 0)
        lax.fori_loop(1 if unrolled else 0, n_grp, step, 0)

    def up(l, k, n):
        half = wu.shape[1] // 2
        cc = pl.ds(n * half, half)
        h = jnp.dot(a_all[p.chip(k)], wu[:, cc], preferred_element_type=F32) + bup[l:l + 1, cc]
        g[k, :, cc] = gelu_tanh(h).astype(BF16)

    half_col = col_w // 2
    below, above, far_side = p.side(num_tx - 1), p.side(1), p.side(2)
    blocks = (((y, 0), (y, 1)), ((below, 0), (above, 1)), ((below, 1), (above, 0)), ((far_side, 0), (far_side, 1)))
    cols = [[rows(t * col_w + h * half_col, half_col) for t, h in pair] for pair in blocks]
    top, bottom = rows(c * n_row, half_row), rows(c * n_row + half_row, half_row)

    def to_sibling(k, j):
        out = []
        for i in range(2):
            at_s = (k * num_tx + j) * 2 + i
            out.append(remote(full.at[k, other, cols[j][i]], sibin.at[k, :, cols[j][i]], p_sems.at[SEND, at_s], p_sems.at[RECV, at_s],
                              p.sib))
        return out

    def rs(kind, j):
        k, part, dst, to = ((1, bottom, fin.at[0], p.right), (last, top, fin.at[1], p.left), (2, top, far_in.at[0], p.right),
                            (2, bottom, far_in.at[1], p.left), (1, top, fin.at[2], p.right),
                            (last, bottom, fin.at[3], p.left))[kind]
        out = []
        for i in range(2):
            at_s = (kind * num_tx + j) * 2 + i
            out.append(remote(full.at[k, part, cols[j][i]], dst.at[:, cols[j][i]], r_sems.at[SEND, at_s], r_sems.at[RECV, at_s], to))
        return out

    def start(copies):
        for cp in copies:
            cp.start()

    def landed(copies):
        for cp in copies:
            cp.wait_recv()

    def partial(k, j):
        for i, (t, h) in enumerate(blocks[j]):
            full[k, :, cols[j][i]] = jnp.dot(g[k], wd[t, :, h * half_col:(h + 1) * half_col], preferred_element_type=F32)
        start(to_sibling(k, j))

    def pair_sum(k, j):
        landed(to_sibling(k, j))
        for cc in cols[j]:
            full[k, mine, cc] = full[k, mine, cc] + sibin[k, :, cc]

    def send_near(j):
        pair_sum(1, j)
        start(rs(S_DIRECT_R, j))
        pair_sum(last, j)
        start(rs(S_DIRECT_L, j))

    def send_far(j):
        pair_sum(2, j)
        start(rs(S_FAR_R, j))
        start(rs(S_FAR_L, j))

    def pass_on(j):
        for i, cc in enumerate(cols[j]):
            rs(S_FAR_R, j)[i].wait_recv()
            full[1, top, cc] = full[1, top, cc] + far_in[0, :, cc]
            rs(S_SUM_R, j)[i].start()
            rs(S_FAR_L, j)[i].wait_recv()
            full[last, bottom, cc] = full[last, bottom, cc] + far_in[1, :, cc]
            rs(S_SUM_L, j)[i].start()

    def complete(l, j):
        pair_sum(0, j)
        for kind in (S_DIRECT_R, S_DIRECT_L, S_SUM_R, S_SUM_L):
            landed(rs(kind, j))
        for cc in cols[j]:
            bias = vec[5 * n_layers + l:5 * n_layers + l + 1, cc]
            for part, out, ins in ((top, pl.ds(0, half_row), (1, 2)), (bottom, pl.ds(half_row, half_row), (0, 3))):
                tot = full[0, part, cc] + fin[ins[0], :, cc] + fin[ins[1], :, cc]
                hid[out, cc] = (hid[out, cc].astype(F32) + tot + bias).astype(BF16)

    def give_back(j):
        for t, h in blocks[j]:
            for n in range(half_col // LANES):
                at_c = rows(t * col_w + h * half_col + n * LANES, LANES)
                xt[at_c, :] = hid[:, at_c].T
            for k in range(num_ty // 2):
                to_ty = h * (num_ty // 2) + k
                copy_or_send(jnp.logical_and(t == y, ty == to_ty), xt.at[rows((t * num_ty + to_ty) * piece_w, piece_w)],
                             yt_hbm.at[:, rows(p.me * n_row, n_row)], y_sems.at[SEND], y_sems.at[RECV], p.at(t, to_ty))

    def start_forward():
        @pl.when(c == 0)
        def _():
            remote(kt, kt, kv_sems.at[4], kv_sems.at[5], p.sib).start()

        @pl.when(c != 0)
        def _():
            remote(vt, vt, kv_sems.at[4], kv_sems.at[5], p.sib).start()

    for l in range(n_layers):
        first_layer, last_layer = l == 0, l == n_layers - 1
        a_all[x, mine, :] = rows_norm(hid[...].astype(F32), vector(0, l), vector(1, l))
        ga = row_gather(a_sems)
        ga.start()
        ahead = [] if last_layer else [g_o[l + 1].relay]
        if first_layer:
            g_o[l].relay()
            g_qkv[l].start_second()
            ga.relay()
            g_qkv[l].relay()
            if not last_layer:
                g_o[l + 1].start()
            ga.own()
            ga.near()
            g_o[l].finish()
            s_o[l].start()
            ga.near_right()
            ga.near_left()
            ga.far()
            ga.far_done()
            ga.drain()
            g_qkv[l].finish()
            each(0, n_chip, lambda k: project(l, k), {2: ahead})
            s_o[l].relay()
        else:
            if not last_layer:
                g_o[l + 1].start()
            g_up[l].start_piece(0)
            ga.relay()
            ga.own()
            s_o[l].start_second()
            s_o[l].relay()
            g_qkv[l].finish()
            each(0, last, lambda k: project(l, k), {1: [ga.near, ga.near_right, ga.near_left], 2: ahead})
            ga.far()
            ga.far_done()
            ga.drain()
            project(l, 2)
        for i, (src, dst) in enumerate(((kc, kc_hbm), (vc, vc_hbm))):
            pltpu.make_async_copy(src.at[l], dst.at[l], c_sems.at[i]).start()
        if not last_layer:
            g_o[l + 1].finish()
            s_o[l + 1].start_first()
        sent_away(p, kt, qh, kv_sems, loc_heads)
        g_up[l].start_first(0 if first_layer else 1)
        took(kt, kv_sems.at[RECV])
        start_forward()
        took(qh, kv_sems.at[3])
        took(kt, kv_sems.at[5])
        took(kt, kv_sems.at[4])
        by_chip = [] if first_layer else [
            pltpu.make_async_copy(whole_o(l).at[:, at_r], wo.at[:, at_r], l_sems.at[i])
            for i, at_r in enumerate(rows(p.chip(k) * 2 * o_rows, 2 * o_rows) for k in range(n_chip))]

        def near_o():
            s_o[l].own()
            s_o[l].near_right()
            s_o[l].near_left()
            for k in (0, 1, last):
                for ld in by_chip[k:k + 1]:
                    ld.start()
        attend({0: [s_o[l].near], 1: [near_o, s_o[l].far]}, not first_layer)
        g_up[l].relay([0])
        g_up[l].start_second()
        g_up[l].relay([1])
        g_qkv[l].drain()
        g_down[l].start()
        s_o[l].far_done()
        for ld in by_chip[2:3]:
            ld.start()
        took(obuf, o_sems.at[RECV])
        for ld in by_chip:
            ld.wait()

        def out_product(t, carry):
            cc = rows(t * col_w, col_w)
            bias = vec[4 * n_layers + l:4 * n_layers + l + 1, cc]
            hid[:, cc] = (hid[:, cc].astype(F32) + jnp.dot(obuf[...], wo[t], preferred_element_type=F32) + bias).astype(BF16)
            return carry
        lax.fori_loop(0, num_tx, out_product, 0)
        a_all[x, mine, :] = rows_norm(hid[...].astype(F32), vector(2, l), vector(3, l))
        gu = row_gather(u_sems)
        gu.start()
        if first_layer:
            took(bup, b_sems.at[RECV])
        gu.own()
        gu.relay()
        g_up[l].piece(0)
        each(0, last, lambda k: up(l, k, 0), {1: [gu.near, gu.near_right, gu.near_left]})
        if not first_layer:
            gu.far()
            gu.far_done()
            up(l, 2, 0)
        g_up[l].piece(1)
        g_down[l].step(0)

        def near_partial(n, carry):
            up(l, order(n), 1)
            partial(order(n), 0)
            return carry
        lax.fori_loop(1, last, near_partial, 0)
        if first_layer:
            gu.far()
            gu.far_done()
            up(l, 2, 0)
        up(l, 2, 1)
        gu.drain()
        s_o[l].drain()
        g_o[l].drain()
        g_up[l].drain()
        send_near(0)
        partial(2, 0)
        up(l, 0, 1)
        partial(0, 0)
        g_down[l].relay()
        if not last_layer:
            g_qkv[l + 1].start()
        send_far(0)
        for j in range(1, num_tx):
            g_down[l].step(j)

            def each_partial(n, carry):
                partial(lax.rem(2 + last * n, n_chip), j)
                return carry
            lax.fori_loop(0, n_chip, each_partial, 0)
            send_far(j)
            send_near(j)
            pass_on(j - 1)
            if j > 1:
                complete(l, j - 2)
                if last_layer:
                    give_back(j - 2)
        pass_on(num_tx - 1)
        if not last_layer:
            g_qkv[l + 1].relay()
        for j in range(num_tx - 2, num_tx):
            complete(l, j)
            if last_layer:
                give_back(j)
        for j in range(num_tx):
            for k in range(n_chip):
                for cp in to_sibling(k, j):
                    cp.wait_send()
            for kind in range(6):
                for cp in rs(kind, j):
                    cp.wait_send()
        g_down[l].drain()
        o_away(p, obuf, o_sems, head_w)

    took(kc_hbm, c_sems.at[SEND])
    took(vc_hbm, c_sems.at[RECV])
    took(xt_hbm.at[:, pl.ds(0, (n_dev - 1) * n_row)], x_sems.at[SEND])
    took(vbuf.at[pl.ds(0, num_tx - 1), 0], v_sems.at[SEND])
    took(vbuf.at[:, pl.ds(1, num_ty - 1)], v_sems.at[2])
    took(bup.at[:, pl.ds(0, (num_tx - 1) * bup_w)], b_sems.at[SEND])
    took(yt_hbm, y_sems.at[RECV])
    took(xt.at[pl.ds(0, (n_dev - 1) * piece_w)], y_sems.at[SEND])


def sent_away(p, kt, qh, kv_sems, loc_heads):
    stays = p.c == p.y // loc_heads
    n_tok = kt.shape[0]
    n_q = qh.shape[0]

    @pl.when(stays)
    def _():
        took(kt.at[pl.ds(0, n_tok * 3 // 4)], kv_sems.at[SEND])
        took(qh.at[pl.ds(0, n_q * 3 // 4)], kv_sems.at[2])

    @pl.when(jnp.logical_not(stays))
    def _():
        took(kt, kv_sems.at[SEND])
        took(qh, kv_sems.at[2])


def o_away(p, obuf, o_sems, head_w):
    stays = lax.rem(p.x, 2) == p.c

    @pl.when(stays)
    def _():
        took(obuf.at[:, pl.ds(0, obuf.shape[1] - head_w)], o_sems.at[SEND])

    @pl.when(jnp.logical_not(stays))
    def _():
        took(obuf, o_sems.at[SEND])


def decoder(num_tx, num_ty, xt, vectors, b_up, b_qkv, pos, wq, wk, wv, wo, wu, wd):
    n_layers, d_rows, loc_heads, head_w = wq.shape
    n_dev = num_tx * num_ty
    n_chip = num_ty // 2
    piece_w, n_tok = xt.shape
    width = piece_w * n_dev
    n_row = n_tok // n_dev
    blk = 2 * n_row
    loc_w = loc_heads * head_w
    tok_loc = n_tok // num_tx
    ff = wu.shape[2]
    col_w = wd.shape[2]
    n_q = n_tok // (2 * blk)
    n_vec = -(-len(vectors) * n_layers // 16) * 16
    vm = pl.BlockSpec(memory_space=pltpu.VMEM)
    hb = pl.BlockSpec(memory_space=pl.ANY)
    V = pltpu.VMEM
    dma = pltpu.SemaphoreType.DMA
    ends = dma((2,))
    cache = jax.ShapeDtypeStruct((n_layers, tok_loc, loc_heads, head_w), BF16)
    CG, RG = ColumnGather.SEMS, RingGather.SEMS
    return pl.pallas_call(
        functools.partial(decoder_kernel, num_tx, num_ty, n_layers),
        out_shape=(jax.ShapeDtypeStruct((piece_w, n_tok), BF16), cache, cache,
                   jax.ShapeDtypeStruct((max(n_layers - 1, 1), num_tx, width, col_w), BF16)),
        in_specs=[hb] + [vm] * 10 + [hb] * 7,
        out_specs=(hb,) * 4,
        scratch_shapes=[V((n_tok,), jnp.int32), V((width, n_row), BF16), V((n_vec, LANES), F32), V((n_vec, LANES), BF16), V((num_tx, num_ty, n_vec, LANES), BF16),
                        V((n_vec, width), F32), V((8, b_up.shape[1]), F32), V((8, ff), F32),
                        V((3, d_rows, loc_heads, head_w), BF16), V((n_layers, 3, d_rows, loc_w), BF16),
                        V((width, 3 * loc_w), BF16), V((width, ff), BF16), V((num_tx, ff, col_w), BF16),
                        V((num_tx, width, col_w), BF16), V((2, tok_loc, head_w), F32),
                        V((n_chip, blk, width), BF16), V((n_row, width), BF16),
                        V((n_chip, loc_heads, 2, blk, head_w), BF16), V((n_chip, loc_heads, head_w, blk), BF16), V(cache.shape, BF16),
                        V(cache.shape, BF16),
                        V((n_tok, head_w), BF16), V((head_w, n_tok), BF16), V((n_q * blk, head_w), BF16),
                        V((n_q, blk, head_w), BF16), V((n_row, width), BF16), V((n_chip, blk, ff), BF16),
                        V((n_chip, blk, width), F32), V((n_chip, n_row, width), F32),
                        V((2, n_row // 2, width), F32), V((4, n_row // 2, width), F32),
                        ends, dma((4,)), ends, ends, dma((2, RG)), dma((2, RG)), dma((2, 3 * CG)),
                        dma((n_layers, 2, CG)), dma((n_layers, 2, RG)), dma((2, 2 * CG)), dma((2, CG)), dma((6,)), ends, dma((2, 2 * n_chip * num_tx)),
                        dma((2, 12 * num_tx)), dma((4,)), ends],
        compiler_params=pltpu.CompilerParams(collective_id=1, has_side_effects=True, vmem_limit_bytes=63 << 20),
        name="decoder",
    )(xt, *vectors, b_up, *b_qkv, pos, wq, wk, wv, wo, wu, wd)[:3]


def hand_over_kernel(n, *refs):
    src, dst, buf, sems = refs[:n], refs[n:2 * n], refs[2 * n:3 * n], refs[3 * n]
    copies = []
    for i in range(n):
        step = src[i].shape[0] // 2
        for h in range(2):
            part = pl.ds(h * step, step)
            copies.append((pltpu.make_async_copy(src[i].at[part], buf[i].at[part], sems.at[SEND, 2 * i + h]),
                           pltpu.make_async_copy(buf[i].at[part], dst[i].at[part], sems.at[RECV, 2 * i + h])))
    for load, _ in copies:
        load.start()
    for load, store in copies:
        load.wait()
        store.start()
    for _, store in copies:
        store.wait()


def hand_over(arrays):
    n = len(arrays)
    hb = pl.BlockSpec(memory_space=pl.ANY)
    return pl.pallas_call(
        functools.partial(hand_over_kernel, n),
        out_shape=tuple(jax.ShapeDtypeStruct(a.shape, a.dtype) for a in arrays),
        in_specs=[hb] * n,
        out_specs=(hb,) * n,
        scratch_shapes=[pltpu.VMEM(a.shape, a.dtype) for a in arrays] + [pltpu.SemaphoreType.DMA((2, 2 * n))],
        name="hand_over",
    )(*arrays)


def solution(mesh):
    num_tx = mesh.shape['tx']
    num_ty = mesh.shape['ty']
    width_spec = P('dp', ('tx', 'ty'))
    vec_spec = P(None, ('tx', 'ty'))
    proj_spec = P(None, 'tx', 'ty', None)
    head_spec = P(None, 'ty', None)
    cache_spec = P(None, ('dp', 'tx'), 'ty', None)
    in_specs = (width_spec, P('dp'), P('dp'), vec_spec, vec_spec, proj_spec, head_spec, proj_spec, head_spec,
                proj_spec, head_spec, P(None, 'ty', None, 'tx'), vec_spec, vec_spec, vec_spec,
                P(None, 'tx', 'ty'), P(None, ('ty', 'tx')), P(None, 'ty', 'tx'), vec_spec)
    out_specs = (width_spec, cache_spec, cache_spec)

    def device_fn(x_loc, seg_all, pos_all, ln1_gain, ln1_bias, w_q, b_q, w_k, b_k, w_v, b_v, w_o, b_o,
                  ln2_gain, ln2_bias, w_up, b_up, w_down, b_down):
        yt, k, v = decoder(num_tx, num_ty, x_loc.T, (ln1_gain, ln1_bias, ln2_gain, ln2_bias, b_o, b_down), b_up,
                           (b_q, b_k, b_v), pos_all, w_q, w_k, w_v,
                           w_o.reshape(w_o.shape[0], -1, w_o.shape[-1]), w_up, w_down)
        yt, k, v = hand_over((yt, k, v))
        return yt.T, k, v

    return jax.shard_map(device_fn, mesh=mesh, in_specs=in_specs, out_specs=out_specs, check_vma=False)
```
